32 devices in a mesh: dp: 4 (over y, x), head: 4 (over z), ctx: 2 (over core).
Axes of the slice: x: 2, y: 2, z: 4, core: 2. Of those that a mesh axis runs over, the one named last changes fastest.
Arguments:
- tokens: bfloat16 [8192, 768], P(('dp', 'head', 'ctx')), may hold values from -6 to 6
- cotangent: bfloat16 [8192, 768], P(('dp', 'head', 'ctx')), may hold values from -6 to 6
- in_master: float32 [768, 3968], P('head'), may hold values from -4 to 4
- in_moment: float32 [768, 3968], P('head'), may hold values from -245760 to 245760
- in_second: float32 [768, 3968], P('head'), may hold values from 0 to 8192000, as said below
- out_master: float32 [3840, 768], P('head'), may hold values from -4 to 4
- out_moment: float32 [3840, 768], P('head'), may hold values from -245760 to 245760
- out_second: float32 [3840, 768], P('head'), may hold values from 0 to 8192000, as said below
- vec_master: float32 [7808], replicated, may hold values from -4 to 4
- vec_moment: float32 [7808], replicated, may hold values from -245760 to 245760
- vec_second: float32 [7808], replicated, may hold values from 0 to 8192000, as said below
- rotary_scale: int32 [1], replicated, may hold values from 2 to 8
Outputs:
- output: bfloat16 [8192, 768], P(('dp', 'head', 'ctx'))
- input_grad: bfloat16 [8192, 768], P(('dp', 'head', 'ctx'))
- in_moment_new: float32 [768, 3968], P('head')
- in_second_new: float32 [768, 3968], P('head')
- in_master_new: float32 [768, 3968], P('head')
- in_copy: bfloat16 [768, 3968], P('head')
- out_moment_new: float32 [3840, 768], P('head')
- out_second_new: float32 [3840, 768], P('head')
- out_master_new: float32 [3840, 768], P('head')
- out_copy: bfloat16 [3840, 768], P('head')
- vec_moment_new: float32 [7808], replicated
- vec_second_new: float32 [7808], replicated
- vec_master_new: float32 [7808], replicated
The draws below stay inside these ranges and needn't reach their ends.
Inputs may be any that keep to these rules, and one draw needn't show every extreme that they name: `in_second`: positive entries. `out_second`: positive entries. `vec_second`: positive entries.
All inputs are finite; a program needn't handle non-finite values.
Results may differ from the reference program's by a relative error of at most 0.014.
The reference program's roundings to bfloat16 on the way count: a program that leaves them out, or rounds other values in their place, can miss the bound.
Values may be sent and summed in bfloat16 or wider, within the bound.
A program may use at most 192 MiB of HBM per device.

```python
import math
import jax
import jax.numpy as jnp
from jax import lax

HEADS = 12
HEAD_DIM = 64
FF = 3072
ROT = 16
D = 768
KEY_BLOCK = 1024
ADAM_STEP = 3
SEQ_LEN = 2048
TOKENS = 8192
C_IN = 3968
C_OUT = 3840
VEC = 7808


def rough_field(key, dims_shape):
    return jnp.clip(jax.random.normal(key, dims_shape, jnp.float32), -4.0, 4.0)


def attention_spread():
    return max(SEQ_LEN / 110.0, 1.0) ** 0.5


def in_scales():
    columns = jnp.arange(C_IN)
    return jnp.where(columns < D + HEAD_DIM, (2.0 / D) ** 0.5, D ** (-0.5))


def out_scales():
    rows_index = jnp.arange(C_OUT)
    return jnp.where(rows_index < D, 4.0 * D ** (-0.5), 1.5 * FF ** (-0.5))


def in_grad_scales():
    columns = jnp.arange(C_IN)
    spread = attention_spread()
    return TOKENS ** 0.5 * jnp.where(columns < D, 5.6 / spread, jnp.where(columns < D + 2 * HEAD_DIM, 15.0 / spread, 0.45))


def out_grad_scales():
    rows_index = jnp.arange(C_OUT)
    return TOKENS ** 0.5 * jnp.where(rows_index < D, 1.0 / attention_spread(), 0.6)


def vec_grad_scales():
    places = jnp.arange(VEC)
    spread = attention_spread()
    return TOKENS ** 0.5 * jnp.where(places < 4 * D, 2.0, jnp.where(places < 5 * D, 1.0, jnp.where(places < 6 * D, 5.6 / spread, jnp.where(places < 6 * D + 2 * HEAD_DIM, 15.0 / spread, 0.45))))


def signed_moment(key, scales):
    front_key, back_key = jax.random.split(key)
    signs = jnp.where(jax.random.bernoulli(front_key, 0.5, scales.shape), 1.0, -1.0)
    return signs * jax.random.uniform(back_key, scales.shape, jnp.float32, 0.5, 1.5) * scales


def square_moment(key, scales):
    return scales * scales * jnp.exp(jax.random.uniform(key, scales.shape, jnp.float32, 0.0, math.log(4.0)))


def draw_in_master(key, part):
    return in_scales()[None, :] * rough_field(key, (D, C_IN))


def draw_in_moment(key, part):
    return signed_moment(key, jnp.broadcast_to(in_grad_scales()[None, :], (D, C_IN)))


def draw_in_second(key, part):
    return square_moment(key, jnp.broadcast_to(in_grad_scales()[None, :], (D, C_IN)))


def draw_out_master(key, part):
    return out_scales()[:, None] * rough_field(key, (C_OUT, D))


def draw_out_moment(key, part):
    return signed_moment(key, jnp.broadcast_to(out_grad_scales()[:, None], (C_OUT, D)))


def draw_out_second(key, part):
    return square_moment(key, jnp.broadcast_to(out_grad_scales()[:, None], (C_OUT, D)))


def draw_vec_master(key, part):
    places = jnp.arange(VEC)
    entries = jnp.clip(jax.random.normal(key, (VEC,), jnp.float32), -4.0, 4.0)
    is_gain = (places < D) | (places >= 2 * D) & (places < 3 * D)
    return jnp.where(is_gain, 1.0 + 0.2 * entries, 0.4 * entries)


def draw_vec_moment(key, part):
    return signed_moment(key, vec_grad_scales())


def draw_vec_second(key, part):
    return square_moment(key, vec_grad_scales())


def shard_levels(key, dims, pieces, least, high):
    level = 1.0
    for axis_at, parts in pieces:
        heights = jax.random.uniform(jax.random.fold_in(jax.random.fold_in(key, 6), axis_at), (parts,), jnp.float32, least / len(pieces), high / len(pieces))
        level = level * jnp.repeat(jnp.exp(heights), dims[axis_at] // parts).reshape((-1,) + (1,) * (len(dims) - 1 - axis_at))
    return level


def bell_draw(own_key, dims, deviation, most, shards=(), kind=jnp.bfloat16):
    result = jax.random.normal(own_key, dims, jnp.float32) * deviation
    if len(shards) > 0:
        result = shard_levels(own_key, dims, shards, -0.22, 0.18) * result
    return jnp.clip(result, min=-most, max=most).astype(kind)


def setup_inputs(seed: int = 0) -> dict:
    key_list = jax.random.split(jax.random.key(seed), 13)
    return {
        "tokens": bell_draw(key_list[0], (TOKENS, D), 1.0, 6.0, ((0, 32),)),
        "cotangent": bell_draw(key_list[1], (TOKENS, D), 1.0, 6.0, ((0, 32),)),
        "in_master": draw_in_master(jax.random.fold_in(key_list[12], 71), 0),
        "in_moment": draw_in_moment(jax.random.fold_in(key_list[12], 71), 0),
        "in_second": draw_in_second(jax.random.fold_in(key_list[12], 71), 0),
        "out_master": draw_out_master(jax.random.fold_in(key_list[12], 71), 0),
        "out_moment": draw_out_moment(jax.random.fold_in(key_list[12], 71), 0),
        "out_second": draw_out_second(jax.random.fold_in(key_list[12], 71), 0),
        "vec_master": draw_vec_master(jax.random.fold_in(key_list[12], 71), 0),
        "vec_moment": draw_vec_moment(jax.random.fold_in(key_list[12], 71), 0),
        "vec_second": draw_vec_second(jax.random.fold_in(key_list[12], 71), 0),
        "rotary_scale": jax.random.randint(key_list[11], (1,), 2, 9).astype(jnp.int32),
    }


@jax.custom_vjp
def low(v):
    return lax.optimization_barrier(v.astype(jnp.bfloat16)).astype(jnp.float32)

@jax.custom_vjp
def low_back(v):
    return v

def low_keep(v):
    return (low(v), None)

def low_pass(kept, grad):
    return (grad,)

def back_keep(v):
    return (v, None)

def back_low(kept, grad):
    return (low(grad),)
low.defvjp(low_keep, low_pass)
low_back.defvjp(back_keep, back_low)
neg_fill = -1e+30
matrix_rate = 0.03
vector_rate = 0.3
weight_decay = 0.1
adam_epsilon = 1e-08

def layer_norm(values, norm_gain, norm_shift):
    center = values - lax.optimization_barrier(jnp.mean(values, axis=-1, keepdims=True))
    return center * lax.rsqrt(lax.optimization_barrier(jnp.mean(center * center, axis=-1, keepdims=True)) + 1e-05) * norm_gain + norm_shift

def rotary_tables(positions, scale_value):
    half_rot = ROT // 2
    frequency = 10000.0 ** (-(2.0 * jnp.arange(half_rot, dtype=jnp.float32)) / ROT)
    angles = (positions / scale_value)[:, None] * frequency[None, :]
    return (jnp.cos(angles), jnp.sin(angles))

def rotate(values, cosine, sine_table):
    half_rot = ROT // 2
    front_half = values[..., :half_rot]
    back_half = values[..., half_rot:ROT]
    return jnp.concatenate([front_half * cosine - back_half * sine_table, back_half * cosine + front_half * sine_table, values[..., ROT:]], axis=-1)

def query_block(block_start, queries, key_rows, value_rows):
    row_block = lax.dynamic_slice_in_dim(queries, block_start, KEY_BLOCK, 0)
    scores = low_back(jnp.einsum('qhd,kd->qhk', row_block, key_rows, precision=lax.Precision.HIGHEST))
    row_pos = block_start + jnp.arange(KEY_BLOCK, dtype=jnp.int32)
    key_pos = jnp.arange(key_rows.shape[0], dtype=jnp.int32)
    allowed = key_pos[None, None, :] <= row_pos[:, None, None]
    scores = jnp.where(allowed, scores, neg_fill)
    run_max = lax.optimization_barrier(jnp.max(scores, axis=-1, keepdims=True))
    weights = jnp.exp(scores - run_max)
    probs = low(weights / lax.optimization_barrier(jnp.sum(weights, axis=-1, keepdims=True)))
    return jnp.einsum('qhk,kd->qhd', probs, value_rows, precision=lax.Precision.HIGHEST)

def attention(queries, key_rows, value_rows):
    length = queries.shape[0]
    starts = jnp.arange(length // KEY_BLOCK, dtype=jnp.int32) * KEY_BLOCK
    checked = jax.checkpoint(query_block)
    blocks = lax.map(lambda block_start: checked(block_start, queries, key_rows, value_rows), starts)
    return blocks.reshape(length, HEADS * HEAD_DIM)

def one_sequence(seq_tokens, weights_in, weights_out, vectors, cosine, sine_table):
    norm_one = low(layer_norm(seq_tokens, vectors[0:D], vectors[D:2 * D]))
    norm_two = low(layer_norm(seq_tokens, vectors[2 * D:3 * D], vectors[3 * D:4 * D]))
    queries = low_back(jnp.dot(norm_one, weights_in[:, :D], precision=lax.Precision.HIGHEST) + vectors[5 * D:6 * D])
    shared = low_back(jnp.dot(norm_one, weights_in[:, D:D + 2 * HEAD_DIM], precision=lax.Precision.HIGHEST) + vectors[6 * D:6 * D + 2 * HEAD_DIM])
    hidden_in = low_back(jnp.dot(norm_two, weights_in[:, D + 2 * HEAD_DIM:], precision=lax.Precision.HIGHEST) + vectors[6 * D + 2 * HEAD_DIM:])
    length = seq_tokens.shape[0]
    query_heads = queries.reshape(length, HEADS, HEAD_DIM)
    rotated = low(rotate(query_heads, cosine[:, None, :], sine_table[:, None, :]) * 0.125)
    key_rows = low(rotate(shared[:, :HEAD_DIM], cosine, sine_table))
    value_rows = low(shared[:, HEAD_DIM:])
    mixed_heads = attention(rotated, key_rows, value_rows)
    branch = low(low_back(mixed_heads))
    activated = low(jax.nn.gelu(hidden_in, approximate=False))
    branch_pair = jnp.concatenate([branch, activated], axis=1)
    return seq_tokens + jnp.dot(branch_pair, weights_out, precision=lax.Precision.HIGHEST) + vectors[4 * D:5 * D]

def adam_update(master, moment, second, gradient, step_rate, decay_rate):
    moment_new = 0.5 * moment + 0.5 * gradient
    second_new = 0.5 * second + 0.5 * gradient * gradient
    correction = 1.0 - 0.5 ** ADAM_STEP
    normalized = moment_new / correction / (jnp.sqrt(second_new / correction) + adam_epsilon)
    return (moment_new, second_new, master - step_rate * (normalized + decay_rate * master))

def reference(tokens, cotangent, in_master, in_moment, in_second, out_master, out_moment, out_second, vec_master, vec_moment, vec_second, rotary_scale):
    inputs = tokens.astype(jnp.float32)
    weights_in = lax.optimization_barrier(in_master.astype(jnp.bfloat16)).astype(jnp.float32)
    weights_out = lax.optimization_barrier(out_master.astype(jnp.bfloat16)).astype(jnp.float32)
    positions = jnp.arange(SEQ_LEN, dtype=jnp.int32).astype(jnp.float32)
    cosine, sine_table = rotary_tables(positions, rotary_scale[0].astype(jnp.float32))

    def forward(inputs, weights_in, weights_out, vectors):
        seq_blocks = inputs.reshape(TOKENS // SEQ_LEN, SEQ_LEN, D)

        def scan_step(state_now, seq_block):
            return (state_now, one_sequence(seq_block, weights_in, weights_out, vectors, cosine, sine_table))
        _, results = lax.scan(scan_step, jnp.zeros((), jnp.float32), seq_blocks)
        return results.reshape(TOKENS, D)
    output, pullback = jax.vjp(forward, inputs, weights_in, weights_out, vec_master)
    grad_tokens, grad_in, grad_out, grad_vec = pullback(cotangent.astype(jnp.float32))
    in_moment_new, in_second_new, in_master_new = adam_update(in_master, in_moment, in_second, grad_in, matrix_rate, weight_decay)
    out_moment_new, out_second_new, out_master_new = adam_update(out_master, out_moment, out_second, grad_out, matrix_rate, weight_decay)
    vec_moment_new, vec_second_new, vec_master_new = adam_update(vec_master, vec_moment, vec_second, grad_vec, vector_rate, 0.0)
    return (output.astype(jnp.bfloat16), grad_tokens.astype(jnp.bfloat16), in_moment_new, in_second_new, in_master_new, in_master_new.astype(jnp.bfloat16), out_moment_new, out_second_new, out_master_new, out_master_new.astype(jnp.bfloat16), vec_moment_new, vec_second_new, vec_master_new)
```

```python
import jax
import jax.numpy as jnp
from jax import lax
from jax.experimental import pallas as pl
from jax.experimental.pallas import tpu as pltpu
from jax.sharding import PartitionSpec as P

HEADS = 12
HEAD_DIM = 64
ROT = 16
D = 768
KEY_BLOCK = 1024
ADAM_STEP = 3


neg_fill = -1e30
matrix_rate = 0.03
vector_rate = 0.3
weight_decay = 0.1
adam_epsilon = 1e-08
contract_rows = (((0,), (0,)), ((), ()))
contract_cols = (((1,), (1,)), ((), ()))


def layer_norm(values, norm_gain, norm_shift):
    center = values - jnp.mean(values, axis=-1, keepdims=True)
    inverse = lax.rsqrt(jnp.mean(center * center, axis=-1, keepdims=True) + 1e-05)
    normed = center * inverse
    return (normed * norm_gain + norm_shift, normed, inverse)


def norm_back(upstream, normed, inverse, norm_gain):
    scaled = upstream * norm_gain
    inside = (
        scaled
        - jnp.mean(scaled, axis=-1, keepdims=True)
        - normed * jnp.mean(scaled * normed, axis=-1, keepdims=True)
    )
    return (inverse * inside, jnp.sum(upstream * normed, axis=0), jnp.sum(upstream, axis=0))


def rotary_tables(positions, scale_value):
    half_rot = ROT // 2
    frequency = 10000.0 ** (-(2.0 * jnp.arange(half_rot, dtype=jnp.float32)) / ROT)
    angles = (positions / scale_value)[:, None] * frequency[None, :]
    return (jnp.cos(angles), jnp.sin(angles))


def rotate(values, cosine, sine_table):
    half_rot = ROT // 2
    front_half = values[..., :half_rot]
    back_half = values[..., half_rot:ROT]
    return jnp.concatenate(
        [
            front_half * cosine - back_half * sine_table,
            back_half * cosine + front_half * sine_table,
            values[..., ROT:],
        ],
        axis=-1,
    )


def score_block(query_rows, row_pos, whole_kv, block_index):
    key_block = lax.dynamic_slice_in_dim(whole_kv, block_index * KEY_BLOCK, KEY_BLOCK, 0)
    scores = lax.dot_general(
        query_rows, key_block[:, :HEAD_DIM], contract_cols, preferred_element_type=jnp.float32
    )
    key_pos = block_index * KEY_BLOCK + jnp.arange(KEY_BLOCK, dtype=jnp.int32)
    allowed = key_pos[None, :] <= row_pos[:, None]
    return (jnp.where(allowed, scores, neg_fill), allowed, key_block)


def log_totals(query_rows, row_pos, whole_kv):
    row_count = query_rows.shape[0]
    last_pos = jnp.max(row_pos)

    def advance(block_index, state_now):

        def process(state_old):
            run_max, run_sum = state_old
            scores, allowed, key_block = score_block(query_rows, row_pos, whole_kv, block_index)
            new_max = jnp.maximum(run_max, jnp.max(scores, axis=1))
            weights = jnp.where(allowed, jnp.exp(scores - new_max[:, None]), 0.0)
            return (new_max, run_sum * jnp.exp(run_max - new_max) + jnp.sum(weights, axis=1))

        return lax.cond(
            block_index * KEY_BLOCK <= last_pos, process, lambda state_same: state_same, state_now
        )

    start_state = (
        jnp.full((row_count,), neg_fill, jnp.float32),
        jnp.zeros((row_count,), jnp.float32),
    )
    run_max, run_sum = lax.fori_loop(0, whole_kv.shape[0] // KEY_BLOCK, advance, start_state)
    return run_max + jnp.log(run_sum)


def attend(query_rows, row_pos, whole_kv, log_sum):
    last_pos = jnp.max(row_pos)

    def advance(block_index, summed):

        def process(summed_old):
            scores, allowed, key_block = score_block(query_rows, row_pos, whole_kv, block_index)
            probs = jnp.where(allowed, jnp.exp(scores - log_sum[:, None]), 0.0).astype(jnp.bfloat16)
            return summed_old + jnp.dot(
                probs, key_block[:, HEAD_DIM:], preferred_element_type=jnp.float32
            )

        return lax.cond(
            block_index * KEY_BLOCK <= last_pos, process, lambda summed_same: summed_same, summed
        )

    start_state = jnp.zeros((query_rows.shape[0], HEAD_DIM), jnp.float32)
    return lax.fori_loop(0, whole_kv.shape[0] // KEY_BLOCK, advance, start_state)


def attend_back(query_rows, row_pos, whole_kv, log_sum, grad_rows, row_inner):
    last_pos = jnp.max(row_pos)

    def advance(block_index, state_now):

        def process(state_old):
            query_grad, kv_terms = state_old
            scores, allowed, key_block = score_block(query_rows, row_pos, whole_kv, block_index)
            probs = jnp.where(allowed, jnp.exp(scores - log_sum[:, None]), 0.0)
            prob_grad = lax.dot_general(
                grad_rows,
                key_block[:, HEAD_DIM:],
                contract_cols,
                preferred_element_type=jnp.float32,
            )
            score_grad = (probs * (prob_grad - row_inner[:, None])).astype(jnp.bfloat16)
            query_grad = query_grad + jnp.dot(
                score_grad, key_block[:, :HEAD_DIM], preferred_element_type=jnp.float32
            )
            key_grad = lax.dot_general(
                score_grad, query_rows, contract_rows, preferred_element_type=jnp.float32
            )
            value_grad = lax.dot_general(
                probs.astype(jnp.bfloat16),
                grad_rows,
                contract_rows,
                preferred_element_type=jnp.float32,
            )
            kv_terms = lax.dynamic_update_slice_in_dim(
                kv_terms,
                jnp.concatenate([key_grad, value_grad], axis=1),
                block_index * KEY_BLOCK,
                0,
            )
            return (query_grad, kv_terms)

        return lax.cond(
            block_index * KEY_BLOCK <= last_pos, process, lambda state_same: state_same, state_now
        )

    start_state = (
        jnp.zeros((query_rows.shape[0], HEAD_DIM), jnp.float32),
        jnp.zeros((whole_kv.shape[0], 2 * HEAD_DIM), jnp.float32),
    )
    return lax.fori_loop(0, whole_kv.shape[0] // KEY_BLOCK, advance, start_state)


def adam_update(master, moment, second, gradient, step_rate, decay_rate):
    moment_new = 0.5 * moment + 0.5 * gradient
    second_new = 0.5 * second + 0.5 * gradient * gradient
    correction = 1.0 - 0.5**ADAM_STEP
    normalized = moment_new / correction / (jnp.sqrt(second_new / correction) + adam_epsilon)
    return (moment_new, second_new, master - step_rate * (normalized + decay_rate * master))


def shards(
    tokens,
    cotangent,
    in_master,
    in_moment,
    in_second,
    out_master,
    out_moment,
    out_second,
    vec_master,
    vec_moment,
    vec_second,
    rotary_scale,
):
    local_rows = tokens.shape[0]
    full_in, full_out = (
        lax.all_gather(in_master.astype(jnp.bfloat16), "head", axis=0, tiled=True),
        lax.all_gather(out_master.astype(jnp.bfloat16), "head", axis=0, tiled=True),
    )
    scale_value = rotary_scale[0].astype(jnp.float32)
    local_pos = lax.axis_index(("head", "ctx")) * local_rows + jnp.arange(
        local_rows, dtype=jnp.int32
    )
    cosine, sine_table = rotary_tables(local_pos.astype(jnp.float32), scale_value)
    inputs = tokens.astype(jnp.float32)
    norm_one, normed_one, inverse_one = layer_norm(inputs, vec_master[0:D], vec_master[D : 2 * D])
    norm_two, normed_two, inverse_two = layer_norm(
        inputs, vec_master[2 * D : 3 * D], vec_master[3 * D : 4 * D]
    )
    first_in = norm_one.astype(jnp.bfloat16)
    second_in = norm_two.astype(jnp.bfloat16)
    projected = (
        jnp.dot(first_in, full_in[:, : D + 2 * HEAD_DIM], preferred_element_type=jnp.float32)
        + vec_master[5 * D : 6 * D + 2 * HEAD_DIM]
    )
    hidden_in = (
        jnp.dot(second_in, full_in[:, D + 2 * HEAD_DIM :], preferred_element_type=jnp.float32)
        + vec_master[6 * D + 2 * HEAD_DIM :]
    )
    query_heads = projected[:, :D].reshape(local_rows, HEADS, HEAD_DIM)
    queries = (
        (rotate(query_heads, cosine[:, None, :], sine_table[:, None, :]) * 0.125)
        .astype(jnp.bfloat16)
        .reshape(local_rows, D)
    )
    key_part = rotate(projected[:, D : D + HEAD_DIM], cosine, sine_table)
    shared = jnp.concatenate([key_part, projected[:, D + HEAD_DIM :]], axis=1).astype(jnp.bfloat16)
    whole_kv = lax.all_gather(shared, ("head", "ctx"), axis=0, tiled=True)
    activated = jax.nn.gelu(hidden_in, approximate=False).astype(jnp.bfloat16)
    heads_here = queries.shape[1] // HEAD_DIM
    query_rows = queries.reshape(-1, HEAD_DIM)
    row_pos = jnp.repeat(local_pos, heads_here)
    log_sum = log_totals(query_rows, row_pos, whole_kv)
    attended = attend(query_rows, row_pos, whole_kv, log_sum)
    att_out = attended.reshape(queries.shape).astype(jnp.bfloat16)
    branch_pair = jnp.concatenate([att_out, activated], axis=1)
    output = (
        inputs
        + jnp.dot(branch_pair, full_out, preferred_element_type=jnp.float32)
        + vec_master[4 * D : 5 * D]
    ).astype(jnp.bfloat16)
    cot_in = cotangent.astype(jnp.float32)
    grad_out = lax.dot_general(
        branch_pair, cotangent, contract_rows, preferred_element_type=jnp.float32
    )
    back_proj = lax.dot_general(
        cotangent, full_out, contract_cols, preferred_element_type=jnp.float32
    )
    branch_grad = back_proj[:, :D].astype(jnp.bfloat16)
    gelu_back = jax.vjp(lambda pre_act: jax.nn.gelu(pre_act, approximate=False), hidden_in)[1]
    hidden_grad = gelu_back(back_proj[:, D:])[0].astype(jnp.bfloat16)
    grad_rows = branch_grad.reshape(-1, HEAD_DIM)
    row_inner = jnp.sum(grad_rows.astype(jnp.float32) * attended, axis=1)
    query_grad, kv_terms = attend_back(query_rows, row_pos, whole_kv, log_sum, grad_rows, row_inner)
    att_cos, att_sin = rotary_tables(local_pos.astype(jnp.float32), scale_value)
    query_pre = rotate(
        query_grad.reshape(-1, heads_here, HEAD_DIM) * 0.125,
        att_cos[:, None, :],
        -att_sin[:, None, :],
    )
    query_pre = query_pre.reshape(queries.shape).astype(jnp.bfloat16)
    kv_sum = lax.psum_scatter(kv_terms, ("head", "ctx"), scatter_dimension=0, tiled=True)
    shared_grad = jnp.concatenate(
        [rotate(kv_sum[:, :HEAD_DIM], cosine, -sine_table), kv_sum[:, HEAD_DIM:]], axis=1
    ).astype(jnp.bfloat16)
    attn_grad = jnp.concatenate([query_pre, shared_grad], axis=1)
    grad_in = jnp.concatenate(
        [
            lax.dot_general(first_in, attn_grad, contract_rows, preferred_element_type=jnp.float32),
            lax.dot_general(
                second_in, hidden_grad, contract_rows, preferred_element_type=jnp.float32
            ),
        ],
        axis=1,
    )
    norm_grad_one = lax.dot_general(
        attn_grad, full_in[:, : D + 2 * HEAD_DIM], contract_cols, preferred_element_type=jnp.float32
    )
    norm_grad_two = lax.dot_general(
        hidden_grad,
        full_in[:, D + 2 * HEAD_DIM :],
        contract_cols,
        preferred_element_type=jnp.float32,
    )
    input_one, gain_one, shift_one = norm_back(
        norm_grad_one, normed_one, inverse_one, vec_master[0:D]
    )
    input_two, gain_two, shift_two = norm_back(
        norm_grad_two, normed_two, inverse_two, vec_master[2 * D : 3 * D]
    )
    input_grad = (cot_in + input_one + input_two).astype(jnp.bfloat16)
    grad_vec = jnp.concatenate(
        [
            gain_one,
            shift_one,
            gain_two,
            shift_two,
            jnp.sum(cot_in, axis=0),
            jnp.sum(attn_grad.astype(jnp.float32), axis=0),
            jnp.sum(hidden_grad.astype(jnp.float32), axis=0),
        ]
    )
    shard_in, shard_out = (
        lax.psum_scatter(
            grad_in.astype(jnp.bfloat16), "head", scatter_dimension=0, tiled=True
        ).astype(jnp.float32),
        lax.psum_scatter(
            grad_out.astype(jnp.bfloat16), "head", scatter_dimension=0, tiled=True
        ).astype(jnp.float32),
    )
    summed_in, summed_out = lax.psum((shard_in, shard_out), ("dp", "ctx"))
    summed_vec = lax.psum(grad_vec, ("dp", "head", "ctx"))
    in_moment_new, in_second_new, in_master_new = adam_update(
        in_master, in_moment, in_second, summed_in, matrix_rate, weight_decay
    )
    out_moment_new, out_second_new, out_master_new = adam_update(
        out_master, out_moment, out_second, summed_out, matrix_rate, weight_decay
    )
    vec_moment_new, vec_second_new, vec_master_new = adam_update(
        vec_master, vec_moment, vec_second, summed_vec, vector_rate, 0.0
    )
    return (
        output,
        input_grad,
        in_moment_new,
        in_second_new,
        in_master_new,
        in_master_new.astype(jnp.bfloat16),
        out_moment_new,
        out_second_new,
        out_master_new,
        out_master_new.astype(jnp.bfloat16),
        vec_moment_new,
        vec_second_new,
        vec_master_new,
    )


MESH = pl.DeviceIdType.MESH
F32 = jnp.float32
BF16 = jnp.bfloat16
HALF_HEADS = HEADS // 2
VMEM_LIMIT = 60 * 1024 * 1024
contract_plain = (((1,), (0,)), ((), ()))


def vmem_specs(count):
    return [pl.BlockSpec(memory_space=pltpu.VMEM)] * count


def places():
    z = lax.axis_index("head")
    q = lax.axis_index("dp")
    c = lax.axis_index("ctx")
    qx = lax.rem(q, 2)
    qy = q // 2
    return z, q, c, qx, qy, qy * 2 + 1 - qx, (1 - qy) * 2 + qx


def greet(partners):
    barrier = pltpu.get_barrier_semaphore()
    for partner in partners:
        pl.semaphore_signal(barrier, inc=1, device_id=partner, device_id_type=MESH)
    pl.semaphore_wait(barrier, len(partners))


def remote(source, target, send_sem, recv_sem, device):
    return pltpu.make_async_remote_copy(
        src_ref=source,
        dst_ref=target,
        send_sem=send_sem,
        recv_sem=recv_sem,
        device_id=device,
        device_id_type=MESH,
    )


def gather_kernel(
    win, wout, tok, cot, all_in, all_out, all_tok, all_cot, send_sem, recv_sem, pair_send, pair_recv, local_sem
):
    z, q, c, qx, qy, xn, yn = places()
    dg = (1 - qy) * 2 + 1 - qx
    greet(
        [(q, lax.rem(z + k, 4), c) for k in (1, 2, 3)]
        + [(xn, z, c), (yn, z, c), (q, z, 1 - c)]
    )
    groups = ((0, 0, 512), (1, 0, 768), (0, 512, 2048))
    own = (win, wout)
    full = (all_in, all_out)

    def span(group, part):
        which, first, last = groups[group]
        middle = (first + last) // 2
        if part == 1:
            return which, pl.ds(first, middle - first)
        if part == 2:
            return which, pl.ds(middle, last - middle)
        return which, pl.ds(first, last - first)

    def place(group, part, plane, quarter):
        which, cols = span(group, part)
        return full[which].at[plane, quarter, :, cols]

    copies = []
    for number, (source, target) in enumerate(((tok, all_tok), (cot, all_cot))):
        copy = remote(source, target.at[c], pair_send.at[number], pair_recv.at[number], (q, z, 1 - c))
        copy.start()
        copies.append(copy)
    steps = [(group, k) for group in range(3) for k in (1, 2, 3)]
    for number, (group, k) in enumerate(steps):
        which, cols = span(group, 0)
        copy = remote(
            own[which].at[q, :, cols],
            place(group, 0, z, q),
            send_sem.at[0, number],
            recv_sem.at[0, number],
            (q, lax.rem(z + k, 4), c),
        )
        copy.start()
        copies.append(copy)
    locals_ = [
        pltpu.make_async_copy(win, all_in.at[z], local_sem.at[0]),
        pltpu.make_async_copy(wout, all_out.at[z], local_sem.at[1]),
        pltpu.make_async_copy(tok, all_tok.at[c], local_sem.at[2]),
        pltpu.make_async_copy(cot, all_cot.at[c], local_sem.at[3]),
    ]
    for copy in locals_:
        copy.start()

    def landed(path, number, target):
        remote(target, target, send_sem.at[path, number], recv_sem.at[path, number], (q, z, c)).wait_recv()

    def spread(number):
        group, k = steps[number]
        plane = lax.rem(z + 4 - k, 4)
        landed(0, number, place(group, 0, plane, q))
        for path, device in ((1, (xn, z, c)), (2, (yn, z, c))):
            piece = place(group, 0, plane, q)
            copy = remote(piece, piece, send_sem.at[path, number], recv_sem.at[path, number], device)
            copy.start()
            copies.append(copy)

    def relay(number):
        group, k = steps[number]
        plane = lax.rem(z + 4 - k, 4)
        landed(1, number, place(group, 0, plane, xn))
        piece = place(group, 1, plane, xn)
        copy = remote(piece, piece, send_sem.at[3, number], recv_sem.at[3, number], (yn, z, c))
        copy.start()
        copies.append(copy)
        landed(2, number, place(group, 0, plane, yn))
        piece = place(group, 2, plane, yn)
        copy = remote(piece, piece, send_sem.at[4, number], recv_sem.at[4, number], (xn, z, c))
        copy.start()
        copies.append(copy)

    for number in range(len(steps)):
        spread(number)
        if number > 0:
            relay(number - 1)
    relay(len(steps) - 1)
    for number, (group, k) in enumerate(steps):
        plane = lax.rem(z + 4 - k, 4)
        landed(3, number, place(group, 1, plane, dg))
        landed(4, number, place(group, 2, plane, dg))
    for number, target in enumerate((all_tok, all_cot)):
        remote(
            target.at[1 - c], target.at[1 - c], pair_send.at[number], pair_recv.at[number], (q, z, 1 - c)
        ).wait_recv()
    for copy in copies:
        copy.wait_send()
    for copy in locals_:
        copy.wait()


def gather_weights(win, wout, tok, cot):
    rows_in, cols_in = win.shape[1:]
    rows_out, cols_out = wout.shape[1:]
    rows, width = tok.shape
    return pl.pallas_call(
        gather_kernel,
        out_shape=(
            jax.ShapeDtypeStruct((4, 4, rows_in, cols_in), BF16),
            jax.ShapeDtypeStruct((4, 4, rows_out, cols_out), BF16),
            jax.ShapeDtypeStruct((2, rows, width), BF16),
            jax.ShapeDtypeStruct((2, rows, width), BF16),
        ),
        in_specs=vmem_specs(4),
        out_specs=vmem_specs(4),
        scratch_shapes=[
            pltpu.SemaphoreType.DMA((5, 9)),
            pltpu.SemaphoreType.DMA((5, 9)),
            pltpu.SemaphoreType.DMA((2,)),
            pltpu.SemaphoreType.DMA((2,)),
            pltpu.SemaphoreType.DMA((4,)),
        ],
        compiler_params=pltpu.CompilerParams(
            collective_id=0, has_side_effects=True, vmem_limit_bytes=VMEM_LIMIT
        ),
        name="gather_weights",
    )(win, wout, tok, cot)


BLOCK = 256


def attention_kernel(
    q_ref,
    g_ref,
    kv_ref,
    att_ref,
    dq_ref,
    dkv_ref,
    kv_all,
    keys,
    values,
    keys_t,
    values_t,
    scores,
    probs,
    dkeys,
    dvalues,
    packed,
    pair_in,
    summed,
    zone,
    send_sem,
    recv_sem,
    local_sem,
):
    z, q, c, qx, qy, xn, yn = places()
    greet([(q, lax.rem(z + k, 4), c) for k in (1, 2, 3)] + [(q, z, 1 - c)])
    for k in (1, 2, 3):

        @pl.when(z + k < 4)
        def _():
            remote(
                kv_ref, kv_all.at[z], send_sem.at[0, k], recv_sem.at[0, k], (q, lax.rem(z + k, 4), c)
            ).start()

    dkeys[...] = jnp.zeros_like(dkeys)
    dvalues[...] = jnp.zeros_like(dvalues)

    def spread_block(block, index):
        rows = pl.ds(pl.multiple_of(index * 512, 512), 512)
        keys[rows, :] = block[:, :HEAD_DIM]
        values[rows, :] = block[:, HEAD_DIM:]
        turned = block.astype(F32).T.astype(BF16)
        keys_t[:, rows] = turned[:HEAD_DIM]
        values_t[:, rows] = turned[HEAD_DIM:]

    spread_block(kv_ref[...], z)
    for k in (1, 2, 3):

        @pl.when(z - k >= 0)
        def _():
            source = lax.rem(z + 4 - k, 4)
            remote(
                kv_ref, kv_all.at[source], send_sem.at[0, k], recv_sem.at[0, k], (q, z, c)
            ).wait_recv()
            spread_block(kv_all[source], source)

    def one(step, carry):
        head = step // 2
        half = lax.rem(step, 2)
        dims = pl.ds(pl.multiple_of(head * HEAD_DIM, HEAD_DIM), HEAD_DIM)
        cols = pl.ds(pl.multiple_of(half * BLOCK, BLOCK), BLOCK)
        queries = q_ref[dims, cols]
        grads = g_ref[dims, cols]
        count = 2 * z + 1 + half
        key_place = lax.broadcasted_iota(jnp.int32, (BLOCK, BLOCK), 0)
        row_place = lax.broadcasted_iota(jnp.int32, (BLOCK, BLOCK), 1)

        def rows_at(index):
            return pl.ds(pl.multiple_of(index * BLOCK, BLOCK), BLOCK)

        def score(index, top):
            rows = rows_at(index)
            part = jnp.dot(keys[rows, :], queries, preferred_element_type=F32)
            hidden = (index - (count - 1)) * BLOCK + key_place > row_place
            part = jnp.where(hidden, neg_fill, part)
            scores[rows, :] = part
            return jnp.maximum(top, jnp.max(part, axis=0, keepdims=True))

        top = lax.fori_loop(0, count, score, jnp.full((1, BLOCK), neg_fill, F32))

        def weigh(index, total):
            rows = rows_at(index)
            part = jnp.exp(scores[rows, :] - top)
            scores[rows, :] = part
            return total + jnp.sum(part, axis=0, keepdims=True)

        total = lax.fori_loop(0, count, weigh, jnp.zeros((1, BLOCK), F32))
        inverse = 1.0 / total

        def attend_block(index, out):
            rows = rows_at(index)
            part = scores[rows, :] * inverse
            scores[rows, :] = part
            rounded = part.astype(BF16)
            probs[rows, :] = rounded
            return out + jnp.dot(values_t[:, rows], rounded, preferred_element_type=F32)

        out = lax.fori_loop(0, count, attend_block, jnp.zeros((HEAD_DIM, BLOCK), F32))
        att_ref[dims, cols] = out.astype(BF16)
        inner = jnp.sum(grads.astype(F32) * out, axis=0, keepdims=True)

        def back(index, dq):
            rows = rows_at(index)
            grad = jnp.dot(values[rows, :], grads, preferred_element_type=F32)
            dscore = (scores[rows, :] * (grad - inner)).astype(BF16)
            dkeys[rows, :] += lax.dot_general(
                dscore, queries, contract_cols, preferred_element_type=F32
            )
            dvalues[rows, :] += lax.dot_general(
                probs[rows, :], grads, contract_cols, preferred_element_type=F32
            )
            return dq + jnp.dot(keys_t[:, rows], dscore, preferred_element_type=F32)

        dq_ref[dims, cols] = lax.fori_loop(0, count, back, jnp.zeros((HEAD_DIM, BLOCK), F32))
        return carry

    lax.fori_loop(0, 2 * HALF_HEADS, one, 0)

    for index in range(4):
        rows = pl.ds(index * 512, 512)
        packed[index] = jnp.concatenate([dkeys[rows, :], dvalues[rows, :]], axis=1)
    mine = pl.ds(pl.multiple_of(c * 256, 256), 256)
    other = pl.ds(pl.multiple_of((1 - c) * 256, 256), 256)
    pair = remote(
        packed.at[:, other, :], pair_in, send_sem.at[1, 0], recv_sem.at[1, 0], (q, z, 1 - c)
    )
    pair.start()
    pair.wait_recv()
    for index in range(4):
        summed[index] = packed[index, mine, :] + pair_in[index]
    for k in (1, 2, 3):

        @pl.when(z - k >= 0)
        def _():
            target = lax.rem(z + 4 - k, 4)
            remote(
                summed.at[target], zone.at[k - 1], send_sem.at[2, k], recv_sem.at[2, k], (q, target, c)
            ).start()

    dkv_ref[mine, :] = summed[z]
    for k in (1, 2, 3):

        @pl.when(z + k < 4)
        def _():
            remote(
                zone.at[k - 1], zone.at[k - 1], send_sem.at[2, k], recv_sem.at[2, k], (q, z, c)
            ).wait_recv()
            dkv_ref[mine, :] += zone[k - 1]

    last = remote(
        dkv_ref.at[mine, :], dkv_ref.at[mine, :], send_sem.at[1, 1], recv_sem.at[1, 1], (q, z, 1 - c)
    )
    last.start()
    remote(
        dkv_ref.at[other, :], dkv_ref.at[other, :], send_sem.at[1, 1], recv_sem.at[1, 1], (q, z, 1 - c)
    ).wait_recv()
    last.wait_send()
    pair.wait_send()
    for k in (1, 2, 3):

        @pl.when(z + k < 4)
        def _():
            remote(
                kv_ref, kv_all.at[z], send_sem.at[0, k], recv_sem.at[0, k], (q, lax.rem(z + k, 4), c)
            ).wait_send()

        @pl.when(z - k >= 0)
        def _():
            target = lax.rem(z + 4 - k, 4)
            remote(
                summed.at[target], zone.at[k - 1], send_sem.at[2, k], recv_sem.at[2, k], (q, target, c)
            ).wait_send()


def attention(queries_t, grads_t, own_kv):
    dims, rows = queries_t.shape
    whole = 4 * rows
    return pl.pallas_call(
        attention_kernel,
        out_shape=(
            jax.ShapeDtypeStruct((dims, rows), BF16),
            jax.ShapeDtypeStruct((dims, rows), F32),
            jax.ShapeDtypeStruct((rows, 2 * HEAD_DIM), F32),
        ),
        in_specs=vmem_specs(3),
        out_specs=vmem_specs(3),
        scratch_shapes=[
            pltpu.VMEM((4, rows, 2 * HEAD_DIM), BF16),
            pltpu.VMEM((whole, HEAD_DIM), BF16),
            pltpu.VMEM((whole, HEAD_DIM), BF16),
            pltpu.VMEM((HEAD_DIM, whole), BF16),
            pltpu.VMEM((HEAD_DIM, whole), BF16),
            pltpu.VMEM((whole, BLOCK), F32),
            pltpu.VMEM((whole, BLOCK), BF16),
            pltpu.VMEM((whole, HEAD_DIM), F32),
            pltpu.VMEM((whole, HEAD_DIM), F32),
            pltpu.VMEM((4, rows, 2 * HEAD_DIM), F32),
            pltpu.VMEM((4, rows // 2, 2 * HEAD_DIM), F32),
            pltpu.VMEM((4, rows // 2, 2 * HEAD_DIM), F32),
            pltpu.VMEM((3, rows // 2, 2 * HEAD_DIM), F32),
            pltpu.SemaphoreType.DMA((3, 4)),
            pltpu.SemaphoreType.DMA((3, 4)),
            pltpu.SemaphoreType.DMA((2,)),
        ],
        compiler_params=pltpu.CompilerParams(
            collective_id=1, has_side_effects=True, vmem_limit_bytes=VMEM_LIMIT
        ),
        name="attention",
    )(queries_t, grads_t, own_kv)


PLANE_ORDER = (2, 1, 3, 0)


def reduce_kernel(
    g_in,
    g_out,
    vec,
    all_in,
    all_out,
    vec_sum,
    x_in,
    x_out,
    y_in,
    y_out,
    ax_in,
    ax_out,
    ay_in,
    ay_out,
    bx_in,
    bx_out,
    by_in,
    by_out,
    t_in,
    t_out,
    z_in,
    z_out,
    own_in,
    own_out,
    vec_send,
    vec_recv,
    vec_zone,
    send_sem,
    recv_sem,
    vec_send_sem,
    vec_recv_sem,
    last_send_sem,
    last_recv_sem,
    pair_send_sem,
    pair_recv_sem,
):
    z, q, c, qx, qy, xn, yn = places()
    dg = (1 - qy) * 2 + 1 - qx
    to_x, to_y, to_pair = (xn, z, c), (yn, z, c), (q, z, 1 - c)
    greet([(q, lax.rem(z + k, 4), c) for k in (1, 2, 3)] + [to_x, to_y, to_pair])
    sent = []

    def send(source, target, sems, index, device):
        copy = remote(source, target, sems[0].at[index], sems[1].at[index], device)
        copy.start()
        sent.append(copy)

    def landed(target, sems, index):
        remote(target, target, sems[0].at[index], sems[1].at[index], to_pair).wait_recv()

    main = (send_sem, recv_sem)
    vecs = (vec_send_sem, vec_recv_sem)
    lasts = (last_send_sem, last_recv_sem)
    pairs = (pair_send_sem, pair_recv_sem)
    grads = (g_in, g_out)
    halves = tuple(ref.shape[-1] // 2 for ref in grads)
    first = tuple(pl.ds(0, half) for half in halves)
    second = tuple(pl.ds(half, half) for half in halves)
    from_x, from_y = (x_in, x_out), (y_in, y_out)
    ax, ay, bx, by = (ax_in, ax_out), (ay_in, ay_out), (bx_in, bx_out), (by_in, by_out)
    totals, zones, own = (t_in, t_out), (z_in, z_out), (own_in, own_out)

    def plane(step):
        return lax.rem(z + PLANE_ORDER[step], 4)

    def exchange(step):
        h = plane(step)
        for a in range(2):
            send(grads[a].at[h, :, 1 - qx, :, first[a]], from_x[a].at[step], main, (step, 0, a), to_x)
            send(grads[a].at[h, 1 - qy, :, :, second[a]], from_y[a].at[step], main, (step, 1, a), to_y)

    def halve(step):
        h = plane(step)
        for a in range(2):
            landed(from_x[a].at[step], main, (step, 0, a))
            ax[a][step] = (
                grads[a][h, 1 - qy, qx, :, first[a]].astype(F32) + from_x[a][step, 1 - qy].astype(F32)
            ).astype(BF16)
            send(ax[a].at[step], ay[a].at[step], main, (step, 2, a), to_y)
            landed(from_y[a].at[step], main, (step, 1, a))
            bx[a][step] = (
                grads[a][h, qy, 1 - qx, :, second[a]].astype(F32) + from_y[a][step, 1 - qx].astype(F32)
            ).astype(BF16)
            send(bx[a].at[step], by[a].at[step], main, (step, 3, a), to_x)

    def finish(step):
        h = plane(step)
        shift = PLANE_ORDER[step]
        for a in range(2):
            landed(ay[a].at[step], main, (step, 2, a))
            left = (
                grads[a][h, qy, qx, :, first[a]].astype(F32)
                + from_x[a][step, qy].astype(F32)
                + ay[a][step].astype(F32)
            )
            landed(by[a].at[step], main, (step, 3, a))
            right = (
                grads[a][h, qy, qx, :, second[a]].astype(F32)
                + from_y[a][step, qx].astype(F32)
                + by[a][step].astype(F32)
            )
            if shift == 0:
                own[a][:, first[a]] = left
                own[a][:, second[a]] = right
            else:
                totals[a][shift - 1, :, first[a]] = left.astype(BF16)
                totals[a][shift - 1, :, second[a]] = right.astype(BF16)
                send(
                    totals[a].at[shift - 1],
                    zones[a].at[shift - 1],
                    main,
                    (step, 4, a),
                    (q, h, c),
                )

    send(vec, vec_recv.at[0], vecs, 0, to_x)
    exchange(0)
    exchange(1)
    for step in range(4):
        halve(step)
        if step + 2 < 4:
            exchange(step + 2)
        if step < 3:
            landed(vec_recv.at[step], vecs, step)
            have = vec[...] if step == 0 else vec_send[step - 1]
            vec_send[step] = have + vec_recv[step]
            if step < 2:
                send(vec_send.at[step], vec_recv.at[step + 1], vecs, step + 1, (to_y, to_pair)[step])
            else:
                for k in (1, 2, 3):
                    send(
                        vec_send.at[2], vec_zone.at[z], vecs, 2 + k, (q, lax.rem(z + k, 4), c)
                    )
                vec_zone[z] = vec_send[2]
        if step > 0:
            finish(step - 1)
    finish(3)
    for step in range(3):
        shift = PLANE_ORDER[step]
        for a in range(2):
            landed(zones[a].at[shift - 1], main, (step, 4, a))
    outs = (all_in, all_out)
    for a in range(2):
        whole = own[a][...] + zones[a][0].astype(F32) + zones[a][1].astype(F32) + zones[a][2].astype(F32)
        outs[a][c, q] = whole.astype(BF16)
        piece = outs[a].at[c, q]
        send(piece, piece, lasts, (0, a), to_x)
        send(piece, piece, lasts, (1, a), to_y)
        send(piece, piece, pairs, (0, a), to_pair)
    for a in range(2):
        piece = outs[a].at[c, xn]
        landed(piece, lasts, (0, a))
        part = outs[a].at[c, xn, :, first[a]]
        send(part, part, lasts, (2, a), to_y)
        send(piece, piece, pairs, (1, a), to_pair)
        piece = outs[a].at[c, yn]
        landed(piece, lasts, (1, a))
        part = outs[a].at[c, yn, :, second[a]]
        send(part, part, lasts, (3, a), to_x)
        send(piece, piece, pairs, (2, a), to_pair)
    for k in (1, 2, 3):
        landed(vec_zone.at[lax.rem(z + 4 - k, 4)], vecs, 2 + k)
    vec_sum[...] = (vec_zone[0] + vec_zone[1]) + (vec_zone[2] + vec_zone[3])
    for a in range(2):
        landed(outs[a].at[c, dg, :, first[a]], lasts, (2, a))
        landed(outs[a].at[c, dg, :, second[a]], lasts, (3, a))
        piece = outs[a].at[c, dg]
        send(piece, piece, pairs, (3, a), to_pair)
    for a in range(2):
        for index, quarter in enumerate((q, xn, yn, dg)):
            landed(outs[a].at[1 - c, quarter], pairs, (index, a))
    for copy in sent:
        copy.wait_send()


def reduce_grads(grad_in, grad_out, vec):
    rows_in, cols_in = grad_in.shape[3:]
    rows_out, cols_out = grad_out.shape[3:]

    def both(lead, cut, kind):
        return [
            pltpu.VMEM(lead + (rows_in, cols_in // cut), kind),
            pltpu.VMEM(lead + (rows_out, cols_out // cut), kind),
        ]

    return pl.pallas_call(
        reduce_kernel,
        out_shape=(
            jax.ShapeDtypeStruct((2, 4, rows_in, cols_in), BF16),
            jax.ShapeDtypeStruct((2, 4, rows_out, cols_out), BF16),
            jax.ShapeDtypeStruct(vec.shape, F32),
        ),
        in_specs=vmem_specs(3),
        out_specs=vmem_specs(3),
        scratch_shapes=both((4, 2), 2, BF16)
        + both((4, 2), 2, BF16)
        + both((4,), 2, BF16) * 4
        + both((3,), 1, BF16) * 2
        + both((), 1, F32)
        + [
            pltpu.VMEM((3,) + vec.shape, F32),
            pltpu.VMEM((3,) + vec.shape, F32),
            pltpu.VMEM((4,) + vec.shape, F32),
            pltpu.SemaphoreType.DMA((4, 5, 2)),
            pltpu.SemaphoreType.DMA((4, 5, 2)),
            pltpu.SemaphoreType.DMA((6,)),
            pltpu.SemaphoreType.DMA((6,)),
            pltpu.SemaphoreType.DMA((4, 2)),
            pltpu.SemaphoreType.DMA((4, 2)),
            pltpu.SemaphoreType.DMA((4, 2)),
            pltpu.SemaphoreType.DMA((4, 2)),
        ],
        compiler_params=pltpu.CompilerParams(
            collective_id=2, has_side_effects=True, vmem_limit_bytes=VMEM_LIMIT
        ),
        name="reduce_grads",
    )(grad_in, grad_out, vec)


KV_END = D + 2 * HEAD_DIM
HALF_D = D // 2


def hidden_spans(core, ff, row_share):
    spans = []
    for owner in range((D + ff) // row_share):
        first = max(owner * row_share - D, 0)
        last = (owner + 1) * row_share - D
        if last > first:
            half = (last - first) // 2
            spans.append((first + core * half, half))
    return spans


def core_columns(array, core, ff, row_share):
    pieces = [array[..., core * HALF_D : (core + 1) * HALF_D], array[..., D:KV_END]]
    pieces += [
        array[..., KV_END + first : KV_END + first + size]
        for first, size in hidden_spans(core, ff, row_share)
    ]
    return jnp.concatenate(pieces, axis=-1)


def join_columns(pair, ff, row_share):
    pieces = [pair[0][..., :HALF_D], pair[1][..., :HALF_D], pair[0][..., HALF_D : HALF_D + 2 * HEAD_DIM]]
    at = HALF_D + 2 * HEAD_DIM
    for _, size in hidden_spans(0, ff, row_share):
        pieces += [pair[0][..., at : at + size], pair[1][..., at : at + size]]
        at += size
    return jnp.concatenate(pieces, axis=-1)


def fast_shards(
    tokens,
    cotangent,
    in_master,
    in_moment,
    in_second,
    out_master,
    out_moment,
    out_second,
    vec_master,
    vec_moment,
    vec_second,
    rotary_scale,
):
    z = lax.axis_index("head")
    c = lax.axis_index("ctx")
    first_core = c == 0
    rows = tokens.shape[0]
    chip_rows = 2 * rows
    row_share = out_master.shape[0]
    ff = in_master.shape[1] - KV_END
    half_share = row_share // 2
    attn_share = D // 2

    def pick(array):
        return jnp.where(
            first_core, core_columns(array, 0, ff, row_share), core_columns(array, 1, ff, row_share)
        )

    win = pick(in_master.astype(BF16))
    out_low = out_master.astype(BF16)
    start_one = jnp.where(z == 0, attn_share * c, half_share * c)
    start_two = jnp.where(z == 0, D + (half_share - attn_share) * c, half_share * c + attn_share)
    wout = jnp.concatenate(
        [
            lax.dynamic_slice_in_dim(out_low, start_one, attn_share, 0),
            lax.dynamic_slice_in_dim(out_low, start_two, half_share - attn_share, 0),
        ],
        axis=0,
    )
    full_in, full_out, all_tok, all_cot = gather_weights(
        win.reshape(4, -1, win.shape[1]), wout.reshape(4, -1, D), tokens, cotangent
    )
    full_in = full_in.reshape(D, -1)
    full_out = full_out.reshape(-1, D)
    inputs = all_tok.reshape(chip_rows, D).astype(F32)
    cot = all_cot.reshape(chip_rows, D)
    attn_cols = HALF_D + 2 * HEAD_DIM

    gain_one, gain_two = vec_master[0:D], vec_master[2 * D : 3 * D]
    center = inputs - jnp.mean(inputs, axis=-1, keepdims=True)
    inverse = lax.rsqrt(jnp.mean(center * center, axis=-1, keepdims=True) + 1e-05)
    normed = center * inverse
    norm_one = (normed * gain_one + vec_master[D : 2 * D]).astype(BF16)
    norm_two = (normed * gain_two + vec_master[3 * D : 4 * D]).astype(BF16)
    bias = pick(vec_master[5 * D :])

    positions = z * chip_rows + jnp.arange(chip_rows, dtype=jnp.int32)
    cosine, sine_table = rotary_tables(
        positions.astype(F32), rotary_scale[0].astype(F32)
    )
    half_rot = ROT // 2
    cos_t, sin_t = cosine.T, sine_table.T

    def turn(values, sine):
        front, back = values[:, :half_rot], values[:, half_rot:ROT]
        return jnp.concatenate(
            [front * cos_t - back * sine, back * cos_t + front * sine, values[:, ROT:]], axis=1
        )

    projected = lax.dot_general(
        full_in[:, :HALF_D], norm_one, (((0,), (1,)), ((), ())), preferred_element_type=F32
    ) + bias[:HALF_D, None]
    queries_t = (
        (turn(projected.reshape(HALF_HEADS, HEAD_DIM, chip_rows), sin_t) * 0.125)
        .astype(BF16)
        .reshape(HALF_D, chip_rows)
    )
    shared = jnp.dot(norm_one, full_in[:, HALF_D:attn_cols], preferred_element_type=F32) + bias[
        HALF_D:attn_cols
    ]
    own_kv = jnp.concatenate(
        [rotate(shared[:, :HEAD_DIM], cosine, sine_table), shared[:, HEAD_DIM:]], axis=1
    ).astype(BF16)
    grads_t = lax.dot_general(
        full_out[:HALF_D], cot, contract_cols, preferred_element_type=F32
    ).astype(BF16)
    att_t, query_grad, kv_grad = attention(queries_t, grads_t, own_kv)

    hidden_in = jnp.dot(norm_two, full_in[:, attn_cols:], preferred_element_type=F32) + bias[attn_cols:]
    activated = jax.nn.gelu(hidden_in, approximate=False).astype(BF16)
    partial_out = lax.dot_general(
        att_t, full_out[:HALF_D], contract_rows, preferred_element_type=F32
    ) + jnp.dot(activated, full_out[HALF_D:], preferred_element_type=F32)
    back_hidden = lax.dot_general(cot, full_out[HALF_D:], contract_cols, preferred_element_type=F32)
    gelu_back = jax.vjp(lambda pre_act: jax.nn.gelu(pre_act, approximate=False), hidden_in)[1]
    hidden_grad = gelu_back(back_hidden)[0].astype(BF16)
    grad_out = jnp.concatenate(
        [
            jnp.dot(att_t, cot, preferred_element_type=F32).astype(BF16),
            lax.dot_general(activated, cot, contract_rows, preferred_element_type=F32).astype(BF16),
        ],
        axis=0,
    )
    query_pre = (
        turn(query_grad.reshape(HALF_HEADS, HEAD_DIM, chip_rows) * 0.125, -sin_t)
        .reshape(HALF_D, chip_rows)
        .astype(BF16)
    )
    shared_grad = jnp.concatenate(
        [rotate(kv_grad[:, :HEAD_DIM], cosine, -sine_table), kv_grad[:, HEAD_DIM:]], axis=1
    ).astype(BF16)
    shared_once = jnp.where(first_core, shared_grad, jnp.zeros_like(shared_grad))
    grad_in = jnp.concatenate(
        [
            lax.dot_general(
                norm_one, query_pre, (((0,), (1,)), ((), ())), preferred_element_type=F32
            ).astype(BF16),
            lax.dot_general(norm_one, shared_grad, contract_rows, preferred_element_type=F32).astype(BF16),
            lax.dot_general(norm_two, hidden_grad, contract_rows, preferred_element_type=F32).astype(BF16),
        ],
        axis=1,
    )
    norm_grad_one = lax.dot_general(
        query_pre, full_in[:, :HALF_D], (((0,), (1,)), ((), ())), preferred_element_type=F32
    ) + lax.dot_general(
        shared_once, full_in[:, HALF_D:attn_cols], contract_cols, preferred_element_type=F32
    )
    norm_grad_two = lax.dot_general(
        hidden_grad, full_in[:, attn_cols:], contract_cols, preferred_element_type=F32
    )
    upstream = norm_grad_one * gain_one + norm_grad_two * gain_two

    def mine(array):
        return lax.dynamic_slice_in_dim(array, c * rows, rows, 0)

    def swap(array):
        other = lax.dynamic_slice_in_dim(array, (1 - c) * rows, rows, 0)
        return mine(array) + lax.ppermute(other, "ctx", [(0, 1), (1, 0)])

    inputs_own = tokens.astype(F32)
    cot_own = cotangent.astype(F32)
    output = (inputs_own + swap(partial_out) + vec_master[4 * D : 5 * D]).astype(BF16)
    upstream_own = swap(upstream)
    normed_own = mine(normed)
    inside = (
        upstream_own
        - jnp.mean(upstream_own, axis=-1, keepdims=True)
        - normed_own * jnp.mean(upstream_own * normed_own, axis=-1, keepdims=True)
    )
    input_grad = (cot_own + mine(inverse) * inside).astype(BF16)

    column_sums = jnp.concatenate(
        [
            jnp.sum(query_pre.astype(F32), axis=1),
            jnp.sum(shared_once.astype(F32), axis=0),
            jnp.sum(hidden_grad.astype(F32), axis=0),
        ]
    )
    nothing = jnp.zeros_like(column_sums)
    placed_sums = join_columns(
        (jnp.where(first_core, column_sums, nothing), jnp.where(first_core, nothing, column_sums)),
        ff,
        row_share,
    )
    grad_vec = jnp.concatenate(
        [
            jnp.sum(norm_grad_one * normed, axis=0),
            jnp.sum(norm_grad_one, axis=0),
            jnp.sum(norm_grad_two * normed, axis=0),
            jnp.sum(norm_grad_two, axis=0),
            jnp.sum(cot_own, axis=0),
            placed_sums,
        ]
    )
    size = grad_vec.shape[0]
    lanes = -(-size // 1024) * 128
    padded = jnp.pad(grad_vec, (0, 8 * lanes - size)).reshape(8, lanes)
    sum_in, sum_out, sum_vec = reduce_grads(
        grad_in.reshape(4, 2, 2, -1, grad_in.shape[1]), grad_out.reshape(4, 2, 2, -1, D), padded
    )
    summed_vec = sum_vec.reshape(-1)[:size]
    sum_in = sum_in.reshape(2, -1, sum_in.shape[-1])
    summed_in = join_columns((sum_in[0], sum_in[1]), ff, row_share).astype(F32)
    low, high = sum_out.reshape(2, half_share, D)
    head_rows = jnp.concatenate([low[:attn_share], high[:attn_share], low[attn_share:], high[attn_share:]], axis=0)
    summed_out = jnp.where(z == 0, head_rows, jnp.concatenate([low, high], axis=0)).astype(F32)

    in_moment_new, in_second_new, in_master_new = adam_update(
        in_master, in_moment, in_second, summed_in, matrix_rate, weight_decay
    )
    out_moment_new, out_second_new, out_master_new = adam_update(
        out_master, out_moment, out_second, summed_out, matrix_rate, weight_decay
    )
    vec_moment_new, vec_second_new, vec_master_new = adam_update(
        vec_master, vec_moment, vec_second, summed_vec, vector_rate, 0.0
    )
    return (
        output,
        input_grad,
        in_moment_new,
        in_second_new,
        in_master_new,
        in_master_new.astype(BF16),
        out_moment_new,
        out_second_new,
        out_master_new,
        out_master_new.astype(BF16),
        vec_moment_new,
        vec_second_new,
        vec_master_new,
    )


def solution(mesh):
    placed = (
        P(("dp", "head", "ctx"), None),
        P(("dp", "head", "ctx"), None),
        P("head", None),
        P("head", None),
        P("head", None),
        P("head", None),
        P("head", None),
        P("head", None),
        P(),
        P(),
        P(),
        P(),
    )
    paired = dict(mesh.shape) == {"dp": 4, "head": 4, "ctx": 2}
    body = fast_shards if paired else shards
    return jax.shard_map(
        body,
        mesh=mesh,
        in_specs=placed,
        out_specs=(
            P(("dp", "head", "ctx"), None),
            P(("dp", "head", "ctx"), None),
            P("head", None),
            P("head", None),
            P("head", None),
            P("head", None),
            P("head", None),
            P("head", None),
            P("head", None),
            P("head", None),
            P(),
            P(),
            P(),
        ),
        check_vma=False,
    )
```

```python
import jax
import jax.numpy as jnp
from jax import lax
from jax.experimental import pallas as pl
from jax.experimental.pallas import tpu as pltpu
from jax.sharding import PartitionSpec as P

HEADS = 12
HEAD_DIM = 64
ROT = 16
D = 768
KEY_BLOCK = 1024
ADAM_STEP = 3


neg_fill = -1e30
matrix_rate = 0.03
vector_rate = 0.3
weight_decay = 0.1
adam_epsilon = 1e-08
contract_rows = (((0,), (0,)), ((), ()))
contract_cols = (((1,), (1,)), ((), ()))


def layer_norm(values, norm_gain, norm_shift):
    center = values - jnp.mean(values, axis=-1, keepdims=True)
    inverse = lax.rsqrt(jnp.mean(center * center, axis=-1, keepdims=True) + 1e-05)
    normed = center * inverse
    return (normed * norm_gain + norm_shift, normed, inverse)


def norm_back(upstream, normed, inverse, norm_gain):
    scaled = upstream * norm_gain
    inside = (
        scaled
        - jnp.mean(scaled, axis=-1, keepdims=True)
        - normed * jnp.mean(scaled * normed, axis=-1, keepdims=True)
    )
    return (inverse * inside, jnp.sum(upstream * normed, axis=0), jnp.sum(upstream, axis=0))


def rotary_tables(positions, scale_value):
    half_rot = ROT // 2
    frequency = 10000.0 ** (-(2.0 * jnp.arange(half_rot, dtype=jnp.float32)) / ROT)
    angles = (positions / scale_value)[:, None] * frequency[None, :]
    return (jnp.cos(angles), jnp.sin(angles))


def rotate(values, cosine, sine_table):
    half_rot = ROT // 2
    front_half = values[..., :half_rot]
    back_half = values[..., half_rot:ROT]
    return jnp.concatenate(
        [
            front_half * cosine - back_half * sine_table,
            back_half * cosine + front_half * sine_table,
            values[..., ROT:],
        ],
        axis=-1,
    )


def score_block(query_rows, row_pos, whole_kv, block_index):
    key_block = lax.dynamic_slice_in_dim(whole_kv, block_index * KEY_BLOCK, KEY_BLOCK, 0)
    scores = lax.dot_general(
        query_rows, key_block[:, :HEAD_DIM], contract_cols, preferred_element_type=jnp.float32
    )
    key_pos = block_index * KEY_BLOCK + jnp.arange(KEY_BLOCK, dtype=jnp.int32)
    allowed = key_pos[None, :] <= row_pos[:, None]
    return (jnp.where(allowed, scores, neg_fill), allowed, key_block)


def log_totals(query_rows, row_pos, whole_kv):
    row_count = query_rows.shape[0]
    last_pos = jnp.max(row_pos)

    def advance(block_index, state_now):

        def process(state_old):
            run_max, run_sum = state_old
            scores, allowed, key_block = score_block(query_rows, row_pos, whole_kv, block_index)
            new_max = jnp.maximum(run_max, jnp.max(scores, axis=1))
            weights = jnp.where(allowed, jnp.exp(scores - new_max[:, None]), 0.0)
            return (new_max, run_sum * jnp.exp(run_max - new_max) + jnp.sum(weights, axis=1))

        return lax.cond(
            block_index * KEY_BLOCK <= last_pos, process, lambda state_same: state_same, state_now
        )

    start_state = (
        jnp.full((row_count,), neg_fill, jnp.float32),
        jnp.zeros((row_count,), jnp.float32),
    )
    run_max, run_sum = lax.fori_loop(0, whole_kv.shape[0] // KEY_BLOCK, advance, start_state)
    return run_max + jnp.log(run_sum)


def attend(query_rows, row_pos, whole_kv, log_sum):
    last_pos = jnp.max(row_pos)

    def advance(block_index, summed):

        def process(summed_old):
            scores, allowed, key_block = score_block(query_rows, row_pos, whole_kv, block_index)
            probs = jnp.where(allowed, jnp.exp(scores - log_sum[:, None]), 0.0).astype(jnp.bfloat16)
            return summed_old + jnp.dot(
                probs, key_block[:, HEAD_DIM:], preferred_element_type=jnp.float32
            )

        return lax.cond(
            block_index * KEY_BLOCK <= last_pos, process, lambda summed_same: summed_same, summed
        )

    start_state = jnp.zeros((query_rows.shape[0], HEAD_DIM), jnp.float32)
    return lax.fori_loop(0, whole_kv.shape[0] // KEY_BLOCK, advance, start_state)


def attend_back(query_rows, row_pos, whole_kv, log_sum, grad_rows, row_inner):
    last_pos = jnp.max(row_pos)

    def advance(block_index, state_now):

        def process(state_old):
            query_grad, kv_terms = state_old
            scores, allowed, key_block = score_block(query_rows, row_pos, whole_kv, block_index)
            probs = jnp.where(allowed, jnp.exp(scores - log_sum[:, None]), 0.0)
            prob_grad = lax.dot_general(
                grad_rows,
                key_block[:, HEAD_DIM:],
                contract_cols,
                preferred_element_type=jnp.float32,
            )
            score_grad = (probs * (prob_grad - row_inner[:, None])).astype(jnp.bfloat16)
            query_grad = query_grad + jnp.dot(
                score_grad, key_block[:, :HEAD_DIM], preferred_element_type=jnp.float32
            )
            key_grad = lax.dot_general(
                score_grad, query_rows, contract_rows, preferred_element_type=jnp.float32
            )
            value_grad = lax.dot_general(
                probs.astype(jnp.bfloat16),
                grad_rows,
                contract_rows,
                preferred_element_type=jnp.float32,
            )
            kv_terms = lax.dynamic_update_slice_in_dim(
                kv_terms,
                jnp.concatenate([key_grad, value_grad], axis=1),
                block_index * KEY_BLOCK,
                0,
            )
            return (query_grad, kv_terms)

        return lax.cond(
            block_index * KEY_BLOCK <= last_pos, process, lambda state_same: state_same, state_now
        )

    start_state = (
        jnp.zeros((query_rows.shape[0], HEAD_DIM), jnp.float32),
        jnp.zeros((whole_kv.shape[0], 2 * HEAD_DIM), jnp.float32),
    )
    return lax.fori_loop(0, whole_kv.shape[0] // KEY_BLOCK, advance, start_state)


def adam_update(master, moment, second, gradient, step_rate, decay_rate):
    moment_new = 0.5 * moment + 0.5 * gradient
    second_new = 0.5 * second + 0.5 * gradient * gradient
    correction = 1.0 - 0.5**ADAM_STEP
    normalized = moment_new / correction / (jnp.sqrt(second_new / correction) + adam_epsilon)
    return (moment_new, second_new, master - step_rate * (normalized + decay_rate * master))


def shards(
    tokens,
    cotangent,
    in_master,
    in_moment,
    in_second,
    out_master,
    out_moment,
    out_second,
    vec_master,
    vec_moment,
    vec_second,
    rotary_scale,
):
    local_rows = tokens.shape[0]
    full_in, full_out = (
        lax.all_gather(in_master.astype(jnp.bfloat16), "head", axis=0, tiled=True),
        lax.all_gather(out_master.astype(jnp.bfloat16), "head", axis=0, tiled=True),
    )
    scale_value = rotary_scale[0].astype(jnp.float32)
    local_pos = lax.axis_index(("head", "ctx")) * local_rows + jnp.arange(
        local_rows, dtype=jnp.int32
    )
    cosine, sine_table = rotary_tables(local_pos.astype(jnp.float32), scale_value)
    inputs = tokens.astype(jnp.float32)
    norm_one, normed_one, inverse_one = layer_norm(inputs, vec_master[0:D], vec_master[D : 2 * D])
    norm_two, normed_two, inverse_two = layer_norm(
        inputs, vec_master[2 * D : 3 * D], vec_master[3 * D : 4 * D]
    )
    first_in = norm_one.astype(jnp.bfloat16)
    second_in = norm_two.astype(jnp.bfloat16)
    projected = (
        jnp.dot(first_in, full_in[:, : D + 2 * HEAD_DIM], preferred_element_type=jnp.float32)
        + vec_master[5 * D : 6 * D + 2 * HEAD_DIM]
    )
    hidden_in = (
        jnp.dot(second_in, full_in[:, D + 2 * HEAD_DIM :], preferred_element_type=jnp.float32)
        + vec_master[6 * D + 2 * HEAD_DIM :]
    )
    query_heads = projected[:, :D].reshape(local_rows, HEADS, HEAD_DIM)
    queries = (
        (rotate(query_heads, cosine[:, None, :], sine_table[:, None, :]) * 0.125)
        .astype(jnp.bfloat16)
        .reshape(local_rows, D)
    )
    key_part = rotate(projected[:, D : D + HEAD_DIM], cosine, sine_table)
    shared = jnp.concatenate([key_part, projected[:, D + HEAD_DIM :]], axis=1).astype(jnp.bfloat16)
    whole_kv = lax.all_gather(shared, ("head", "ctx"), axis=0, tiled=True)
    activated = jax.nn.gelu(hidden_in, approximate=False).astype(jnp.bfloat16)
    heads_here = queries.shape[1] // HEAD_DIM
    query_rows = queries.reshape(-1, HEAD_DIM)
    row_pos = jnp.repeat(local_pos, heads_here)
    log_sum = log_totals(query_rows, row_pos, whole_kv)
    attended = attend(query_rows, row_pos, whole_kv, log_sum)
    att_out = attended.reshape(queries.shape).astype(jnp.bfloat16)
    branch_pair = jnp.concatenate([att_out, activated], axis=1)
    output = (
        inputs
        + jnp.dot(branch_pair, full_out, preferred_element_type=jnp.float32)
        + vec_master[4 * D : 5 * D]
    ).astype(jnp.bfloat16)
    cot_in = cotangent.astype(jnp.float32)
    grad_out = lax.dot_general(
        branch_pair, cotangent, contract_rows, preferred_element_type=jnp.float32
    )
    back_proj = lax.dot_general(
        cotangent, full_out, contract_cols, preferred_element_type=jnp.float32
    )
    branch_grad = back_proj[:, :D].astype(jnp.bfloat16)
    gelu_back = jax.vjp(lambda pre_act: jax.nn.gelu(pre_act, approximate=False), hidden_in)[1]
    hidden_grad = gelu_back(back_proj[:, D:])[0].astype(jnp.bfloat16)
    grad_rows = branch_grad.reshape(-1, HEAD_DIM)
    row_inner = jnp.sum(grad_rows.astype(jnp.float32) * attended, axis=1)
    query_grad, kv_terms = attend_back(query_rows, row_pos, whole_kv, log_sum, grad_rows, row_inner)
    att_cos, att_sin = rotary_tables(local_pos.astype(jnp.float32), scale_value)
    query_pre = rotate(
        query_grad.reshape(-1, heads_here, HEAD_DIM) * 0.125,
        att_cos[:, None, :],
        -att_sin[:, None, :],
    )
    query_pre = query_pre.reshape(queries.shape).astype(jnp.bfloat16)
    kv_sum = lax.psum_scatter(kv_terms, ("head", "ctx"), scatter_dimension=0, tiled=True)
    shared_grad = jnp.concatenate(
        [rotate(kv_sum[:, :HEAD_DIM], cosine, -sine_table), kv_sum[:, HEAD_DIM:]], axis=1
    ).astype(jnp.bfloat16)
    attn_grad = jnp.concatenate([query_pre, shared_grad], axis=1)
    grad_in = jnp.concatenate(
        [
            lax.dot_general(first_in, attn_grad, contract_rows, preferred_element_type=jnp.float32),
            lax.dot_general(
                second_in, hidden_grad, contract_rows, preferred_element_type=jnp.float32
            ),
        ],
        axis=1,
    )
    norm_grad_one = lax.dot_general(
        attn_grad, full_in[:, : D + 2 * HEAD_DIM], contract_cols, preferred_element_type=jnp.float32
    )
    norm_grad_two = lax.dot_general(
        hidden_grad,
        full_in[:, D + 2 * HEAD_DIM :],
        contract_cols,
        preferred_element_type=jnp.float32,
    )
    input_one, gain_one, shift_one = norm_back(
        norm_grad_one, normed_one, inverse_one, vec_master[0:D]
    )
    input_two, gain_two, shift_two = norm_back(
        norm_grad_two, normed_two, inverse_two, vec_master[2 * D : 3 * D]
    )
    input_grad = (cot_in + input_one + input_two).astype(jnp.bfloat16)
    grad_vec = jnp.concatenate(
        [
            gain_one,
            shift_one,
            gain_two,
            shift_two,
            jnp.sum(cot_in, axis=0),
            jnp.sum(attn_grad.astype(jnp.float32), axis=0),
            jnp.sum(hidden_grad.astype(jnp.float32), axis=0),
        ]
    )
    shard_in, shard_out = (
        lax.psum_scatter(
            grad_in.astype(jnp.bfloat16), "head", scatter_dimension=0, tiled=True
        ).astype(jnp.float32),
        lax.psum_scatter(
            grad_out.astype(jnp.bfloat16), "head", scatter_dimension=0, tiled=True
        ).astype(jnp.float32),
    )
    summed_in, summed_out = lax.psum((shard_in, shard_out), ("dp", "ctx"))
    summed_vec = lax.psum(grad_vec, ("dp", "head", "ctx"))
    in_moment_new, in_second_new, in_master_new = adam_update(
        in_master, in_moment, in_second, summed_in, matrix_rate, weight_decay
    )
    out_moment_new, out_second_new, out_master_new = adam_update(
        out_master, out_moment, out_second, summed_out, matrix_rate, weight_decay
    )
    vec_moment_new, vec_second_new, vec_master_new = adam_update(
        vec_master, vec_moment, vec_second, summed_vec, vector_rate, 0.0
    )
    return (
        output,
        input_grad,
        in_moment_new,
        in_second_new,
        in_master_new,
        in_master_new.astype(jnp.bfloat16),
        out_moment_new,
        out_second_new,
        out_master_new,
        out_master_new.astype(jnp.bfloat16),
        vec_moment_new,
        vec_second_new,
        vec_master_new,
    )


MESH = pl.DeviceIdType.MESH
F32 = jnp.float32
BF16 = jnp.bfloat16
HALF_HEADS = HEADS // 2
VMEM_LIMIT = 60 * 1024 * 1024
BACK_LIMIT = 67000000


def vmem_specs(count):
    return [pl.BlockSpec(memory_space=pltpu.VMEM)] * count


def places():
    z = lax.axis_index("head")
    q = lax.axis_index("dp")
    c = lax.axis_index("ctx")
    qx = lax.rem(q, 2)
    qy = q // 2
    return z, q, c, qx, qy, qy * 2 + 1 - qx, (1 - qy) * 2 + qx


def greet(partners):
    barrier = pltpu.get_barrier_semaphore()
    for partner in partners:
        pl.semaphore_signal(barrier, inc=1, device_id=partner, device_id_type=MESH)
    pl.semaphore_wait(barrier, len(partners))


def remote(source, target, send_sem, recv_sem, device):
    return pltpu.make_async_remote_copy(
        src_ref=source,
        dst_ref=target,
        send_sem=send_sem,
        recv_sem=recv_sem,
        device_id=device,
        device_id_type=MESH,
    )


CHUNK = 512
IN_ROWS = 48
OUT_ROWS = 120


def front_kernel(
    win,
    wout,
    tok,
    cot,
    affine,
    bias,
    cos_ref,
    sin_ref,
    full_in,
    full_out,
    all_tok,
    all_cot,
    norm_one,
    norm_two,
    att_ref,
    dq_ref,
    dkv_ref,
    q_all,
    g_all,
    kv_all,
    keys,
    values,
    weights,
    tops,
    dkeys,
    dvalues,
    z_send,
    z_recv,
    xy_send,
    xy_recv,
    pair_send,
    pair_recv,
    kv_send,
    kv_recv,
    local_sem,
):
    z, q, c, qx, qy, xn, yn = places()
    dg = (1 - qy) * 2 + 1 - qx
    to_x, to_y, to_pair = (xn, z, c), (yn, z, c), (q, z, 1 - c)
    greet([(q, lax.rem(z + k, 4), c) for k in (1, 2, 3)] + [to_x, to_y, to_pair])
    attn_cols = HALF_D + 2 * HEAD_DIM
    groups = ((0, 0, attn_cols), (1, 0, D), (0, attn_cols, win.shape[1]))
    own = (win, wout)
    full = (full_in, full_out)
    piece_rows = (IN_ROWS, OUT_ROWS)

    def span(group, part):
        which, first, last = groups[group]
        middle = (first + last) // 2
        if part == 1:
            return which, pl.ds(first, middle - first)
        if part == 2:
            return which, pl.ds(middle, last - middle)
        return which, pl.ds(first, last - first)

    def rows_of(which, plane, quarter):
        size = piece_rows[which]
        return pl.ds(pl.multiple_of((plane * 4 + quarter) * size, 8), size)

    def place(group, part, plane, quarter):
        which, cols = span(group, part)
        return full[which].at[rows_of(which, plane, quarter), cols]

    def z_copy(group, k):
        which, cols = span(group, 0)
        return remote(
            own[which].at[rows_of(which, 0, q), cols],
            place(group, 0, z, q),
            z_send.at[group, k],
            z_recv.at[group, z],
            (q, lax.rem(z + k, 4), c),
        )

    def pair_copy(number):
        source, target = ((tok, all_tok), (cot, all_cot))[number]
        return remote(source, target.at[c], pair_send.at[number], pair_recv.at[number], to_pair)

    for number in range(2):
        pair_copy(number).start()
    for group in range(3):
        for k in (1, 2, 3):
            z_copy(group, k).start()

    locals_ = []
    for number, (source, target) in enumerate(
        (
            (win, full_in.at[pl.ds(pl.multiple_of(z * 4 * IN_ROWS, 8), 4 * IN_ROWS), :]),
            (wout, full_out.at[pl.ds(pl.multiple_of(z * 4 * OUT_ROWS, 8), 4 * OUT_ROWS), :]),
            (tok, all_tok.at[c]),
            (cot, all_cot.at[c]),
        )
    ):
        copy = pltpu.make_async_copy(source, target, local_sem.at[number])
        copy.start()
        locals_.append(copy)

    def xy_copy(path, group, plane):
        quarter = (q, q, xn, yn)[path]
        piece = place(group, (0, 0, 1, 2)[path], plane, quarter)
        return remote(
            piece,
            piece,
            xy_send.at[path, group, plane],
            xy_recv.at[path, group, plane],
            (to_x, to_y, to_y, to_x)[path],
        )

    def xy_landed(path, group, plane):
        quarter = (xn, yn, dg, dg)[path]
        piece = place(group, (0, 0, 1, 2)[path], plane, quarter)
        remote(
            piece, piece, xy_send.at[path, group, plane], xy_recv.at[path, group, plane], to_pair
        ).wait_recv()

    def spread(group, plane):
        @pl.when(z != plane)
        def _():
            piece = place(group, 0, plane, q)
            remote(piece, piece, z_send.at[group, 1], z_recv.at[group, plane], to_pair).wait_recv()
            xy_copy(0, group, plane).start()
            xy_copy(1, group, plane).start()

    def relay(group, plane):
        @pl.when(z != plane)
        def _():
            xy_landed(0, group, plane)
            xy_copy(2, group, plane).start()
            xy_landed(1, group, plane)
            xy_copy(3, group, plane).start()

    def settle(group, plane):
        @pl.when(z != plane)
        def _():
            xy_landed(2, group, plane)
            xy_landed(3, group, plane)

    locals_[2].wait()
    locals_[3].wait()
    for number, target in enumerate((all_tok, all_cot)):
        piece = target.at[1 - c]
        remote(piece, piece, pair_send.at[number], pair_recv.at[number], to_pair).wait_recv()
    rows = tok.shape[0]
    for half in range(2):
        inputs = all_tok[half].astype(F32)
        center = inputs - jnp.mean(inputs, axis=-1, keepdims=True)
        inverse = lax.rsqrt(jnp.mean(center * center, axis=-1, keepdims=True) + 1e-05)
        normed = center * inverse
        norm_one[pl.ds(half * rows, rows), :] = (normed * affine[0:1, :] + affine[1:2, :]).astype(BF16)
        norm_two[pl.ds(half * rows, rows), :] = (normed * affine[2:3, :] + affine[3:4, :]).astype(BF16)
    for plane in range(4):
        spread(0, plane)
    for plane in range(4):
        relay(0, plane)
    for plane in range(4):
        settle(0, plane)
    locals_[0].wait()
    locals_[1].wait()

    half_rot = ROT // 2
    cosine, sine = cos_ref[...], sin_ref[...]

    def turn(block, cosine, sine):
        front, back = block[:half_rot], block[half_rot:ROT]
        return jnp.concatenate(
            [front * cosine - back * sine, back * cosine + front * sine, block[ROT:]], axis=0
        )

    projected = (
        jnp.dot(norm_one[...], full_in[:, :attn_cols], preferred_element_type=F32) + bias[...]
    ).T
    key_t = turn(projected[HALF_D : HALF_D + HEAD_DIM], cosine, sine)
    kv_all[z] = jnp.concatenate([key_t, projected[HALF_D + HEAD_DIM :]], axis=0).astype(BF16)

    def kv_copy(k):
        return remote(
            kv_all.at[z], kv_all.at[z], kv_send.at[0, k], kv_recv.at[0, k], (q, lax.rem(z + k, 4), c)
        )

    for k in (1, 2, 3):

        @pl.when(z + k < 4)
        def _():
            kv_copy(k).start()

    for head in range(HALF_HEADS):
        block = turn(projected[head * HEAD_DIM : (head + 1) * HEAD_DIM], cosine, sine) * 0.125
        q_all[:, head * CHUNK : (head + 1) * CHUNK] = block.astype(BF16)
    spread(1, 0)
    dkeys[...] = jnp.zeros_like(dkeys)
    dvalues[...] = jnp.zeros_like(dvalues)

    def spread_block(index):
        place_rows = pl.ds(pl.multiple_of(index * CHUNK, CHUNK), CHUNK)
        turned = kv_all[index].astype(F32).T.astype(BF16)
        keys[place_rows, :] = turned[:, :HEAD_DIM]
        values[place_rows, :] = turned[:, HEAD_DIM:]

    spread_block(z)
    relay(1, 0)
    for k in (1, 2, 3):

        @pl.when(z - k >= 0)
        def _():
            source = lax.rem(z + 4 - k, 4)
            remote(
                kv_all.at[source], kv_all.at[source], kv_send.at[0, k], kv_recv.at[0, k], to_pair
            ).wait_recv()
            spread_block(source)

    settle(1, 0)
    grads_t = jnp.concatenate(
        [
            lax.dot_general(
                full_out[:HALF_D, :], all_cot[half], contract_cols, preferred_element_type=F32
            )
            for half in range(2)
        ],
        axis=1,
    ).astype(BF16)
    for head in range(HALF_HEADS):
        g_all[:, head * CHUNK : (head + 1) * CHUNK] = grads_t[head * HEAD_DIM : (head + 1) * HEAD_DIM]

    width = 2 * CHUNK
    cos_two = jnp.concatenate([cosine, cosine], axis=1)
    sin_two = jnp.concatenate([sine, sine], axis=1)
    polls = (
        ((spread, 1, 1), (spread, 1, 2)),
        ((relay, 1, 1), (relay, 1, 2), (spread, 1, 3)),
        ((relay, 1, 3), (spread, 2, 0)),
        ((relay, 2, 0), (spread, 2, 1), (spread, 2, 2)),
        ((relay, 2, 1), (relay, 2, 2), (spread, 2, 3)),
        ((relay, 2, 3),),
    )

    def poll(pair, late):
        for number in range(3):

            @pl.when(pair == number)
            def _():
                for action, group, plane in polls[2 * number + late]:
                    action(group, plane)

    def two_heads(pair, carry):
        cols = pl.ds(pl.multiple_of(pair * width, width), width)
        queries = q_all[:, cols]
        grads = g_all[:, cols].astype(F32)

        def rows_at(index):
            return pl.ds(pl.multiple_of(index * CHUNK, CHUNK), CHUNK)

        def forward(index, state, diagonal):
            top, total, out = state
            part = jnp.dot(keys[rows_at(index), :], queries, preferred_element_type=F32)
            if diagonal:
                key_place = lax.broadcasted_iota(jnp.int32, (CHUNK, width), 0)
                row_place = lax.rem(lax.broadcasted_iota(jnp.int32, (CHUNK, width), 1), CHUNK)
                part = jnp.where(key_place > row_place, neg_fill, part)
            above = jnp.maximum(top, jnp.max(part, axis=0, keepdims=True))
            part = jnp.exp(part - above)
            rounded = part.astype(BF16)
            weights[rows_at(index), :] = rounded
            tops[index] = above
            scale = jnp.exp(top - above)
            total = total * scale + jnp.sum(part, axis=0, keepdims=True)
            out = out * scale + jnp.dot(
                kv_all[index, HEAD_DIM:, :], rounded, preferred_element_type=F32
            )
            return above, total, out

        state = (
            jnp.full((1, width), neg_fill, F32),
            jnp.zeros((1, width), F32),
            jnp.zeros((HEAD_DIM, width), F32),
        )
        state = lax.fori_loop(0, z, lambda index, state: forward(index, state, False), state)
        top, total, out = forward(z, state, True)
        inverse = 1.0 / total
        out = out * inverse
        base = pl.multiple_of(pair * 2 * HEAD_DIM, 2 * HEAD_DIM)
        second = pl.multiple_of(base + HEAD_DIM, HEAD_DIM)
        att_ref[pl.ds(base, HEAD_DIM), :] = out[:, :CHUNK].astype(BF16)
        att_ref[pl.ds(second, HEAD_DIM), :] = out[:, CHUNK:].astype(BF16)
        inner = jnp.sum(grads * out, axis=0, keepdims=True)
        poll(pair, 0)

        def backward(index, dq):
            here = rows_at(index)
            factor = inverse * jnp.exp(tops[index] - top)
            scaled = (grads * factor).astype(BF16)
            dprob = jnp.dot(values[here, :], scaled, preferred_element_type=F32)
            rounded = weights[here, :]
            dscore = (rounded.astype(F32) * (dprob - inner * factor)).astype(BF16)
            dkeys[here, :] += lax.dot_general(
                dscore, queries, contract_cols, preferred_element_type=F32
            )
            dvalues[here, :] += lax.dot_general(
                rounded, scaled, contract_cols, preferred_element_type=F32
            )
            return dq + jnp.dot(kv_all[index, :HEAD_DIM, :], dscore, preferred_element_type=F32)

        dq = lax.fori_loop(0, z + 1, backward, jnp.zeros((HEAD_DIM, width), F32))
        dq = turn(dq * 0.125, cos_two, -sin_two)
        dq_ref[pl.ds(base, HEAD_DIM), :] = dq[:, :CHUNK].astype(BF16)
        dq_ref[pl.ds(second, HEAD_DIM), :] = dq[:, CHUNK:].astype(BF16)
        poll(pair, 1)
        return carry

    lax.fori_loop(0, HALF_HEADS // 2, two_heads, 0)

    for index in range(4):
        here = pl.ds(index * CHUNK, CHUNK)
        dkv_ref[index] = jnp.concatenate([dkeys[here, :], dvalues[here, :]], axis=1)
    for group, plane in ((1, 1), (1, 2), (1, 3), (2, 0), (2, 1), (2, 2), (2, 3)):
        settle(group, plane)
    for number in range(2):
        pair_copy(number).wait_send()
    for k in (1, 2, 3):
        for group in range(3):
            z_copy(group, k).wait_send()

        @pl.when(z + k < 4)
        def _():
            kv_copy(k).wait_send()

    for group in range(3):
        for plane in range(4):

            @pl.when(z != plane)
            def _():
                for path in range(4):
                    xy_copy(path, group, plane).wait_send()


def front(win, wout, tok, cot, affine, bias, cosine, sine):
    rows, width = tok.shape
    chip_rows = 2 * rows
    dma = pltpu.SemaphoreType.DMA
    return pl.pallas_call(
        front_kernel,
        out_shape=(
            jax.ShapeDtypeStruct((4 * win.shape[0], win.shape[1]), BF16),
            jax.ShapeDtypeStruct((4 * wout.shape[0], wout.shape[1]), BF16),
            jax.ShapeDtypeStruct((2, rows, width), BF16),
            jax.ShapeDtypeStruct((2, rows, width), BF16),
            jax.ShapeDtypeStruct((chip_rows, width), BF16),
            jax.ShapeDtypeStruct((chip_rows, width), BF16),
            jax.ShapeDtypeStruct((HALF_D, chip_rows), BF16),
            jax.ShapeDtypeStruct((HALF_D, chip_rows), BF16),
            jax.ShapeDtypeStruct((4, chip_rows, 2 * HEAD_DIM), F32),
        ),
        in_specs=vmem_specs(8),
        out_specs=vmem_specs(9),
        scratch_shapes=[
            pltpu.VMEM((HEAD_DIM, HALF_HEADS * CHUNK), BF16),
            pltpu.VMEM((HEAD_DIM, HALF_HEADS * CHUNK), BF16),
            pltpu.VMEM((4, 2 * HEAD_DIM, CHUNK), BF16),
            pltpu.VMEM((4 * CHUNK, HEAD_DIM), BF16),
            pltpu.VMEM((4 * CHUNK, HEAD_DIM), BF16),
            pltpu.VMEM((4 * CHUNK, 2 * CHUNK), BF16),
            pltpu.VMEM((4, 1, 2 * CHUNK), F32),
            pltpu.VMEM((4 * CHUNK, HEAD_DIM), F32),
            pltpu.VMEM((4 * CHUNK, HEAD_DIM), F32),
            dma((3, 4)),
            dma((3, 4)),
            dma((4, 3, 4)),
            dma((4, 3, 4)),
            dma((2,)),
            dma((2,)),
            dma((1, 4)),
            dma((1, 4)),
            dma((4,)),
        ],
        compiler_params=pltpu.CompilerParams(
            collective_id=0, has_side_effects=True, vmem_limit_bytes=VMEM_LIMIT
        ),
        name="front",
    )(win, wout, tok, cot, affine, bias, cosine, sine)


PLANE_ORDER = (2, 1, 3, 0)
HIDDEN_BLOCK = 512
ROOT_HALF = 0.7071067811865476
GAUSS = 0.3989422804014327


def back_kernel(
    full_in,
    full_out,
    all_tok,
    all_cot,
    norm_one,
    norm_two,
    att_ref,
    dq_ref,
    dkv_part,
    affine,
    bias_up,
    bias_out,
    cos_ref,
    sin_ref,
    output_ref,
    input_grad_ref,
    sum_in,
    sum_out,
    vec_sum,
    one_t,
    two_t,
    act,
    slope,
    dhid,
    branch_t,
    qkv_grad,
    partial_out,
    upstream,
    out_other,
    up_other,
    g_in,
    g_out,
    x_in,
    x_out,
    y_in,
    y_out,
    ax_in,
    ax_out,
    ay_in,
    ay_out,
    bx_in,
    bx_out,
    by_in,
    by_out,
    t_in,
    t_out,
    z_in,
    z_out,
    own_in,
    own_out,
    vec_send,
    vec_recv,
    vec_zone,
    pair_in,
    summed,
    zone,
    dkv,
    send_sem,
    recv_sem,
    vec_send_sem,
    vec_recv_sem,
    last_send_sem,
    last_recv_sem,
    pair_send_sem,
    pair_recv_sem,
    part_send_sem,
    part_recv_sem,
    zone_send_sem,
    zone_recv_sem,
):
    z, q, c, qx, qy, xn, yn = places()
    dg = (1 - qy) * 2 + 1 - qx
    to_x, to_y, to_pair = (xn, z, c), (yn, z, c), (q, z, 1 - c)
    greet([(q, lax.rem(z + k, 4), c) for k in (1, 2, 3)] + [to_x, to_y, to_pair])
    sent = []

    def send(source, target, sems, index, device):
        copy = remote(source, target, sems[0].at[index], sems[1].at[index], device)
        copy.start()
        sent.append(copy)

    def landed(target, sems, index):
        remote(target, target, sems[0].at[index], sems[1].at[index], to_pair).wait_recv()

    main = (send_sem, recv_sem)
    vecs = (vec_send_sem, vec_recv_sem)
    lasts = (last_send_sem, last_recv_sem)
    pairs = (pair_send_sem, pair_recv_sem)
    parts = (part_send_sem, part_recv_sem)
    grads = (g_in, g_out)
    halves = tuple(ref.shape[-1] // 2 for ref in grads)
    first = tuple(pl.ds(0, half) for half in halves)
    second = tuple(pl.ds(half, half) for half in halves)
    from_x, from_y = (x_in, x_out), (y_in, y_out)
    ax, ay, bx, by = (ax_in, ax_out), (ay_in, ay_out), (bx_in, bx_out), (by_in, by_out)
    totals, zones, own = (t_in, t_out), (z_in, z_out), (own_in, own_out)
    outs = (sum_in, sum_out)
    rows = all_tok.shape[1]
    mine = pl.ds(pl.multiple_of(c * rows, rows), rows)
    other = pl.ds(pl.multiple_of((1 - c) * rows, rows), rows)
    attn_cols = HALF_D + 2 * HEAD_DIM
    hidden = full_in.shape[1] - attn_cols

    def plane_of(step):
        return lax.rem(z + PLANE_ORDER[step % 4], 4)

    def kind(step):
        return 1 if step < 4 else 0

    def exchange(step):
        h, a, j = plane_of(step), kind(step), step % 4
        if a == 1:
            size = 4 * OUT_ROWS
            left = branch_t[pl.ds(pl.multiple_of(h * size, 16), size), :]
            for half in range(2):
                cols = pl.ds(half * halves[1], halves[1])
                block = sum(
                    jnp.dot(
                        left[:, k * rows : (k + 1) * rows],
                        all_cot[k, :, cols],
                        preferred_element_type=F32,
                    )
                    for k in range(2)
                ).astype(BF16)
                for quarter in range(4):
                    g_out[h, quarter // 2, quarter % 2, :, cols] = block[
                        quarter * OUT_ROWS : (quarter + 1) * OUT_ROWS
                    ]
        else:
            size = 4 * IN_ROWS
            here = pl.ds(pl.multiple_of(h * size, 16), size)
            for number in range(4):
                cols = pl.ds(number * HIDDEN_BLOCK, HIDDEN_BLOCK)
                if number == 0:
                    block = jnp.dot(one_t[here, :], qkv_grad[...], preferred_element_type=F32)
                else:
                    block = jnp.dot(
                        two_t[here, :],
                        dhid[:, pl.ds((number - 1) * HIDDEN_BLOCK, HIDDEN_BLOCK)],
                        preferred_element_type=F32,
                    )
                block = block.astype(BF16)
                for quarter in range(4):
                    g_in[h, quarter // 2, quarter % 2, :, cols] = block[
                        quarter * IN_ROWS : (quarter + 1) * IN_ROWS
                    ]
        send(grads[a].at[h, :, 1 - qx, :, first[a]], from_x[a].at[j], main, (j, 0, a), to_x)
        send(grads[a].at[h, 1 - qy, :, :, second[a]], from_y[a].at[j], main, (j, 1, a), to_y)

    def halve(step):
        h, a, j = plane_of(step), kind(step), step % 4
        landed(from_x[a].at[j], main, (j, 0, a))
        ax[a][j] = (
            grads[a][h, 1 - qy, qx, :, first[a]].astype(F32) + from_x[a][j, 1 - qy].astype(F32)
        ).astype(BF16)
        send(ax[a].at[j], ay[a].at[j], main, (j, 2, a), to_y)
        landed(from_y[a].at[j], main, (j, 1, a))
        bx[a][j] = (
            grads[a][h, qy, 1 - qx, :, second[a]].astype(F32) + from_y[a][j, 1 - qx].astype(F32)
        ).astype(BF16)
        send(bx[a].at[j], by[a].at[j], main, (j, 3, a), to_x)

    def finish(step):
        h, a, j = plane_of(step), kind(step), step % 4
        shift = PLANE_ORDER[j]
        landed(ay[a].at[j], main, (j, 2, a))
        left = (
            grads[a][h, qy, qx, :, first[a]].astype(F32)
            + from_x[a][j, qy].astype(F32)
            + ay[a][j].astype(F32)
        )
        landed(by[a].at[j], main, (j, 3, a))
        right = (
            grads[a][h, qy, qx, :, second[a]].astype(F32)
            + from_y[a][j, qx].astype(F32)
            + by[a][j].astype(F32)
        )
        if shift == 0:
            own[a][:, first[a]] = left
            own[a][:, second[a]] = right
        else:
            totals[a][shift - 1, :, first[a]] = left.astype(BF16)
            totals[a][shift - 1, :, second[a]] = right.astype(BF16)
            send(totals[a].at[shift - 1], zones[a].at[shift - 1], main, (j, 4, a), (q, h, c))

    def share(a):
        for j in range(3):
            landed(zones[a].at[PLANE_ORDER[j] - 1], main, (j, 4, a))
        whole = own[a][...] + zones[a][0].astype(F32) + zones[a][1].astype(F32) + zones[a][2].astype(F32)
        outs[a][c, q] = whole.astype(BF16)
        piece = outs[a].at[c, q]
        send(piece, piece, lasts, (0, a), to_x)
        send(piece, piece, lasts, (1, a), to_y)
        send(piece, piece, pairs, (0, a), to_pair)

    def pass_on(a):
        piece = outs[a].at[c, xn]
        landed(piece, lasts, (0, a))
        part = outs[a].at[c, xn, :, first[a]]
        send(part, part, lasts, (2, a), to_y)
        send(piece, piece, pairs, (1, a), to_pair)
        piece = outs[a].at[c, yn]
        landed(piece, lasts, (1, a))
        part = outs[a].at[c, yn, :, second[a]]
        send(part, part, lasts, (3, a), to_x)
        send(piece, piece, pairs, (2, a), to_pair)

    def close(a):
        landed(outs[a].at[c, dg, :, first[a]], lasts, (2, a))
        landed(outs[a].at[c, dg, :, second[a]], lasts, (3, a))
        piece = outs[a].at[c, dg]
        send(piece, piece, pairs, (3, a), to_pair)

    def zone_copy(k):
        target = lax.rem(z + 4 - k, 4)
        return remote(
            summed.at[target],
            zone.at[k - 1],
            zone_send_sem.at[k],
            zone_recv_sem.at[k],
            (q, target, c),
        )

    send(dkv_part.at[:, other, :], pair_in, parts, 0, to_pair)

    branch_t[pl.ds(0, HALF_D), :] = att_ref[...]
    for number in range(hidden // HIDDEN_BLOCK):
        cols = pl.ds(number * HIDDEN_BLOCK, HIDDEN_BLOCK)
        before = (
            jnp.dot(
                norm_two[...],
                full_in[:, pl.ds(attn_cols + number * HIDDEN_BLOCK, HIDDEN_BLOCK)],
                preferred_element_type=F32,
            )
            + bias_up[:, cols]
        )
        normal = 0.5 * (1.0 + lax.erf(before * ROOT_HALF))
        active = before * normal
        act[:, cols] = active.astype(BF16)
        slope[:, cols] = normal + before * (GAUSS * jnp.exp(-0.5 * before * before))
        branch_t[pl.ds(HALF_D + number * HIDDEN_BLOCK, HIDDEN_BLOCK), :] = active.T.astype(BF16)
    exchange(0)
    exchange(1)
    landed(pair_in, parts, 0)
    for index in range(4):
        summed[index] = dkv_part[index, mine, :] + pair_in[index]
    for k in (1, 2, 3):

        @pl.when(z - k >= 0)
        def _():
            zone_copy(k).start()

    one_t[...] = norm_one[...].astype(F32).T.astype(BF16)
    two_t[...] = norm_two[...].astype(F32).T.astype(BF16)
    for number in range(hidden // HIDDEN_BLOCK):
        cols = pl.ds(number * HIDDEN_BLOCK, HIDDEN_BLOCK)
        for k in range(2):
            here = pl.ds(k * rows, rows)
            back = lax.dot_general(
                all_cot[k],
                full_out[pl.ds(HALF_D + number * HIDDEN_BLOCK, HIDDEN_BLOCK), :],
                contract_cols,
                preferred_element_type=F32,
            )
            dhid[here, cols] = (back * slope[here, cols]).astype(BF16)
    halve(0)
    exchange(2)
    dkv[mine, :] = summed[z]
    for k in (1, 2, 3):

        @pl.when(z + k < 4)
        def _():
            remote(
                zone.at[k - 1], zone.at[k - 1], zone_send_sem.at[k], zone_recv_sem.at[k], to_pair
            ).wait_recv()
            dkv[mine, :] += zone[k - 1]

    send(dkv.at[mine, :], dkv.at[mine, :], parts, 1, to_pair)
    halve(1)
    exchange(3)
    finish(0)
    partial_out[...] = jnp.dot(
        att_ref[...].astype(F32).T.astype(BF16), full_out[:HALF_D, :], preferred_element_type=F32
    ) + jnp.dot(act[...], full_out[pl.ds(HALF_D, hidden), :], preferred_element_type=F32)
    send(partial_out.at[other, :], out_other, parts, 2, to_pair)
    landed(dkv.at[other, :], parts, 1)
    half_rot = ROT // 2
    turned = dkv[...].T
    front_part, back_part = turned[:half_rot], turned[half_rot:ROT]
    cosine, sine = cos_ref[...], sin_ref[...]
    turned = jnp.concatenate(
        [
            front_part * cosine + back_part * sine,
            back_part * cosine - front_part * sine,
            turned[ROT:],
        ],
        axis=0,
    )
    qkv_grad[:, :HALF_D] = dq_ref[...].astype(F32).T.astype(BF16)
    qkv_grad[:, HALF_D:] = turned.T.astype(BF16)
    halve(2)
    exchange(4)
    finish(1)
    keep = jnp.where(c == 0, 1.0, 0.0)
    vec_send[...] = jnp.zeros_like(vec_send)
    mine_vec = vec_send.at[0]
    column = lax.broadcasted_iota(jnp.int32, (1, attn_cols), 1)
    once = jnp.where(column < HALF_D, 1.0, keep)
    first_rows = jnp.zeros((1, D), F32)
    sums = [first_rows] * 4
    for k in range(2):
        here = pl.ds(k * rows, rows)
        inputs = all_tok[k].astype(F32)
        center = inputs - jnp.mean(inputs, axis=-1, keepdims=True)
        inverse = lax.rsqrt(jnp.mean(center * center, axis=-1, keepdims=True) + 1e-05)
        normed = center * inverse
        masked = (qkv_grad[here, :].astype(F32) * once).astype(BF16)
        one = lax.dot_general(
            masked, full_in[:, :attn_cols], contract_cols, preferred_element_type=F32
        )
        two = lax.dot_general(
            dhid[here, :],
            full_in[:, pl.ds(attn_cols, hidden)],
            contract_cols,
            preferred_element_type=F32,
        )
        terms = (one * normed, one, two * normed, two)
        sums = [old + jnp.sum(term, axis=0, keepdims=True) for old, term in zip(sums, terms)]
        upstream[here, :] = one * affine[0:1, :] + two * affine[2:3, :]
    send(upstream.at[other, :], up_other, parts, 3, to_pair)
    halve(3)
    exchange(5)
    finish(2)
    for number in range(4):
        mine_vec[number : number + 1, :D] = sums[number]
    mine_vec[4:5, :D] = jnp.sum(all_cot[c].astype(F32), axis=0, keepdims=True)
    query_sums = jnp.sum(qkv_grad[...].astype(F32), axis=0, keepdims=True) * once
    hidden_sums = [
        jnp.sum(
            dhid[:, pl.ds(number * HIDDEN_BLOCK, HIDDEN_BLOCK)].astype(F32), axis=0, keepdims=True
        )
        for number in range(hidden // HIDDEN_BLOCK)
    ]
    for core in range(2):
        for number, piece in enumerate([query_sums] + hidden_sums):
            row = 4 * core + number
            mine_vec[row : row + 1, D:] = jnp.where(c == core, piece, 0.0)
    send(vec_send.at[0], vec_recv.at[0], vecs, 0, to_x)
    halve(4)
    exchange(6)
    finish(3)
    landed(vec_recv.at[0], vecs, 0)
    vec_send[1] = vec_send[0] + vec_recv[0]
    send(vec_send.at[1], vec_recv.at[1], vecs, 1, to_y)
    halve(5)
    exchange(7)
    finish(4)
    share(1)
    landed(vec_recv.at[1], vecs, 1)
    vec_send[2] = vec_send[1] + vec_recv[1]
    send(vec_send.at[2], vec_recv.at[2], vecs, 2, to_pair)
    halve(6)
    finish(5)
    pass_on(1)
    landed(vec_recv.at[2], vecs, 2)
    vec_send[3] = vec_send[2] + vec_recv[2]
    vec_zone[z] = vec_send[3]
    for k in (1, 2, 3):
        send(vec_send.at[3], vec_zone.at[z], vecs, 2 + k, (q, lax.rem(z + k, 4), c))
    halve(7)
    finish(6)
    close(1)
    landed(out_other, parts, 2)
    output_ref[...] = (
        all_tok[c].astype(F32) + (partial_out[mine, :] + out_other[...]) + bias_out[...]
    ).astype(BF16)
    landed(up_other, parts, 3)
    inputs = all_tok[c].astype(F32)
    center = inputs - jnp.mean(inputs, axis=-1, keepdims=True)
    inverse = lax.rsqrt(jnp.mean(center * center, axis=-1, keepdims=True) + 1e-05)
    normed = center * inverse
    total = upstream[mine, :] + up_other[...]
    inside = (
        total
        - jnp.mean(total, axis=-1, keepdims=True)
        - normed * jnp.mean(total * normed, axis=-1, keepdims=True)
    )
    finish(7)
    share(0)
    input_grad_ref[...] = (all_cot[c].astype(F32) + inverse * inside).astype(BF16)
    pass_on(0)
    for k in (1, 2, 3):
        landed(vec_zone.at[lax.rem(z + 4 - k, 4)], vecs, 2 + k)
    vec_sum[...] = (vec_zone[0] + vec_zone[1]) + (vec_zone[2] + vec_zone[3])
    close(0)
    for a in (1, 0):
        for index, quarter in enumerate((q, xn, yn, dg)):
            landed(outs[a].at[1 - c, quarter], pairs, (index, a))
    for copy in sent:
        copy.wait_send()
    for k in (1, 2, 3):

        @pl.when(z - k >= 0)
        def _():
            zone_copy(k).wait_send()


def back(full_in, full_out, all_tok, all_cot, norm_one, norm_two, att_t, dq_t, dkv, affine, bias_up, bias_out, cosine, sine):
    rows = all_tok.shape[1]
    chip_rows = 2 * rows
    cols_in, cols_out = full_in.shape[1], full_out.shape[1]
    hidden = bias_up.shape[1]
    kv_width = 2 * HEAD_DIM
    vec_shape = (8, D + HALF_D + kv_width)
    dma = pltpu.SemaphoreType.DMA

    def both(lead, cut, kind):
        return [
            pltpu.VMEM(lead + (IN_ROWS, cols_in // cut), kind),
            pltpu.VMEM(lead + (OUT_ROWS, cols_out // cut), kind),
        ]

    def twice(*shape):
        return [dma(shape), dma(shape)]

    return pl.pallas_call(
        back_kernel,
        out_shape=(
            jax.ShapeDtypeStruct((rows, D), BF16),
            jax.ShapeDtypeStruct((rows, D), BF16),
            jax.ShapeDtypeStruct((2, 4, IN_ROWS, cols_in), BF16),
            jax.ShapeDtypeStruct((2, 4, OUT_ROWS, cols_out), BF16),
            jax.ShapeDtypeStruct(vec_shape, F32),
        ),
        in_specs=vmem_specs(14),
        out_specs=vmem_specs(5),
        scratch_shapes=[
            pltpu.VMEM((D, chip_rows), BF16),
            pltpu.VMEM((D, chip_rows), BF16),
            pltpu.VMEM((chip_rows, hidden), BF16),
            pltpu.VMEM((chip_rows, hidden), F32),
            pltpu.VMEM((chip_rows, hidden), BF16),
            pltpu.VMEM((HALF_D + hidden, chip_rows), BF16),
            pltpu.VMEM((chip_rows, HALF_D + kv_width), BF16),
            pltpu.VMEM((chip_rows, D), F32),
            pltpu.VMEM((chip_rows, D), F32),
            pltpu.VMEM((rows, D), F32),
            pltpu.VMEM((rows, D), F32),
        ]
        + both((4, 2, 2), 1, BF16)
        + both((4, 2), 2, BF16)
        + both((4, 2), 2, BF16)
        + both((4,), 2, BF16) * 4
        + both((3,), 1, BF16) * 2
        + both((), 1, F32)
        + [
            pltpu.VMEM((4,) + vec_shape, F32),
            pltpu.VMEM((3,) + vec_shape, F32),
            pltpu.VMEM((4,) + vec_shape, F32),
            pltpu.VMEM((4, rows, kv_width), F32),
            pltpu.VMEM((4, rows, kv_width), F32),
            pltpu.VMEM((3, rows, kv_width), F32),
            pltpu.VMEM((chip_rows, kv_width), F32),
        ]
        + twice(4, 5, 2)
        + twice(6)
        + twice(4, 2)
        + twice(4, 2)
        + twice(4)
        + twice(4),
        compiler_params=pltpu.CompilerParams(
            collective_id=1, has_side_effects=True, vmem_limit_bytes=BACK_LIMIT
        ),
        name="back",
    )(full_in, full_out, all_tok, all_cot, norm_one, norm_two, att_t, dq_t, dkv, affine, bias_up, bias_out, cosine, sine)


KV_END = D + 2 * HEAD_DIM
HALF_D = D // 2


def hidden_spans(core, ff, row_share):
    spans = []
    for owner in range((D + ff) // row_share):
        first = max(owner * row_share - D, 0)
        last = (owner + 1) * row_share - D
        if last > first:
            half = (last - first) // 2
            spans.append((first + core * half, half))
    return spans


def core_columns(array, core, ff, row_share):
    pieces = [array[..., core * HALF_D : (core + 1) * HALF_D], array[..., D:KV_END]]
    pieces += [
        array[..., KV_END + first : KV_END + first + size]
        for first, size in hidden_spans(core, ff, row_share)
    ]
    return jnp.concatenate(pieces, axis=-1)


def join_columns(pair, ff, row_share):
    pieces = [pair[0][..., :HALF_D], pair[1][..., :HALF_D], pair[0][..., HALF_D : HALF_D + 2 * HEAD_DIM]]
    at = HALF_D + 2 * HEAD_DIM
    for _, size in hidden_spans(0, ff, row_share):
        pieces += [pair[0][..., at : at + size], pair[1][..., at : at + size]]
        at += size
    return jnp.concatenate(pieces, axis=-1)


def fast_shards(
    tokens,
    cotangent,
    in_master,
    in_moment,
    in_second,
    out_master,
    out_moment,
    out_second,
    vec_master,
    vec_moment,
    vec_second,
    rotary_scale,
):
    z = lax.axis_index("head")
    c = lax.axis_index("ctx")
    first_core = c == 0
    rows = tokens.shape[0]
    chip_rows = 2 * rows
    row_share = out_master.shape[0]
    ff = in_master.shape[1] - KV_END
    half_share = row_share // 2
    attn_share = D // 2

    def pick(array):
        return jnp.where(
            first_core, core_columns(array, 0, ff, row_share), core_columns(array, 1, ff, row_share)
        )

    win = pick(in_master.astype(BF16))
    out_low = out_master.astype(BF16)
    start_one = jnp.where(z == 0, attn_share * c, half_share * c)
    start_two = jnp.where(z == 0, D + (half_share - attn_share) * c, half_share * c + attn_share)
    wout = jnp.concatenate(
        [
            lax.dynamic_slice_in_dim(out_low, start_one, attn_share, 0),
            lax.dynamic_slice_in_dim(out_low, start_two, half_share - attn_share, 0),
        ],
        axis=0,
    )
    bias = pick(vec_master[5 * D :])
    attn_cols = HALF_D + 2 * HEAD_DIM
    positions = z * chip_rows + jnp.arange(chip_rows, dtype=jnp.int32)
    cosine, sine_table = rotary_tables(positions.astype(F32), rotary_scale[0].astype(F32))
    affine = vec_master[: 4 * D].reshape(4, D)
    cos_t, sin_t = cosine.T, sine_table.T
    full_in, full_out, all_tok, all_cot, norm_one, norm_two, att_t, dq_t, dkv = front(
        win,
        wout,
        tokens,
        cotangent,
        affine,
        bias[:attn_cols].reshape(1, attn_cols),
        cos_t,
        sin_t,
    )
    output, input_grad, sum_in, sum_out, sum_vec = back(
        full_in,
        full_out,
        all_tok,
        all_cot,
        norm_one,
        norm_two,
        att_t,
        dq_t,
        dkv,
        affine,
        bias[attn_cols:].reshape(1, -1),
        vec_master[4 * D : 5 * D].reshape(1, D),
        cos_t,
        sin_t,
    )
    core_sums = sum_vec[:, D:].reshape(2, -1)
    summed_vec = jnp.concatenate(
        [sum_vec[:5, :D].reshape(-1), join_columns((core_sums[0], core_sums[1]), ff, row_share)]
    )
    sum_in = sum_in.reshape(2, -1, sum_in.shape[-1])
    summed_in = join_columns((sum_in[0], sum_in[1]), ff, row_share).astype(F32)
    low, high = sum_out.reshape(2, half_share, D)
    head_rows = jnp.concatenate([low[:attn_share], high[:attn_share], low[attn_share:], high[attn_share:]], axis=0)
    summed_out = jnp.where(z == 0, head_rows, jnp.concatenate([low, high], axis=0)).astype(F32)

    in_moment_new, in_second_new, in_master_new = adam_update(
        in_master, in_moment, in_second, summed_in, matrix_rate, weight_decay
    )
    out_moment_new, out_second_new, out_master_new = adam_update(
        out_master, out_moment, out_second, summed_out, matrix_rate, weight_decay
    )
    vec_moment_new, vec_second_new, vec_master_new = adam_update(
        vec_master, vec_moment, vec_second, summed_vec, vector_rate, 0.0
    )
    return (
        output,
        input_grad,
        in_moment_new,
        in_second_new,
        in_master_new,
        in_master_new.astype(BF16),
        out_moment_new,
        out_second_new,
        out_master_new,
        out_master_new.astype(BF16),
        vec_moment_new,
        vec_second_new,
        vec_master_new,
    )


def solution(mesh):
    placed = (
        P(("dp", "head", "ctx"), None),
        P(("dp", "head", "ctx"), None),
        P("head", None),
        P("head", None),
        P("head", None),
        P("head", None),
        P("head", None),
        P("head", None),
        P(),
        P(),
        P(),
        P(),
    )
    paired = dict(mesh.shape) == {"dp": 4, "head": 4, "ctx": 2}
    body = fast_shards if paired else shards
    return jax.shard_map(
        body,
        mesh=mesh,
        in_specs=placed,
        out_specs=(
            P(("dp", "head", "ctx"), None),
            P(("dp", "head", "ctx"), None),
            P("head", None),
            P("head", None),
            P("head", None),
            P("head", None),
            P("head", None),
            P("head", None),
            P("head", None),
            P("head", None),
            P(),
            P(),
            P(),
        ),
        check_vma=False,
    )
```

```python
import jax
import jax.numpy as jnp
from jax import lax
from jax.experimental import pallas as pl
from jax.experimental.pallas import tpu as pltpu
from jax.sharding import PartitionSpec as P

HEADS = 12
HEAD_DIM = 64
ROT = 16
D = 768
KEY_BLOCK = 1024
ADAM_STEP = 3


neg_fill = -1e30
matrix_rate = 0.03
vector_rate = 0.3
weight_decay = 0.1
adam_epsilon = 1e-08
contract_rows = (((0,), (0,)), ((), ()))
contract_cols = (((1,), (1,)), ((), ()))


def layer_norm(values, norm_gain, norm_shift):
    center = values - jnp.mean(values, axis=-1, keepdims=True)
    inverse = lax.rsqrt(jnp.mean(center * center, axis=-1, keepdims=True) + 1e-05)
    normed = center * inverse
    return (normed * norm_gain + norm_shift, normed, inverse)


def norm_back(upstream, normed, inverse, norm_gain):
    scaled = upstream * norm_gain
    inside = (
        scaled
        - jnp.mean(scaled, axis=-1, keepdims=True)
        - normed * jnp.mean(scaled * normed, axis=-1, keepdims=True)
    )
    return (inverse * inside, jnp.sum(upstream * normed, axis=0), jnp.sum(upstream, axis=0))


def rotary_tables(positions, scale_value):
    half_rot = ROT // 2
    frequency = 10000.0 ** (-(2.0 * jnp.arange(half_rot, dtype=jnp.float32)) / ROT)
    angles = (positions / scale_value)[:, None] * frequency[None, :]
    return (jnp.cos(angles), jnp.sin(angles))


def rotate(values, cosine, sine_table):
    half_rot = ROT // 2
    front_half = values[..., :half_rot]
    back_half = values[..., half_rot:ROT]
    return jnp.concatenate(
        [
            front_half * cosine - back_half * sine_table,
            back_half * cosine + front_half * sine_table,
            values[..., ROT:],
        ],
        axis=-1,
    )


def score_block(query_rows, row_pos, whole_kv, block_index):
    key_block = lax.dynamic_slice_in_dim(whole_kv, block_index * KEY_BLOCK, KEY_BLOCK, 0)
    scores = lax.dot_general(
        query_rows, key_block[:, :HEAD_DIM], contract_cols, preferred_element_type=jnp.float32
    )
    key_pos = block_index * KEY_BLOCK + jnp.arange(KEY_BLOCK, dtype=jnp.int32)
    allowed = key_pos[None, :] <= row_pos[:, None]
    return (jnp.where(allowed, scores, neg_fill), allowed, key_block)


def log_totals(query_rows, row_pos, whole_kv):
    row_count = query_rows.shape[0]
    last_pos = jnp.max(row_pos)

    def advance(block_index, state_now):

        def process(state_old):
            run_max, run_sum = state_old
            scores, allowed, key_block = score_block(query_rows, row_pos, whole_kv, block_index)
            new_max = jnp.maximum(run_max, jnp.max(scores, axis=1))
            weights = jnp.where(allowed, jnp.exp(scores - new_max[:, None]), 0.0)
            return (new_max, run_sum * jnp.exp(run_max - new_max) + jnp.sum(weights, axis=1))

        return lax.cond(
            block_index * KEY_BLOCK <= last_pos, process, lambda state_same: state_same, state_now
        )

    start_state = (
        jnp.full((row_count,), neg_fill, jnp.float32),
        jnp.zeros((row_count,), jnp.float32),
    )
    run_max, run_sum = lax.fori_loop(0, whole_kv.shape[0] // KEY_BLOCK, advance, start_state)
    return run_max + jnp.log(run_sum)


def attend(query_rows, row_pos, whole_kv, log_sum):
    last_pos = jnp.max(row_pos)

    def advance(block_index, summed):

        def process(summed_old):
            scores, allowed, key_block = score_block(query_rows, row_pos, whole_kv, block_index)
            probs = jnp.where(allowed, jnp.exp(scores - log_sum[:, None]), 0.0).astype(jnp.bfloat16)
            return summed_old + jnp.dot(
                probs, key_block[:, HEAD_DIM:], preferred_element_type=jnp.float32
            )

        return lax.cond(
            block_index * KEY_BLOCK <= last_pos, process, lambda summed_same: summed_same, summed
        )

    start_state = jnp.zeros((query_rows.shape[0], HEAD_DIM), jnp.float32)
    return lax.fori_loop(0, whole_kv.shape[0] // KEY_BLOCK, advance, start_state)


def attend_back(query_rows, row_pos, whole_kv, log_sum, grad_rows, row_inner):
    last_pos = jnp.max(row_pos)

    def advance(block_index, state_now):

        def process(state_old):
            query_grad, kv_terms = state_old
            scores, allowed, key_block = score_block(query_rows, row_pos, whole_kv, block_index)
            probs = jnp.where(allowed, jnp.exp(scores - log_sum[:, None]), 0.0)
            prob_grad = lax.dot_general(
                grad_rows,
                key_block[:, HEAD_DIM:],
                contract_cols,
                preferred_element_type=jnp.float32,
            )
            score_grad = (probs * (prob_grad - row_inner[:, None])).astype(jnp.bfloat16)
            query_grad = query_grad + jnp.dot(
                score_grad, key_block[:, :HEAD_DIM], preferred_element_type=jnp.float32
            )
            key_grad = lax.dot_general(
                score_grad, query_rows, contract_rows, preferred_element_type=jnp.float32
            )
            value_grad = lax.dot_general(
                probs.astype(jnp.bfloat16),
                grad_rows,
                contract_rows,
                preferred_element_type=jnp.float32,
            )
            kv_terms = lax.dynamic_update_slice_in_dim(
                kv_terms,
                jnp.concatenate([key_grad, value_grad], axis=1),
                block_index * KEY_BLOCK,
                0,
            )
            return (query_grad, kv_terms)

        return lax.cond(
            block_index * KEY_BLOCK <= last_pos, process, lambda state_same: state_same, state_now
        )

    start_state = (
        jnp.zeros((query_rows.shape[0], HEAD_DIM), jnp.float32),
        jnp.zeros((whole_kv.shape[0], 2 * HEAD_DIM), jnp.float32),
    )
    return lax.fori_loop(0, whole_kv.shape[0] // KEY_BLOCK, advance, start_state)


def adam_update(master, moment, second, gradient, step_rate, decay_rate):
    moment_new = 0.5 * moment + 0.5 * gradient
    second_new = 0.5 * second + 0.5 * gradient * gradient
    correction = 1.0 - 0.5**ADAM_STEP
    normalized = moment_new / correction / (jnp.sqrt(second_new / correction) + adam_epsilon)
    return (moment_new, second_new, master - step_rate * (normalized + decay_rate * master))


def shards(
    tokens,
    cotangent,
    in_master,
    in_moment,
    in_second,
    out_master,
    out_moment,
    out_second,
    vec_master,
    vec_moment,
    vec_second,
    rotary_scale,
):
    local_rows = tokens.shape[0]
    full_in, full_out = (
        lax.all_gather(in_master.astype(jnp.bfloat16), "head", axis=0, tiled=True),
        lax.all_gather(out_master.astype(jnp.bfloat16), "head", axis=0, tiled=True),
    )
    scale_value = rotary_scale[0].astype(jnp.float32)
    local_pos = lax.axis_index(("head", "ctx")) * local_rows + jnp.arange(
        local_rows, dtype=jnp.int32
    )
    cosine, sine_table = rotary_tables(local_pos.astype(jnp.float32), scale_value)
    inputs = tokens.astype(jnp.float32)
    norm_one, normed_one, inverse_one = layer_norm(inputs, vec_master[0:D], vec_master[D : 2 * D])
    norm_two, normed_two, inverse_two = layer_norm(
        inputs, vec_master[2 * D : 3 * D], vec_master[3 * D : 4 * D]
    )
    first_in = norm_one.astype(jnp.bfloat16)
    second_in = norm_two.astype(jnp.bfloat16)
    projected = (
        jnp.dot(first_in, full_in[:, : D + 2 * HEAD_DIM], preferred_element_type=jnp.float32)
        + vec_master[5 * D : 6 * D + 2 * HEAD_DIM]
    )
    hidden_in = (
        jnp.dot(second_in, full_in[:, D + 2 * HEAD_DIM :], preferred_element_type=jnp.float32)
        + vec_master[6 * D + 2 * HEAD_DIM :]
    )
    query_heads = projected[:, :D].reshape(local_rows, HEADS, HEAD_DIM)
    queries = (
        (rotate(query_heads, cosine[:, None, :], sine_table[:, None, :]) * 0.125)
        .astype(jnp.bfloat16)
        .reshape(local_rows, D)
    )
    key_part = rotate(projected[:, D : D + HEAD_DIM], cosine, sine_table)
    shared = jnp.concatenate([key_part, projected[:, D + HEAD_DIM :]], axis=1).astype(jnp.bfloat16)
    whole_kv = lax.all_gather(shared, ("head", "ctx"), axis=0, tiled=True)
    activated = jax.nn.gelu(hidden_in, approximate=False).astype(jnp.bfloat16)
    heads_here = queries.shape[1] // HEAD_DIM
    query_rows = queries.reshape(-1, HEAD_DIM)
    row_pos = jnp.repeat(local_pos, heads_here)
    log_sum = log_totals(query_rows, row_pos, whole_kv)
    attended = attend(query_rows, row_pos, whole_kv, log_sum)
    att_out = attended.reshape(queries.shape).astype(jnp.bfloat16)
    branch_pair = jnp.concatenate([att_out, activated], axis=1)
    output = (
        inputs
        + jnp.dot(branch_pair, full_out, preferred_element_type=jnp.float32)
        + vec_master[4 * D : 5 * D]
    ).astype(jnp.bfloat16)
    cot_in = cotangent.astype(jnp.float32)
    grad_out = lax.dot_general(
        branch_pair, cotangent, contract_rows, preferred_element_type=jnp.float32
    )
    back_proj = lax.dot_general(
        cotangent, full_out, contract_cols, preferred_element_type=jnp.float32
    )
    branch_grad = back_proj[:, :D].astype(jnp.bfloat16)
    gelu_back = jax.vjp(lambda pre_act: jax.nn.gelu(pre_act, approximate=False), hidden_in)[1]
    hidden_grad = gelu_back(back_proj[:, D:])[0].astype(jnp.bfloat16)
    grad_rows = branch_grad.reshape(-1, HEAD_DIM)
    row_inner = jnp.sum(grad_rows.astype(jnp.float32) * attended, axis=1)
    query_grad, kv_terms = attend_back(query_rows, row_pos, whole_kv, log_sum, grad_rows, row_inner)
    att_cos, att_sin = rotary_tables(local_pos.astype(jnp.float32), scale_value)
    query_pre = rotate(
        query_grad.reshape(-1, heads_here, HEAD_DIM) * 0.125,
        att_cos[:, None, :],
        -att_sin[:, None, :],
    )
    query_pre = query_pre.reshape(queries.shape).astype(jnp.bfloat16)
    kv_sum = lax.psum_scatter(kv_terms, ("head", "ctx"), scatter_dimension=0, tiled=True)
    shared_grad = jnp.concatenate(
        [rotate(kv_sum[:, :HEAD_DIM], cosine, -sine_table), kv_sum[:, HEAD_DIM:]], axis=1
    ).astype(jnp.bfloat16)
    attn_grad = jnp.concatenate([query_pre, shared_grad], axis=1)
    grad_in = jnp.concatenate(
        [
            lax.dot_general(first_in, attn_grad, contract_rows, preferred_element_type=jnp.float32),
            lax.dot_general(
                second_in, hidden_grad, contract_rows, preferred_element_type=jnp.float32
            ),
        ],
        axis=1,
    )
    norm_grad_one = lax.dot_general(
        attn_grad, full_in[:, : D + 2 * HEAD_DIM], contract_cols, preferred_element_type=jnp.float32
    )
    norm_grad_two = lax.dot_general(
        hidden_grad,
        full_in[:, D + 2 * HEAD_DIM :],
        contract_cols,
        preferred_element_type=jnp.float32,
    )
    input_one, gain_one, shift_one = norm_back(
        norm_grad_one, normed_one, inverse_one, vec_master[0:D]
    )
    input_two, gain_two, shift_two = norm_back(
        norm_grad_two, normed_two, inverse_two, vec_master[2 * D : 3 * D]
    )
    input_grad = (cot_in + input_one + input_two).astype(jnp.bfloat16)
    grad_vec = jnp.concatenate(
        [
            gain_one,
            shift_one,
            gain_two,
            shift_two,
            jnp.sum(cot_in, axis=0),
            jnp.sum(attn_grad.astype(jnp.float32), axis=0),
            jnp.sum(hidden_grad.astype(jnp.float32), axis=0),
        ]
    )
    shard_in, shard_out = (
        lax.psum_scatter(
            grad_in.astype(jnp.bfloat16), "head", scatter_dimension=0, tiled=True
        ).astype(jnp.float32),
        lax.psum_scatter(
            grad_out.astype(jnp.bfloat16), "head", scatter_dimension=0, tiled=True
        ).astype(jnp.float32),
    )
    summed_in, summed_out = lax.psum((shard_in, shard_out), ("dp", "ctx"))
    summed_vec = lax.psum(grad_vec, ("dp", "head", "ctx"))
    in_moment_new, in_second_new, in_master_new = adam_update(
        in_master, in_moment, in_second, summed_in, matrix_rate, weight_decay
    )
    out_moment_new, out_second_new, out_master_new = adam_update(
        out_master, out_moment, out_second, summed_out, matrix_rate, weight_decay
    )
    vec_moment_new, vec_second_new, vec_master_new = adam_update(
        vec_master, vec_moment, vec_second, summed_vec, vector_rate, 0.0
    )
    return (
        output,
        input_grad,
        in_moment_new,
        in_second_new,
        in_master_new,
        in_master_new.astype(jnp.bfloat16),
        out_moment_new,
        out_second_new,
        out_master_new,
        out_master_new.astype(jnp.bfloat16),
        vec_moment_new,
        vec_second_new,
        vec_master_new,
    )


MESH = pl.DeviceIdType.MESH
F32 = jnp.float32
BF16 = jnp.bfloat16
HALF_HEADS = HEADS // 2
VMEM_LIMIT = 60 * 1024 * 1024
BACK_LIMIT = 67000000


def vmem_specs(count):
    return [pl.BlockSpec(memory_space=pltpu.VMEM)] * count


def places():
    z = lax.axis_index("head")
    q = lax.axis_index("dp")
    c = lax.axis_index("ctx")
    qx = lax.rem(q, 2)
    qy = q // 2
    return z, q, c, qx, qy, qy * 2 + 1 - qx, (1 - qy) * 2 + qx


def greet(partners):
    barrier = pltpu.get_barrier_semaphore()
    for partner in partners:
        pl.semaphore_signal(barrier, inc=1, device_id=partner, device_id_type=MESH)
    pl.semaphore_wait(barrier, len(partners))


def remote(source, target, send_sem, recv_sem, device):
    return pltpu.make_async_remote_copy(
        src_ref=source,
        dst_ref=target,
        send_sem=send_sem,
        recv_sem=recv_sem,
        device_id=device,
        device_id_type=MESH,
    )


KV_END = D + 2 * HEAD_DIM
HALF_D = D // 2


def hidden_spans(core, ff, row_share):
    spans = []
    for owner in range((D + ff) // row_share):
        first = max(owner * row_share - D, 0)
        last = (owner + 1) * row_share - D
        if last > first:
            half = (last - first) // 2
            spans.append((first + core * half, half))
    return spans


def core_columns(array, core, ff, row_share):
    pieces = [array[..., core * HALF_D : (core + 1) * HALF_D], array[..., D:KV_END]]
    pieces += [
        array[..., KV_END + first : KV_END + first + size]
        for first, size in hidden_spans(core, ff, row_share)
    ]
    return jnp.concatenate(pieces, axis=-1)


def join_columns(pair, ff, row_share):
    pieces = [pair[0][..., :HALF_D], pair[1][..., :HALF_D], pair[0][..., HALF_D : HALF_D + 2 * HEAD_DIM]]
    at = HALF_D + 2 * HEAD_DIM
    for _, size in hidden_spans(0, ff, row_share):
        pieces += [pair[0][..., at : at + size], pair[1][..., at : at + size]]
        at += size
    return jnp.concatenate(pieces, axis=-1)


CHUNK = 512
IN_ROWS = 48
OUT_ROWS = 120


def core_bias(vec, c, first, last):
    ff = vec.shape[1] - 5 * D - KV_END
    share = (D + ff) // 4
    tail = vec[:, 5 * D :]
    return jnp.where(
        c == 0, core_columns(tail, 0, ff, share), core_columns(tail, 1, ff, share)
    )[:, first:last]


def front_kernel(
    in_master,
    out_master,
    tok,
    cot,
    vec,
    cos_ref,
    sin_ref,
    full_in,
    full_out,
    all_tok,
    all_cot,
    norm_one,
    norm_two,
    att_ref,
    dq_ref,
    dkv_ref,
    q_all,
    g_all,
    kv_all,
    keys,
    values,
    weights,
    tops,
    dkeys,
    dvalues,
    z_send,
    z_recv,
    xy_send,
    xy_recv,
    pair_send,
    pair_recv,
    kv_send,
    kv_recv,
    local_sem,
):
    z, q, c, qx, qy, xn, yn = places()
    dg = (1 - qy) * 2 + 1 - qx
    to_x, to_y, to_pair = (xn, z, c), (yn, z, c), (q, z, 1 - c)
    greet([(q, lax.rem(z + k, 4), c) for k in (1, 2, 3)] + [to_x, to_y, to_pair])
    attn_cols = HALF_D + 2 * HEAD_DIM
    groups = ((0, 0, attn_cols), (1, 0, D), (0, attn_cols, full_in.shape[1]))
    full = (full_in, full_out)
    piece_rows = (IN_ROWS, OUT_ROWS)

    def span(group, part):
        which, first, last = groups[group]
        middle = (first + last) // 2
        if part == 1:
            return which, pl.ds(first, middle - first)
        if part == 2:
            return which, pl.ds(middle, last - middle)
        return which, pl.ds(first, last - first)

    def rows_of(which, plane, quarter):
        size = piece_rows[which]
        return pl.ds(pl.multiple_of((plane * 4 + quarter) * size, 8), size)

    def place(group, part, plane, quarter):
        which, cols = span(group, part)
        return full[which].at[rows_of(which, plane, quarter), cols]

    def z_copy(group, plane, way):
        piece = place(group, 0, plane, q)
        return remote(
            piece, piece, z_send.at[group, plane, way], z_recv.at[group, plane], (q, z + 1 - 2 * way, c)
        )

    def z_room(way):
        return z < 3 if way == 0 else z > 0

    def z_start(group):
        for way in range(2):

            @pl.when(z_room(way))
            def _():
                z_copy(group, z, way).start()

    def pair_copy(number):
        source, target = ((tok, all_tok), (cot, all_cot))[number]
        return remote(source, target.at[c], pair_send.at[number], pair_recv.at[number], to_pair)

    for number in range(2):
        pair_copy(number).start()
    locals_ = []
    for number, (source, target) in enumerate(((tok, all_tok.at[c]), (cot, all_cot.at[c]))):
        copy = pltpu.make_async_copy(source, target, local_sem.at[number])
        copy.start()
        locals_.append(copy)

    def xy_copy(path, group, plane):
        quarter = (q, q, xn, yn)[path]
        piece = place(group, (0, 0, 1, 2)[path], plane, quarter)
        return remote(
            piece,
            piece,
            xy_send.at[path, group, plane],
            xy_recv.at[path, group, plane],
            (to_x, to_y, to_y, to_x)[path],
        )

    def xy_landed(path, group, plane):
        quarter = (xn, yn, dg, dg)[path]
        piece = place(group, (0, 0, 1, 2)[path], plane, quarter)
        remote(
            piece, piece, xy_send.at[path, group, plane], xy_recv.at[path, group, plane], to_pair
        ).wait_recv()

    row_share = out_master.shape[0]
    ff = in_master.shape[1] - KV_END
    for quarter in range(4):
        block = in_master[quarter * IN_ROWS : (quarter + 1) * IN_ROWS, :]
        full_in[rows_of(0, z, quarter), :] = jnp.where(
            c == 0, core_columns(block, 0, ff, row_share), core_columns(block, 1, ff, row_share)
        ).astype(BF16)
    z_start(0)
    half_share = row_share // 2
    begin = jnp.where(z == 0, HALF_D * c, half_share * c)
    begin_tail = jnp.where(z == 0, D + (half_share - HALF_D) * c, half_share * c + HALF_D)
    base_row = pl.multiple_of(z * half_share, 16)
    full_out[pl.ds(base_row, HALF_D), :] = out_master[
        pl.ds(pl.multiple_of(begin, 8), HALF_D), :
    ].astype(BF16)
    full_out[pl.ds(pl.multiple_of(base_row + HALF_D, 16), half_share - HALF_D), :] = out_master[
        pl.ds(pl.multiple_of(begin_tail, 8), half_share - HALF_D), :
    ].astype(BF16)
    z_start(1)
    z_start(2)

    def spread(group, far):
        for way in range(2):
            plane = z - far if way == 0 else z + far

            @pl.when(plane >= 0 if way == 0 else plane < 4)
            def _():
                piece = place(group, 0, plane, q)
                remote(
                    piece, piece, z_send.at[group, plane, way], z_recv.at[group, plane], to_pair
                ).wait_recv()

                @pl.when(z_room(way))
                def _():
                    z_copy(group, plane, way).start()

                xy_copy(0, group, plane).start()
                xy_copy(1, group, plane).start()

    def either(far, work):
        for way in range(2):
            plane = z - far if way == 0 else z + far

            @pl.when(plane >= 0 if way == 0 else plane < 4)
            def _():
                work(plane)

    def relay(group, far):
        def work(plane):
            xy_landed(0, group, plane)
            xy_copy(2, group, plane).start()
            xy_landed(1, group, plane)
            xy_copy(3, group, plane).start()

        either(far, work)

    def settle(group):
        def work(plane):
            xy_landed(2, group, plane)
            xy_landed(3, group, plane)

        for far in (1, 2, 3):
            either(far, work)

    rows = tok.shape[0]

    def normalize(half):
        inputs = all_tok[half].astype(F32)
        center = inputs - jnp.mean(inputs, axis=-1, keepdims=True)
        inverse = lax.rsqrt(jnp.mean(center * center, axis=-1, keepdims=True) + 1e-05)
        normed = center * inverse
        here = pl.ds(pl.multiple_of(half * rows, rows), rows)
        norm_one[here, :] = (normed * vec[:, :D] + vec[:, D : 2 * D]).astype(BF16)
        norm_two[here, :] = (normed * vec[:, 2 * D : 3 * D] + vec[:, 3 * D : 4 * D]).astype(BF16)

    for copy in locals_:
        copy.wait()
    normalize(c)
    spread(0, 1)
    for number, target in enumerate((all_tok, all_cot)):
        piece = target.at[1 - c]
        remote(piece, piece, pair_send.at[number], pair_recv.at[number], to_pair).wait_recv()
    normalize(1 - c)
    spread(0, 2)
    relay(0, 1)
    spread(0, 3)
    relay(0, 2)
    spread(1, 1)
    relay(0, 3)
    settle(0)

    half_rot = ROT // 2
    cosine, sine = cos_ref[...], sin_ref[...]

    def turn(block, cosine, sine):
        front, back = block[:half_rot], block[half_rot:ROT]
        return jnp.concatenate(
            [front * cosine - back * sine, back * cosine + front * sine, block[ROT:]], axis=0
        )

    projected = (
        jnp.dot(norm_one[...], full_in[:, :attn_cols], preferred_element_type=F32)
        + core_bias(vec, c, 0, attn_cols)
    ).T
    key_t = turn(projected[HALF_D : HALF_D + HEAD_DIM], cosine, sine)
    kv_all[z] = jnp.concatenate([key_t, projected[HALF_D + HEAD_DIM :]], axis=0).astype(BF16)

    def kv_copy(k):
        return remote(
            kv_all.at[z], kv_all.at[z], kv_send.at[0, k], kv_recv.at[0, k], (q, lax.rem(z + k, 4), c)
        )

    for k in (1, 2, 3):

        @pl.when(z + k < 4)
        def _():
            kv_copy(k).start()

    for head in range(HALF_HEADS):
        block = turn(projected[head * HEAD_DIM : (head + 1) * HEAD_DIM], cosine, sine) * 0.125
        q_all[:, head * CHUNK : (head + 1) * CHUNK] = block.astype(BF16)
    spread(1, 2)
    dkeys[...] = jnp.zeros_like(dkeys)
    dvalues[...] = jnp.zeros_like(dvalues)

    def spread_block(index):
        place_rows = pl.ds(pl.multiple_of(index * CHUNK, CHUNK), CHUNK)
        turned = kv_all[index].astype(F32).T.astype(BF16)
        keys[place_rows, :] = turned[:, :HEAD_DIM]
        values[place_rows, :] = turned[:, HEAD_DIM:]

    spread_block(z)
    relay(1, 1)
    for k in (1, 2, 3):

        @pl.when(z - k >= 0)
        def _():
            source = lax.rem(z + 4 - k, 4)
            remote(
                kv_all.at[source], kv_all.at[source], kv_send.at[0, k], kv_recv.at[0, k], to_pair
            ).wait_recv()
            spread_block(source)

    width = 2 * CHUNK
    cos_two = jnp.concatenate([cosine, cosine], axis=1)
    sin_two = jnp.concatenate([sine, sine], axis=1)
    polls = {
        (0, 0, 0): ((spread, 1, 3),),
        (0, 0, 1): ((relay, 1, 2),),
        (0, 0, 3): ((spread, 2, 1),),
        (0, 1, 0): ((spread, 2, 2),),
        (0, 1, 2): ((relay, 2, 1), (spread, 2, 3)),
        (1, 0, 1): ((relay, 2, 2),),
        (1, 1, 0): ((relay, 2, 3),),
    }

    def poll(pair, late, index):
        for (number, phase, chunk), work in polls.items():
            if phase == late:

                @pl.when(jnp.logical_and(pair == number, index == chunk))
                def _():
                    for action, group, far in work:
                        action(group, far)

    def upstream_heads():
        relay(1, 3)
        settle(1)
        for head in range(HALF_HEADS):
            part = full_out[pl.ds(head * HEAD_DIM, HEAD_DIM), :]
            for half in range(2):
                g_all[:, pl.ds(head * CHUNK + half * rows, rows)] = lax.dot_general(
                    part, all_cot[half], contract_cols, preferred_element_type=F32
                ).astype(BF16)

    def two_heads(pair, carry):
        cols = pl.ds(pl.multiple_of(pair * width, width), width)
        queries = q_all[:, cols]

        def rows_at(index):
            return pl.ds(pl.multiple_of(index * CHUNK, CHUNK), CHUNK)

        def forward(index, state, diagonal):
            top, total, out = state
            part = jnp.dot(keys[rows_at(index), :], queries, preferred_element_type=F32)
            if diagonal:
                key_place = lax.broadcasted_iota(jnp.int32, (CHUNK, width), 0)
                row_place = lax.rem(lax.broadcasted_iota(jnp.int32, (CHUNK, width), 1), CHUNK)
                part = jnp.where(key_place > row_place, neg_fill, part)
            above = jnp.maximum(top, jnp.max(part, axis=0, keepdims=True))
            part = jnp.exp(part - above)
            rounded = part.astype(BF16)
            weights[rows_at(index), :] = rounded
            tops[index] = above
            scale = jnp.exp(top - above)
            total = total * scale + jnp.sum(part, axis=0, keepdims=True)
            out = out * scale + jnp.dot(
                kv_all[index, HEAD_DIM:, :], rounded, preferred_element_type=F32
            )
            return above, total, out

        state = (
            jnp.full((1, width), neg_fill, F32),
            jnp.zeros((1, width), F32),
            jnp.zeros((HEAD_DIM, width), F32),
        )

        def forward_or_not(index, state):
            poll(pair, 0, index)
            return lax.cond(
                index < z, lambda old: forward(index, old, False), lambda old: old, state
            )

        state = lax.fori_loop(0, 4, forward_or_not, state)
        top, total, out = forward(z, state, True)
        inverse = 1.0 / total
        out = out * inverse
        base = pl.multiple_of(pair * 2 * HEAD_DIM, 2 * HEAD_DIM)
        second = pl.multiple_of(base + HEAD_DIM, HEAD_DIM)
        att_ref[pl.ds(base, HEAD_DIM), :] = out[:, :CHUNK].astype(BF16)
        att_ref[pl.ds(second, HEAD_DIM), :] = out[:, CHUNK:].astype(BF16)
        pl.when(pair == 0)(upstream_heads)
        grads = g_all[:, cols].astype(F32)
        inner = jnp.sum(grads * out, axis=0, keepdims=True)

        def backward(index, dq):
            here = rows_at(index)
            factor = inverse * jnp.exp(tops[index] - top)
            scaled = (grads * factor).astype(BF16)
            dprob = jnp.dot(values[here, :], scaled, preferred_element_type=F32)
            rounded = weights[here, :]
            dscore = (rounded.astype(F32) * (dprob - inner * factor)).astype(BF16)
            dkeys[here, :] += lax.dot_general(
                dscore, queries, contract_cols, preferred_element_type=F32
            )
            dvalues[here, :] += lax.dot_general(
                rounded, scaled, contract_cols, preferred_element_type=F32
            )
            return dq + jnp.dot(kv_all[index, :HEAD_DIM, :], dscore, preferred_element_type=F32)

        def backward_or_not(index, dq):
            poll(pair, 1, index)
            return lax.cond(index <= z, lambda old: backward(index, old), lambda old: old, dq)

        dq = lax.fori_loop(0, 4, backward_or_not, jnp.zeros((HEAD_DIM, width), F32))
        dq = turn(dq * 0.125, cos_two, -sin_two)
        dq_ref[pl.ds(base, HEAD_DIM), :] = dq[:, :CHUNK].astype(BF16)
        dq_ref[pl.ds(second, HEAD_DIM), :] = dq[:, CHUNK:].astype(BF16)
        return carry

    lax.fori_loop(0, HALF_HEADS // 2, two_heads, 0)

    for index in range(4):
        here = pl.ds(index * CHUNK, CHUNK)
        dkv_ref[index] = jnp.concatenate([dkeys[here, :], dvalues[here, :]], axis=1)
    settle(2)
    for number in range(2):
        pair_copy(number).wait_send()
    for k in (1, 2, 3):

        @pl.when(z + k < 4)
        def _():
            kv_copy(k).wait_send()

    for group in range(3):
        for way in range(2):

            @pl.when(z_room(way))
            def _():
                z_copy(group, z, way).wait_send()

                for far in (1, 2, 3):
                    plane = z - far if way == 0 else z + far

                    @pl.when(plane >= 0 if way == 0 else plane < 4)
                    def _():
                        z_copy(group, plane, way).wait_send()

        for plane in range(4):

            @pl.when(z != plane)
            def _():
                for path in range(4):
                    xy_copy(path, group, plane).wait_send()


def front(in_master, out_master, tok, cot, vec, cosine, sine):
    rows, width = tok.shape
    core_cols = (in_master.shape[1] + 2 * HEAD_DIM) // 2
    chip_rows = 2 * rows
    dma = pltpu.SemaphoreType.DMA
    return pl.pallas_call(
        front_kernel,
        out_shape=(
            jax.ShapeDtypeStruct((4 * in_master.shape[0], core_cols), BF16),
            jax.ShapeDtypeStruct((2 * out_master.shape[0], width), BF16),
            jax.ShapeDtypeStruct((2, rows, width), BF16),
            jax.ShapeDtypeStruct((2, rows, width), BF16),
            jax.ShapeDtypeStruct((chip_rows, width), BF16),
            jax.ShapeDtypeStruct((chip_rows, width), BF16),
            jax.ShapeDtypeStruct((HALF_D, chip_rows), BF16),
            jax.ShapeDtypeStruct((HALF_D, chip_rows), BF16),
            jax.ShapeDtypeStruct((4, chip_rows, 2 * HEAD_DIM), F32),
        ),
        in_specs=vmem_specs(7),
        out_specs=vmem_specs(9),
        scratch_shapes=[
            pltpu.VMEM((HEAD_DIM, HALF_HEADS * CHUNK), BF16),
            pltpu.VMEM((HEAD_DIM, HALF_HEADS * CHUNK), BF16),
            pltpu.VMEM((4, 2 * HEAD_DIM, CHUNK), BF16),
            pltpu.VMEM((4 * CHUNK, HEAD_DIM), BF16),
            pltpu.VMEM((4 * CHUNK, HEAD_DIM), BF16),
            pltpu.VMEM((4 * CHUNK, 2 * CHUNK), BF16),
            pltpu.VMEM((4, 1, 2 * CHUNK), F32),
            pltpu.VMEM((4 * CHUNK, HEAD_DIM), F32),
            pltpu.VMEM((4 * CHUNK, HEAD_DIM), F32),
            dma((3, 4, 2)),
            dma((3, 4)),
            dma((4, 3, 4)),
            dma((4, 3, 4)),
            dma((2,)),
            dma((2,)),
            dma((1, 4)),
            dma((1, 4)),
            dma((2,)),
        ],
        compiler_params=pltpu.CompilerParams(
            collective_id=0, has_side_effects=True, vmem_limit_bytes=VMEM_LIMIT
        ),
        name="front",
    )(in_master, out_master, tok, cot, vec, cosine, sine)


PLANE_ORDER = (2, 1, 3, 0)
HIDDEN_BLOCK = 512
ROOT_HALF = 0.7071067811865476
GAUSS = 0.3989422804014327


def back_kernel(
    full_in,
    full_out,
    all_tok,
    all_cot,
    norm_one,
    norm_two,
    att_ref,
    dq_ref,
    dkv_part,
    vec_ref,
    cos_ref,
    sin_ref,
    output_ref,
    input_grad_ref,
    sum_in,
    sum_out,
    vec_sum,
    one_t,
    two_t,
    act,
    slope,
    dhid,
    branch_t,
    qkv_grad,
    partial_out,
    upstream,
    out_other,
    up_other,
    g_in,
    g_out,
    x_in,
    x_out,
    y_in,
    y_out,
    ax_in,
    ax_out,
    ay_in,
    ay_out,
    bx_in,
    bx_out,
    by_in,
    by_out,
    t_in,
    t_out,
    z_in,
    z_out,
    own_in,
    own_out,
    vec_send,
    vec_recv,
    vec_zone,
    pair_in,
    summed,
    zone,
    dkv,
    send_sem,
    recv_sem,
    vec_send_sem,
    vec_recv_sem,
    last_send_sem,
    last_recv_sem,
    pair_send_sem,
    pair_recv_sem,
    part_send_sem,
    part_recv_sem,
    zone_send_sem,
    zone_recv_sem,
):
    z, q, c, qx, qy, xn, yn = places()
    dg = (1 - qy) * 2 + 1 - qx
    to_x, to_y, to_pair = (xn, z, c), (yn, z, c), (q, z, 1 - c)
    greet([(q, lax.rem(z + k, 4), c) for k in (1, 2, 3)] + [to_x, to_y, to_pair])
    sent = []

    def send(source, target, sems, index, device):
        copy = remote(source, target, sems[0].at[index], sems[1].at[index], device)
        copy.start()
        sent.append(copy)

    def landed(target, sems, index):
        remote(target, target, sems[0].at[index], sems[1].at[index], to_pair).wait_recv()

    main = (send_sem, recv_sem)
    vecs = (vec_send_sem, vec_recv_sem)
    lasts = (last_send_sem, last_recv_sem)
    pairs = (pair_send_sem, pair_recv_sem)
    parts = (part_send_sem, part_recv_sem)
    grads = (g_in, g_out)
    halves = tuple(ref.shape[-1] // 2 for ref in grads)
    first = tuple(pl.ds(0, half) for half in halves)
    second = tuple(pl.ds(half, half) for half in halves)
    from_x, from_y = (x_in, x_out), (y_in, y_out)
    ax, ay, bx, by = (ax_in, ax_out), (ay_in, ay_out), (bx_in, bx_out), (by_in, by_out)
    totals, zones, own = (t_in, t_out), (z_in, z_out), (own_in, own_out)
    outs = (sum_in, sum_out)
    rows = all_tok.shape[1]
    mine = pl.ds(pl.multiple_of(c * rows, rows), rows)
    other = pl.ds(pl.multiple_of((1 - c) * rows, rows), rows)
    attn_cols = HALF_D + 2 * HEAD_DIM
    hidden = full_in.shape[1] - attn_cols

    def plane_of(step):
        return lax.rem(z + PLANE_ORDER[step % 4], 4)

    def kind(step):
        return 1 if step < 4 else 0

    def exchange(step):
        h, a, j = plane_of(step), kind(step), step % 4
        if a == 1:
            size = 4 * OUT_ROWS
            left = branch_t[pl.ds(pl.multiple_of(h * size, 16), size), :]
            for half in range(2):
                cols = pl.ds(half * halves[1], halves[1])
                block = sum(
                    jnp.dot(
                        left[:, k * rows : (k + 1) * rows],
                        all_cot[k, :, cols],
                        preferred_element_type=F32,
                    )
                    for k in range(2)
                ).astype(BF16)
                for quarter in range(4):
                    g_out[h, quarter // 2, quarter % 2, :, cols] = block[
                        quarter * OUT_ROWS : (quarter + 1) * OUT_ROWS
                    ]
        else:
            size = 4 * IN_ROWS
            here = pl.ds(pl.multiple_of(h * size, 16), size)
            for number in range(4):
                cols = pl.ds(number * HIDDEN_BLOCK, HIDDEN_BLOCK)
                if number == 0:
                    block = jnp.dot(one_t[here, :], qkv_grad[...], preferred_element_type=F32)
                else:
                    block = jnp.dot(
                        two_t[here, :],
                        dhid[:, pl.ds((number - 1) * HIDDEN_BLOCK, HIDDEN_BLOCK)],
                        preferred_element_type=F32,
                    )
                block = block.astype(BF16)
                for quarter in range(4):
                    g_in[h, quarter // 2, quarter % 2, :, cols] = block[
                        quarter * IN_ROWS : (quarter + 1) * IN_ROWS
                    ]
        send(grads[a].at[h, :, 1 - qx, :, first[a]], from_x[a].at[j], main, (j, 0, a), to_x)
        send(grads[a].at[h, 1 - qy, :, :, second[a]], from_y[a].at[j], main, (j, 1, a), to_y)

    def halve(step):
        h, a, j = plane_of(step), kind(step), step % 4
        landed(from_x[a].at[j], main, (j, 0, a))
        ax[a][j] = (
            grads[a][h, 1 - qy, qx, :, first[a]].astype(F32) + from_x[a][j, 1 - qy].astype(F32)
        ).astype(BF16)
        send(ax[a].at[j], ay[a].at[j], main, (j, 2, a), to_y)
        landed(from_y[a].at[j], main, (j, 1, a))
        bx[a][j] = (
            grads[a][h, qy, 1 - qx, :, second[a]].astype(F32) + from_y[a][j, 1 - qx].astype(F32)
        ).astype(BF16)
        send(bx[a].at[j], by[a].at[j], main, (j, 3, a), to_x)

    def finish(step):
        h, a, j = plane_of(step), kind(step), step % 4
        shift = PLANE_ORDER[j]
        landed(ay[a].at[j], main, (j, 2, a))
        left = (
            grads[a][h, qy, qx, :, first[a]].astype(F32)
            + from_x[a][j, qy].astype(F32)
            + ay[a][j].astype(F32)
        )
        landed(by[a].at[j], main, (j, 3, a))
        right = (
            grads[a][h, qy, qx, :, second[a]].astype(F32)
            + from_y[a][j, qx].astype(F32)
            + by[a][j].astype(F32)
        )
        if shift == 0:
            own[a][:, first[a]] = left
            own[a][:, second[a]] = right
        else:
            totals[a][shift - 1, :, first[a]] = left.astype(BF16)
            totals[a][shift - 1, :, second[a]] = right.astype(BF16)
            send(totals[a].at[shift - 1], zones[a].at[shift - 1], main, (j, 4, a), (q, h, c))

    def share(a):
        for j in range(3):
            landed(zones[a].at[PLANE_ORDER[j] - 1], main, (j, 4, a))
        whole = own[a][...] + zones[a][0].astype(F32) + zones[a][1].astype(F32) + zones[a][2].astype(F32)
        outs[a][c, q] = whole.astype(BF16)
        piece = outs[a].at[c, q]
        send(piece, piece, lasts, (0, a), to_x)
        send(piece, piece, lasts, (1, a), to_y)
        send(piece, piece, pairs, (0, a), to_pair)

    def pass_on(a):
        piece = outs[a].at[c, xn]
        landed(piece, lasts, (0, a))
        part = outs[a].at[c, xn, :, first[a]]
        send(part, part, lasts, (2, a), to_y)
        send(piece, piece, pairs, (1, a), to_pair)
        piece = outs[a].at[c, yn]
        landed(piece, lasts, (1, a))
        part = outs[a].at[c, yn, :, second[a]]
        send(part, part, lasts, (3, a), to_x)
        send(piece, piece, pairs, (2, a), to_pair)

    def close(a):
        landed(outs[a].at[c, dg, :, first[a]], lasts, (2, a))
        landed(outs[a].at[c, dg, :, second[a]], lasts, (3, a))
        piece = outs[a].at[c, dg]
        send(piece, piece, pairs, (3, a), to_pair)

    def zone_copy(k):
        target = lax.rem(z + 4 - k, 4)
        return remote(
            summed.at[target],
            zone.at[k - 1],
            zone_send_sem.at[k],
            zone_recv_sem.at[k],
            (q, target, c),
        )

    send(dkv_part.at[:, other, :], pair_in, parts, 0, to_pair)

    branch_t[pl.ds(0, HALF_D), :] = att_ref[...]
    bias_up = core_bias(vec_ref, c, attn_cols, attn_cols + hidden)
    for number in range(hidden // HIDDEN_BLOCK):
        cols = pl.ds(number * HIDDEN_BLOCK, HIDDEN_BLOCK)
        before = (
            jnp.dot(
                norm_two[...],
                full_in[:, pl.ds(attn_cols + number * HIDDEN_BLOCK, HIDDEN_BLOCK)],
                preferred_element_type=F32,
            )
            + bias_up[:, number * HIDDEN_BLOCK : (number + 1) * HIDDEN_BLOCK]
        )
        normal = 0.5 * (1.0 + lax.erf(before * ROOT_HALF))
        active = before * normal
        act[:, cols] = active.astype(BF16)
        slope[:, cols] = normal + before * (GAUSS * jnp.exp(-0.5 * before * before))
        branch_t[pl.ds(HALF_D + number * HIDDEN_BLOCK, HIDDEN_BLOCK), :] = active.T.astype(BF16)
    exchange(0)
    exchange(1)
    landed(pair_in, parts, 0)
    for index in range(4):
        summed[index] = dkv_part[index, mine, :] + pair_in[index]
    for k in (1, 2, 3):

        @pl.when(z - k >= 0)
        def _():
            zone_copy(k).start()

    one_t[...] = norm_one[...].astype(F32).T.astype(BF16)
    two_t[...] = norm_two[...].astype(F32).T.astype(BF16)
    for number in range(hidden // HIDDEN_BLOCK):
        cols = pl.ds(number * HIDDEN_BLOCK, HIDDEN_BLOCK)
        for k in range(2):
            here = pl.ds(k * rows, rows)
            back = lax.dot_general(
                all_cot[k],
                full_out[pl.ds(HALF_D + number * HIDDEN_BLOCK, HIDDEN_BLOCK), :],
                contract_cols,
                preferred_element_type=F32,
            )
            dhid[here, cols] = (back * slope[here, cols]).astype(BF16)
    halve(0)
    exchange(2)
    dkv[mine, :] = summed[z]
    for k in (1, 2, 3):

        @pl.when(z + k < 4)
        def _():
            remote(
                zone.at[k - 1], zone.at[k - 1], zone_send_sem.at[k], zone_recv_sem.at[k], to_pair
            ).wait_recv()
            dkv[mine, :] += zone[k - 1]

    send(dkv.at[mine, :], dkv.at[mine, :], parts, 1, to_pair)
    halve(1)
    exchange(3)
    finish(0)
    partial_out[...] = jnp.dot(
        att_ref[...].astype(F32).T.astype(BF16), full_out[:HALF_D, :], preferred_element_type=F32
    ) + jnp.dot(act[...], full_out[pl.ds(HALF_D, hidden), :], preferred_element_type=F32)
    send(partial_out.at[other, :], out_other, parts, 2, to_pair)
    landed(dkv.at[other, :], parts, 1)
    half_rot = ROT // 2
    turned = dkv[...].T
    front_part, back_part = turned[:half_rot], turned[half_rot:ROT]
    cosine, sine = cos_ref[...], sin_ref[...]
    turned = jnp.concatenate(
        [
            front_part * cosine + back_part * sine,
            back_part * cosine - front_part * sine,
            turned[ROT:],
        ],
        axis=0,
    )
    qkv_grad[:, :HALF_D] = dq_ref[...].astype(F32).T.astype(BF16)
    qkv_grad[:, HALF_D:] = turned.T.astype(BF16)
    halve(2)
    exchange(4)
    finish(1)
    keep = jnp.where(c == 0, 1.0, 0.0)
    vec_send[...] = jnp.zeros_like(vec_send)
    mine_vec = vec_send.at[0]
    column = lax.broadcasted_iota(jnp.int32, (1, attn_cols), 1)
    once = jnp.where(column < HALF_D, 1.0, keep)
    first_rows = jnp.zeros((1, D), F32)
    sums = [first_rows] * 4
    for k in range(2):
        here = pl.ds(k * rows, rows)
        inputs = all_tok[k].astype(F32)
        center = inputs - jnp.mean(inputs, axis=-1, keepdims=True)
        inverse = lax.rsqrt(jnp.mean(center * center, axis=-1, keepdims=True) + 1e-05)
        normed = center * inverse
        masked = (qkv_grad[here, :].astype(F32) * once).astype(BF16)
        one = lax.dot_general(
            masked, full_in[:, :attn_cols], contract_cols, preferred_element_type=F32
        )
        two = lax.dot_general(
            dhid[here, :],
            full_in[:, pl.ds(attn_cols, hidden)],
            contract_cols,
            preferred_element_type=F32,
        )
        terms = (one * normed, one, two * normed, two)
        sums = [old + jnp.sum(term, axis=0, keepdims=True) for old, term in zip(sums, terms)]
        upstream[here, :] = one * vec_ref[:, :D] + two * vec_ref[:, 2 * D : 3 * D]
    send(upstream.at[other, :], up_other, parts, 3, to_pair)
    halve(3)
    exchange(5)
    finish(2)
    for number in range(4):
        mine_vec[number : number + 1, :D] = sums[number]
    mine_vec[4:5, :D] = jnp.sum(all_cot[c].astype(F32), axis=0, keepdims=True)
    query_sums = jnp.sum(qkv_grad[...].astype(F32), axis=0, keepdims=True) * once
    hidden_sums = [
        jnp.sum(
            dhid[:, pl.ds(number * HIDDEN_BLOCK, HIDDEN_BLOCK)].astype(F32), axis=0, keepdims=True
        )
        for number in range(hidden // HIDDEN_BLOCK)
    ]
    for core in range(2):
        for number, piece in enumerate([query_sums] + hidden_sums):
            row = 4 * core + number
            mine_vec[row : row + 1, D:] = jnp.where(c == core, piece, 0.0)
    send(vec_send.at[0], vec_recv.at[0], vecs, 0, to_x)
    halve(4)
    exchange(6)
    finish(3)
    landed(vec_recv.at[0], vecs, 0)
    vec_send[1] = vec_send[0] + vec_recv[0]
    send(vec_send.at[1], vec_recv.at[1], vecs, 1, to_y)
    halve(5)
    exchange(7)
    finish(4)
    share(1)
    landed(vec_recv.at[1], vecs, 1)
    vec_send[2] = vec_send[1] + vec_recv[1]
    send(vec_send.at[2], vec_recv.at[2], vecs, 2, to_pair)
    halve(6)
    finish(5)
    pass_on(1)
    landed(vec_recv.at[2], vecs, 2)
    vec_send[3] = vec_send[2] + vec_recv[2]
    vec_zone[z] = vec_send[3]
    for k in (1, 2, 3):
        send(vec_send.at[3], vec_zone.at[z], vecs, 2 + k, (q, lax.rem(z + k, 4), c))
    halve(7)
    finish(6)
    close(1)
    landed(out_other, parts, 2)
    output_ref[...] = (
        all_tok[c].astype(F32) + (partial_out[mine, :] + out_other[...]) + vec_ref[:, 4 * D : 5 * D]
    ).astype(BF16)
    landed(up_other, parts, 3)
    inputs = all_tok[c].astype(F32)
    center = inputs - jnp.mean(inputs, axis=-1, keepdims=True)
    inverse = lax.rsqrt(jnp.mean(center * center, axis=-1, keepdims=True) + 1e-05)
    normed = center * inverse
    total = upstream[mine, :] + up_other[...]
    inside = (
        total
        - jnp.mean(total, axis=-1, keepdims=True)
        - normed * jnp.mean(total * normed, axis=-1, keepdims=True)
    )
    finish(7)
    share(0)
    input_grad_ref[...] = (all_cot[c].astype(F32) + inverse * inside).astype(BF16)
    pass_on(0)
    for k in (1, 2, 3):
        landed(vec_zone.at[lax.rem(z + 4 - k, 4)], vecs, 2 + k)
    vec_sum[...] = (vec_zone[0] + vec_zone[1]) + (vec_zone[2] + vec_zone[3])
    close(0)
    for a in (1, 0):
        for index, quarter in enumerate((q, xn, yn, dg)):
            landed(outs[a].at[1 - c, quarter], pairs, (index, a))
    for copy in sent:
        copy.wait_send()
    for k in (1, 2, 3):

        @pl.when(z - k >= 0)
        def _():
            zone_copy(k).wait_send()


def back(full_in, full_out, all_tok, all_cot, norm_one, norm_two, att_t, dq_t, dkv, vec, cosine, sine):
    rows = all_tok.shape[1]
    chip_rows = 2 * rows
    cols_in, cols_out = full_in.shape[1], full_out.shape[1]
    hidden = cols_in - HALF_D - 2 * HEAD_DIM
    kv_width = 2 * HEAD_DIM
    vec_shape = (8, D + HALF_D + kv_width)
    dma = pltpu.SemaphoreType.DMA

    def both(lead, cut, kind):
        return [
            pltpu.VMEM(lead + (IN_ROWS, cols_in // cut), kind),
            pltpu.VMEM(lead + (OUT_ROWS, cols_out // cut), kind),
        ]

    def twice(*shape):
        return [dma(shape), dma(shape)]

    return pl.pallas_call(
        back_kernel,
        out_shape=(
            jax.ShapeDtypeStruct((rows, D), BF16),
            jax.ShapeDtypeStruct((rows, D), BF16),
            jax.ShapeDtypeStruct((2, 4, IN_ROWS, cols_in), BF16),
            jax.ShapeDtypeStruct((2, 4, OUT_ROWS, cols_out), BF16),
            jax.ShapeDtypeStruct(vec_shape, F32),
        ),
        in_specs=vmem_specs(12),
        out_specs=vmem_specs(5),
        scratch_shapes=[
            pltpu.VMEM((D, chip_rows), BF16),
            pltpu.VMEM((D, chip_rows), BF16),
            pltpu.VMEM((chip_rows, hidden), BF16),
            pltpu.VMEM((chip_rows, hidden), F32),
            pltpu.VMEM((chip_rows, hidden), BF16),
            pltpu.VMEM((HALF_D + hidden, chip_rows), BF16),
            pltpu.VMEM((chip_rows, HALF_D + kv_width), BF16),
            pltpu.VMEM((chip_rows, D), F32),
            pltpu.VMEM((chip_rows, D), F32),
            pltpu.VMEM((rows, D), F32),
            pltpu.VMEM((rows, D), F32),
        ]
        + both((4, 2, 2), 1, BF16)
        + both((4, 2), 2, BF16)
        + both((4, 2), 2, BF16)
        + both((4,), 2, BF16) * 4
        + both((3,), 1, BF16) * 2
        + both((), 1, F32)
        + [
            pltpu.VMEM((4,) + vec_shape, F32),
            pltpu.VMEM((3,) + vec_shape, F32),
            pltpu.VMEM((4,) + vec_shape, F32),
            pltpu.VMEM((4, rows, kv_width), F32),
            pltpu.VMEM((4, rows, kv_width), F32),
            pltpu.VMEM((3, rows, kv_width), F32),
            pltpu.VMEM((chip_rows, kv_width), F32),
        ]
        + twice(4, 5, 2)
        + twice(6)
        + twice(4, 2)
        + twice(4, 2)
        + twice(4)
        + twice(4),
        compiler_params=pltpu.CompilerParams(
            collective_id=1, has_side_effects=True, vmem_limit_bytes=BACK_LIMIT
        ),
        name="back",
    )(full_in, full_out, all_tok, all_cot, norm_one, norm_two, att_t, dq_t, dkv, vec, cosine, sine)


ADAM_ROWS = 32
ADAM_OUT_ROWS = 96


def adam_in_kernel(
    grad, master, moment, second, grad_vec, vec, vec_moment, vec_second, m_new, s_new, w_new, copy, vm, vs, vw
):
    ff = master.shape[1] - KV_END
    share = (D + ff) // 4
    joined = join_columns((grad[0].astype(F32), grad[1].astype(F32)), ff, share)
    first, new_second, weights = adam_update(
        master[...], moment[...], second[...], joined, matrix_rate, weight_decay
    )
    m_new[...] = first
    s_new[...] = new_second
    w_new[...] = weights
    copy[...] = weights.astype(BF16)

    @pl.when(pl.program_id(0) == 0)
    def _():
        cores = [
            jnp.concatenate([grad_vec[4 * core + row : 4 * core + row + 1, D:] for row in range(4)], axis=1)
            for core in range(2)
        ]
        whole = jnp.concatenate(
            [grad_vec[row : row + 1, :D] for row in range(5)] + [join_columns(cores, ff, share)], axis=1
        )
        vm[...], vs[...], vw[...] = adam_update(
            vec[...], vec_moment[...], vec_second[...], whole, vector_rate, 0.0
        )


def adam_in(grad, master, moment, second, grad_vec, vec, vec_moment, vec_second):
    rows, cols = master.shape
    block = pl.BlockSpec((ADAM_ROWS, cols), lambda i: (i, 0))
    still = pl.BlockSpec(vec.shape, lambda i: (0, 0))
    shape = jax.ShapeDtypeStruct((rows, cols), F32)
    vec_shape = jax.ShapeDtypeStruct(vec.shape, F32)
    return pl.pallas_call(
        adam_in_kernel,
        grid=(rows // ADAM_ROWS,),
        in_specs=[
            pl.BlockSpec((2, ADAM_ROWS, grad.shape[2]), lambda i: (0, i, 0)),
            block,
            block,
            block,
            pl.BlockSpec(grad_vec.shape, lambda i: (0, 0)),
            still,
            still,
            still,
        ],
        out_specs=[block] * 4 + [still] * 3,
        out_shape=[shape] * 3 + [jax.ShapeDtypeStruct((rows, cols), BF16)] + [vec_shape] * 3,
        compiler_params=pltpu.CompilerParams(vmem_limit_bytes=VMEM_LIMIT),
        name="adam_in",
    )(grad, master, moment, second, grad_vec, vec, vec_moment, vec_second)


def adam_out_kernel(place_ref, grad, master, moment, second, m_new, s_new, w_new, copy):
    first, new_second, weights = adam_update(
        master[...], moment[...], second[...], grad[0].astype(F32), matrix_rate, weight_decay
    )
    m_new[...] = first
    s_new[...] = new_second
    w_new[...] = weights
    copy[...] = weights.astype(BF16)


def adam_out(places_of, grad, master, moment, second):
    rows, cols = master.shape
    count = rows // ADAM_OUT_ROWS
    per_core = count // 2
    block = pl.BlockSpec((ADAM_OUT_ROWS, cols), lambda i, table: (table[i], 0))
    shape = jax.ShapeDtypeStruct((rows, cols), F32)
    return pl.pallas_call(
        adam_out_kernel,
        grid_spec=pltpu.PrefetchScalarGridSpec(
            num_scalar_prefetch=1,
            grid=(count,),
            in_specs=[
                pl.BlockSpec(
                    (1, ADAM_OUT_ROWS, cols), lambda i, table: (i // per_core, lax.rem(i, per_core), 0)
                ),
                block,
                block,
                block,
            ],
            out_specs=[block] * 4,
        ),
        out_shape=[shape] * 3 + [jax.ShapeDtypeStruct((rows, cols), BF16)],
        compiler_params=pltpu.CompilerParams(vmem_limit_bytes=VMEM_LIMIT),
        name="adam_out",
    )(places_of, grad, master, moment, second)


def fast_shards(
    tokens,
    cotangent,
    in_master,
    in_moment,
    in_second,
    out_master,
    out_moment,
    out_second,
    vec_master,
    vec_moment,
    vec_second,
    rotary_scale,
):
    z = lax.axis_index("head")
    chip_rows = 2 * tokens.shape[0]
    row_share = out_master.shape[0]
    size = vec_master.shape[0]
    vec, moments, seconds = (array.reshape(1, size) for array in (vec_master, vec_moment, vec_second))
    positions = (z * chip_rows + jnp.arange(chip_rows, dtype=jnp.int32)).astype(F32)
    cosine, sine_table = rotary_tables(positions, rotary_scale[0].astype(F32))
    cosine, sine_table = cosine.T, sine_table.T
    full_in, full_out, all_tok, all_cot, norm_one, norm_two, att_t, dq_t, dkv = front(
        in_master, out_master, tokens, cotangent, vec, cosine, sine_table
    )
    output, input_grad, sum_in, sum_out, sum_vec = back(
        full_in, full_out, all_tok, all_cot, norm_one, norm_two, att_t, dq_t, dkv, vec, cosine, sine_table
    )
    count = row_share // ADAM_OUT_ROWS
    half, attn = count // 2, HALF_D // ADAM_OUT_ROWS
    plain = jnp.arange(count, dtype=jnp.int32)
    core, place = plain // half, plain % half
    first_owner = jnp.where(place < attn, core * attn + place, 2 * attn + core * (half - attn) + place - attn)
    table = jnp.where(z == 0, first_owner, plain)
    out_new = adam_out(table, sum_out.reshape(2, -1, D), out_master, out_moment, out_second)
    in_new = adam_in(
        sum_in.reshape(2, -1, sum_in.shape[-1]),
        in_master,
        in_moment,
        in_second,
        sum_vec,
        vec,
        moments,
        seconds,
    )
    return (
        output,
        input_grad,
        *in_new[:4],
        *out_new,
        *(array.reshape(size) for array in in_new[4:]),
    )


def solution(mesh):
    placed = (
        P(("dp", "head", "ctx"), None),
        P(("dp", "head", "ctx"), None),
        P("head", None),
        P("head", None),
        P("head", None),
        P("head", None),
        P("head", None),
        P("head", None),
        P(),
        P(),
        P(),
        P(),
    )
    paired = dict(mesh.shape) == {"dp": 4, "head": 4, "ctx": 2}
    body = fast_shards if paired else shards
    return jax.shard_map(
        body,
        mesh=mesh,
        in_specs=placed,
        out_specs=(
            P(("dp", "head", "ctx"), None),
            P(("dp", "head", "ctx"), None),
            P("head", None),
            P("head", None),
            P("head", None),
            P("head", None),
            P("head", None),
            P("head", None),
            P("head", None),
            P("head", None),
            P(),
            P(),
            P(),
        ),
        check_vma=False,
    )
```

```python
import jax
import jax.numpy as jnp
from jax import lax
from jax.experimental import pallas as pl
from jax.experimental.pallas import tpu as pltpu
from jax.sharding import PartitionSpec as P

HEADS = 12
HEAD_DIM = 64
ROT = 16
D = 768
KEY_BLOCK = 1024
ADAM_STEP = 3


neg_fill = -1e30
matrix_rate = 0.03
vector_rate = 0.3
weight_decay = 0.1
adam_epsilon = 1e-08
contract_rows = (((0,), (0,)), ((), ()))
contract_cols = (((1,), (1,)), ((), ()))


def layer_norm(values, norm_gain, norm_shift):
    center = values - jnp.mean(values, axis=-1, keepdims=True)
    inverse = lax.rsqrt(jnp.mean(center * center, axis=-1, keepdims=True) + 1e-05)
    normed = center * inverse
    return (normed * norm_gain + norm_shift, normed, inverse)


def norm_back(upstream, normed, inverse, norm_gain):
    scaled = upstream * norm_gain
    inside = (
        scaled
        - jnp.mean(scaled, axis=-1, keepdims=True)
        - normed * jnp.mean(scaled * normed, axis=-1, keepdims=True)
    )
    return (inverse * inside, jnp.sum(upstream * normed, axis=0), jnp.sum(upstream, axis=0))


def rotary_tables(positions, scale_value):
    half_rot = ROT // 2
    frequency = 10000.0 ** (-(2.0 * jnp.arange(half_rot, dtype=jnp.float32)) / ROT)
    angles = (positions / scale_value)[:, None] * frequency[None, :]
    return (jnp.cos(angles), jnp.sin(angles))


def rotate(values, cosine, sine_table):
    half_rot = ROT // 2
    front_half = values[..., :half_rot]
    back_half = values[..., half_rot:ROT]
    return jnp.concatenate(
        [
            front_half * cosine - back_half * sine_table,
            back_half * cosine + front_half * sine_table,
            values[..., ROT:],
        ],
        axis=-1,
    )


def score_block(query_rows, row_pos, whole_kv, block_index):
    key_block = lax.dynamic_slice_in_dim(whole_kv, block_index * KEY_BLOCK, KEY_BLOCK, 0)
    scores = lax.dot_general(
        query_rows, key_block[:, :HEAD_DIM], contract_cols, preferred_element_type=jnp.float32
    )
    key_pos = block_index * KEY_BLOCK + jnp.arange(KEY_BLOCK, dtype=jnp.int32)
    allowed = key_pos[None, :] <= row_pos[:, None]
    return (jnp.where(allowed, scores, neg_fill), allowed, key_block)


def log_totals(query_rows, row_pos, whole_kv):
    row_count = query_rows.shape[0]
    last_pos = jnp.max(row_pos)

    def advance(block_index, state_now):

        def process(state_old):
            run_max, run_sum = state_old
            scores, allowed, key_block = score_block(query_rows, row_pos, whole_kv, block_index)
            new_max = jnp.maximum(run_max, jnp.max(scores, axis=1))
            weights = jnp.where(allowed, jnp.exp(scores - new_max[:, None]), 0.0)
            return (new_max, run_sum * jnp.exp(run_max - new_max) + jnp.sum(weights, axis=1))

        return lax.cond(
            block_index * KEY_BLOCK <= last_pos, process, lambda state_same: state_same, state_now
        )

    start_state = (
        jnp.full((row_count,), neg_fill, jnp.float32),
        jnp.zeros((row_count,), jnp.float32),
    )
    run_max, run_sum = lax.fori_loop(0, whole_kv.shape[0] // KEY_BLOCK, advance, start_state)
    return run_max + jnp.log(run_sum)


def attend(query_rows, row_pos, whole_kv, log_sum):
    last_pos = jnp.max(row_pos)

    def advance(block_index, summed):

        def process(summed_old):
            scores, allowed, key_block = score_block(query_rows, row_pos, whole_kv, block_index)
            probs = jnp.where(allowed, jnp.exp(scores - log_sum[:, None]), 0.0).astype(jnp.bfloat16)
            return summed_old + jnp.dot(
                probs, key_block[:, HEAD_DIM:], preferred_element_type=jnp.float32
            )

        return lax.cond(
            block_index * KEY_BLOCK <= last_pos, process, lambda summed_same: summed_same, summed
        )

    start_state = jnp.zeros((query_rows.shape[0], HEAD_DIM), jnp.float32)
    return lax.fori_loop(0, whole_kv.shape[0] // KEY_BLOCK, advance, start_state)


def attend_back(query_rows, row_pos, whole_kv, log_sum, grad_rows, row_inner):
    last_pos = jnp.max(row_pos)

    def advance(block_index, state_now):

        def process(state_old):
            query_grad, kv_terms = state_old
            scores, allowed, key_block = score_block(query_rows, row_pos, whole_kv, block_index)
            probs = jnp.where(allowed, jnp.exp(scores - log_sum[:, None]), 0.0)
            prob_grad = lax.dot_general(
                grad_rows,
                key_block[:, HEAD_DIM:],
                contract_cols,
                preferred_element_type=jnp.float32,
            )
            score_grad = (probs * (prob_grad - row_inner[:, None])).astype(jnp.bfloat16)
            query_grad = query_grad + jnp.dot(
                score_grad, key_block[:, :HEAD_DIM], preferred_element_type=jnp.float32
            )
            key_grad = lax.dot_general(
                score_grad, query_rows, contract_rows, preferred_element_type=jnp.float32
            )
            value_grad = lax.dot_general(
                probs.astype(jnp.bfloat16),
                grad_rows,
                contract_rows,
                preferred_element_type=jnp.float32,
            )
            kv_terms = lax.dynamic_update_slice_in_dim(
                kv_terms,
                jnp.concatenate([key_grad, value_grad], axis=1),
                block_index * KEY_BLOCK,
                0,
            )
            return (query_grad, kv_terms)

        return lax.cond(
            block_index * KEY_BLOCK <= last_pos, process, lambda state_same: state_same, state_now
        )

    start_state = (
        jnp.zeros((query_rows.shape[0], HEAD_DIM), jnp.float32),
        jnp.zeros((whole_kv.shape[0], 2 * HEAD_DIM), jnp.float32),
    )
    return lax.fori_loop(0, whole_kv.shape[0] // KEY_BLOCK, advance, start_state)


def adam_update(master, moment, second, gradient, step_rate, decay_rate):
    moment_new = 0.5 * moment + 0.5 * gradient
    second_new = 0.5 * second + 0.5 * gradient * gradient
    correction = 1.0 - 0.5**ADAM_STEP
    normalized = moment_new / correction / (jnp.sqrt(second_new / correction) + adam_epsilon)
    return (moment_new, second_new, master - step_rate * (normalized + decay_rate * master))


def shards(
    tokens,
    cotangent,
    in_master,
    in_moment,
    in_second,
    out_master,
    out_moment,
    out_second,
    vec_master,
    vec_moment,
    vec_second,
    rotary_scale,
):
    local_rows = tokens.shape[0]
    full_in, full_out = (
        lax.all_gather(in_master.astype(jnp.bfloat16), "head", axis=0, tiled=True),
        lax.all_gather(out_master.astype(jnp.bfloat16), "head", axis=0, tiled=True),
    )
    scale_value = rotary_scale[0].astype(jnp.float32)
    local_pos = lax.axis_index(("head", "ctx")) * local_rows + jnp.arange(
        local_rows, dtype=jnp.int32
    )
    cosine, sine_table = rotary_tables(local_pos.astype(jnp.float32), scale_value)
    inputs = tokens.astype(jnp.float32)
    norm_one, normed_one, inverse_one = layer_norm(inputs, vec_master[0:D], vec_master[D : 2 * D])
    norm_two, normed_two, inverse_two = layer_norm(
        inputs, vec_master[2 * D : 3 * D], vec_master[3 * D : 4 * D]
    )
    first_in = norm_one.astype(jnp.bfloat16)
    second_in = norm_two.astype(jnp.bfloat16)
    projected = (
        jnp.dot(first_in, full_in[:, : D + 2 * HEAD_DIM], preferred_element_type=jnp.float32)
        + vec_master[5 * D : 6 * D + 2 * HEAD_DIM]
    )
    hidden_in = (
        jnp.dot(second_in, full_in[:, D + 2 * HEAD_DIM :], preferred_element_type=jnp.float32)
        + vec_master[6 * D + 2 * HEAD_DIM :]
    )
    query_heads = projected[:, :D].reshape(local_rows, HEADS, HEAD_DIM)
    queries = (
        (rotate(query_heads, cosine[:, None, :], sine_table[:, None, :]) * 0.125)
        .astype(jnp.bfloat16)
        .reshape(local_rows, D)
    )
    key_part = rotate(projected[:, D : D + HEAD_DIM], cosine, sine_table)
    shared = jnp.concatenate([key_part, projected[:, D + HEAD_DIM :]], axis=1).astype(jnp.bfloat16)
    whole_kv = lax.all_gather(shared, ("head", "ctx"), axis=0, tiled=True)
    activated = jax.nn.gelu(hidden_in, approximate=False).astype(jnp.bfloat16)
    heads_here = queries.shape[1] // HEAD_DIM
    query_rows = queries.reshape(-1, HEAD_DIM)
    row_pos = jnp.repeat(local_pos, heads_here)
    log_sum = log_totals(query_rows, row_pos, whole_kv)
    attended = attend(query_rows, row_pos, whole_kv, log_sum)
    att_out = attended.reshape(queries.shape).astype(jnp.bfloat16)
    branch_pair = jnp.concatenate([att_out, activated], axis=1)
    output = (
        inputs
        + jnp.dot(branch_pair, full_out, preferred_element_type=jnp.float32)
        + vec_master[4 * D : 5 * D]
    ).astype(jnp.bfloat16)
    cot_in = cotangent.astype(jnp.float32)
    grad_out = lax.dot_general(
        branch_pair, cotangent, contract_rows, preferred_element_type=jnp.float32
    )
    back_proj = lax.dot_general(
        cotangent, full_out, contract_cols, preferred_element_type=jnp.float32
    )
    branch_grad = back_proj[:, :D].astype(jnp.bfloat16)
    gelu_back = jax.vjp(lambda pre_act: jax.nn.gelu(pre_act, approximate=False), hidden_in)[1]
    hidden_grad = gelu_back(back_proj[:, D:])[0].astype(jnp.bfloat16)
    grad_rows = branch_grad.reshape(-1, HEAD_DIM)
    row_inner = jnp.sum(grad_rows.astype(jnp.float32) * attended, axis=1)
    query_grad, kv_terms = attend_back(query_rows, row_pos, whole_kv, log_sum, grad_rows, row_inner)
    att_cos, att_sin = rotary_tables(local_pos.astype(jnp.float32), scale_value)
    query_pre = rotate(
        query_grad.reshape(-1, heads_here, HEAD_DIM) * 0.125,
        att_cos[:, None, :],
        -att_sin[:, None, :],
    )
    query_pre = query_pre.reshape(queries.shape).astype(jnp.bfloat16)
    kv_sum = lax.psum_scatter(kv_terms, ("head", "ctx"), scatter_dimension=0, tiled=True)
    shared_grad = jnp.concatenate(
        [rotate(kv_sum[:, :HEAD_DIM], cosine, -sine_table), kv_sum[:, HEAD_DIM:]], axis=1
    ).astype(jnp.bfloat16)
    attn_grad = jnp.concatenate([query_pre, shared_grad], axis=1)
    grad_in = jnp.concatenate(
        [
            lax.dot_general(first_in, attn_grad, contract_rows, preferred_element_type=jnp.float32),
            lax.dot_general(
                second_in, hidden_grad, contract_rows, preferred_element_type=jnp.float32
            ),
        ],
        axis=1,
    )
    norm_grad_one = lax.dot_general(
        attn_grad, full_in[:, : D + 2 * HEAD_DIM], contract_cols, preferred_element_type=jnp.float32
    )
    norm_grad_two = lax.dot_general(
        hidden_grad,
        full_in[:, D + 2 * HEAD_DIM :],
        contract_cols,
        preferred_element_type=jnp.float32,
    )
    input_one, gain_one, shift_one = norm_back(
        norm_grad_one, normed_one, inverse_one, vec_master[0:D]
    )
    input_two, gain_two, shift_two = norm_back(
        norm_grad_two, normed_two, inverse_two, vec_master[2 * D : 3 * D]
    )
    input_grad = (cot_in + input_one + input_two).astype(jnp.bfloat16)
    grad_vec = jnp.concatenate(
        [
            gain_one,
            shift_one,
            gain_two,
            shift_two,
            jnp.sum(cot_in, axis=0),
            jnp.sum(attn_grad.astype(jnp.float32), axis=0),
            jnp.sum(hidden_grad.astype(jnp.float32), axis=0),
        ]
    )
    shard_in, shard_out = (
        lax.psum_scatter(
            grad_in.astype(jnp.bfloat16), "head", scatter_dimension=0, tiled=True
        ).astype(jnp.float32),
        lax.psum_scatter(
            grad_out.astype(jnp.bfloat16), "head", scatter_dimension=0, tiled=True
        ).astype(jnp.float32),
    )
    summed_in, summed_out = lax.psum((shard_in, shard_out), ("dp", "ctx"))
    summed_vec = lax.psum(grad_vec, ("dp", "head", "ctx"))
    in_moment_new, in_second_new, in_master_new = adam_update(
        in_master, in_moment, in_second, summed_in, matrix_rate, weight_decay
    )
    out_moment_new, out_second_new, out_master_new = adam_update(
        out_master, out_moment, out_second, summed_out, matrix_rate, weight_decay
    )
    vec_moment_new, vec_second_new, vec_master_new = adam_update(
        vec_master, vec_moment, vec_second, summed_vec, vector_rate, 0.0
    )
    return (
        output,
        input_grad,
        in_moment_new,
        in_second_new,
        in_master_new,
        in_master_new.astype(jnp.bfloat16),
        out_moment_new,
        out_second_new,
        out_master_new,
        out_master_new.astype(jnp.bfloat16),
        vec_moment_new,
        vec_second_new,
        vec_master_new,
    )


MESH = pl.DeviceIdType.MESH
F32 = jnp.float32
BF16 = jnp.bfloat16
HALF_HEADS = HEADS // 2
VMEM_LIMIT = 30 * 1024 * 1024
ADAM_LIMIT = 47 * 1024 * 1024
BACK_LIMIT = 38 * 1024 * 1024


def vmem_specs(count):
    return [pl.BlockSpec(memory_space=pltpu.VMEM)] * count


def places():
    z = lax.axis_index("head")
    q = lax.axis_index("dp")
    c = lax.axis_index("ctx")
    qx = lax.rem(q, 2)
    qy = q // 2
    return z, q, c, qx, qy, qy * 2 + 1 - qx, (1 - qy) * 2 + qx


def greet(partners):
    barrier = pltpu.get_barrier_semaphore()
    for partner in partners:
        pl.semaphore_signal(barrier, inc=1, device_id=partner, device_id_type=MESH)
    pl.semaphore_wait(barrier, len(partners))


def remote(source, target, send_sem, recv_sem, device):
    return pltpu.make_async_remote_copy(
        src_ref=source,
        dst_ref=target,
        send_sem=send_sem,
        recv_sem=recv_sem,
        device_id=device,
        device_id_type=MESH,
    )


KV_END = D + 2 * HEAD_DIM
HALF_D = D // 2


def hidden_spans(core, ff, row_share):
    spans = []
    for owner in range((D + ff) // row_share):
        first = max(owner * row_share - D, 0)
        last = (owner + 1) * row_share - D
        if last > first:
            half = (last - first) // 2
            spans.append((first + core * half, half))
    return spans


def core_columns(array, core, ff, row_share):
    pieces = [array[..., core * HALF_D : (core + 1) * HALF_D], array[..., D:KV_END]]
    pieces += [
        array[..., KV_END + first : KV_END + first + size]
        for first, size in hidden_spans(core, ff, row_share)
    ]
    return jnp.concatenate(pieces, axis=-1)


def join_columns(pair, ff, row_share):
    pieces = [pair[0][..., :HALF_D], pair[1][..., :HALF_D], pair[0][..., HALF_D : HALF_D + 2 * HEAD_DIM]]
    at = HALF_D + 2 * HEAD_DIM
    for _, size in hidden_spans(0, ff, row_share):
        pieces += [pair[0][..., at : at + size], pair[1][..., at : at + size]]
        at += size
    return jnp.concatenate(pieces, axis=-1)


CHUNK = 512
IN_ROWS = 48
OUT_ROWS = 120


LANES = 128


def vec_row(vec, first, last):
    return jnp.concatenate(
        [vec[row : row + 1, :] for row in range(first // LANES, last // LANES)], axis=1
    )


def core_bias(vec, c, first, last):
    size = vec.shape[0] * LANES
    ff = size - 5 * D - KV_END
    share = (D + ff) // 4
    tail = vec_row(vec, 5 * D, size)
    return jnp.where(
        c == 0, core_columns(tail, 0, ff, share), core_columns(tail, 1, ff, share)
    )[:, first:last]


def front_kernel(
    in_master,
    out_master,
    tok,
    cot,
    vec,
    cos_ref,
    sin_ref,
    full_in,
    full_out,
    all_tok,
    all_cot,
    norm_one,
    norm_two,
    att_ref,
    dq_ref,
    dkv_ref,
    q_all,
    g_all,
    kv_all,
    keys,
    values,
    weights,
    tops,
    kept_out,
    kept_top,
    kept_inverse,
    dkeys,
    dvalues,
    z_send,
    z_recv,
    xy_send,
    xy_recv,
    pair_send,
    pair_recv,
    kv_send,
    kv_recv,
    local_sem,
):
    z, q, c, qx, qy, xn, yn = places()
    dg = (1 - qy) * 2 + 1 - qx
    to_x, to_y, to_pair = (xn, z, c), (yn, z, c), (q, z, 1 - c)
    greet([(q, lax.rem(z + k, 4), c) for k in (1, 2, 3)] + [to_x, to_y, to_pair])
    attn_cols = HALF_D + 2 * HEAD_DIM
    groups = ((0, 0, attn_cols), (1, 0, D), (0, attn_cols, full_in.shape[1]))
    full = (full_in, full_out)
    piece_rows = (IN_ROWS, OUT_ROWS)

    def span(group, part):
        which, first, last = groups[group]
        middle = (first + last) // 2
        if part == 1:
            return which, pl.ds(first, middle - first)
        if part == 2:
            return which, pl.ds(middle, last - middle)
        return which, pl.ds(first, last - first)

    def rows_of(which, plane, quarter):
        size = piece_rows[which]
        return pl.ds(pl.multiple_of((plane * 4 + quarter) * size, 8), size)

    def place(group, part, plane, quarter):
        which, cols = span(group, part)
        return full[which].at[rows_of(which, plane, quarter), cols]

    def z_copy(group, plane, way):
        piece = place(group, 0, plane, q)
        return remote(
            piece, piece, z_send.at[group, plane, way], z_recv.at[group, plane], (q, z + 1 - 2 * way, c)
        )

    def z_room(way):
        return z < 3 if way == 0 else z > 0

    def z_start(group):
        for way in range(2):

            @pl.when(z_room(way))
            def _():
                z_copy(group, z, way).start()

    def pair_copy(number):
        source, target = ((tok, all_tok), (cot, all_cot))[number]
        return remote(source, target.at[c], pair_send.at[number], pair_recv.at[number], to_pair)

    for number in range(2):
        pair_copy(number).start()
    locals_ = []
    for number, (source, target) in enumerate(((tok, all_tok.at[c]), (cot, all_cot.at[c]))):
        copy = pltpu.make_async_copy(source, target, local_sem.at[number])
        copy.start()
        locals_.append(copy)

    def xy_copy(path, group, plane):
        quarter = (q, q, xn, yn)[path]
        piece = place(group, (0, 0, 1, 2)[path], plane, quarter)
        return remote(
            piece,
            piece,
            xy_send.at[path, group, plane],
            xy_recv.at[path, group, plane],
            (to_x, to_y, to_y, to_x)[path],
        )

    def xy_landed(path, group, plane):
        quarter = (xn, yn, dg, dg)[path]
        piece = place(group, (0, 0, 1, 2)[path], plane, quarter)
        remote(
            piece, piece, xy_send.at[path, group, plane], xy_recv.at[path, group, plane], to_pair
        ).wait_recv()

    row_share = out_master.shape[0]
    ff = in_master.shape[1] - KV_END
    for quarter in range(4):
        block = in_master[quarter * IN_ROWS : (quarter + 1) * IN_ROWS, :]
        full_in[rows_of(0, z, quarter), :] = jnp.where(
            c == 0, core_columns(block, 0, ff, row_share), core_columns(block, 1, ff, row_share)
        ).astype(BF16)
    z_start(0)
    half_share = row_share // 2
    begin = jnp.where(z == 0, HALF_D * c, half_share * c)
    begin_tail = jnp.where(z == 0, D + (half_share - HALF_D) * c, half_share * c + HALF_D)
    base_row = pl.multiple_of(z * half_share, 16)
    full_out[pl.ds(base_row, HALF_D), :] = out_master[
        pl.ds(pl.multiple_of(begin, 8), HALF_D), :
    ].astype(BF16)
    full_out[pl.ds(pl.multiple_of(base_row + HALF_D, 16), half_share - HALF_D), :] = out_master[
        pl.ds(pl.multiple_of(begin_tail, 8), half_share - HALF_D), :
    ].astype(BF16)
    z_start(1)
    z_start(2)

    def spread(group, far):
        for way in range(2):
            plane = z - far if way == 0 else z + far

            @pl.when(plane >= 0 if way == 0 else plane < 4)
            def _():
                piece = place(group, 0, plane, q)
                remote(
                    piece, piece, z_send.at[group, plane, way], z_recv.at[group, plane], to_pair
                ).wait_recv()

                @pl.when(z_room(way))
                def _():
                    z_copy(group, plane, way).start()

                xy_copy(0, group, plane).start()
                xy_copy(1, group, plane).start()

    def either(far, work):
        for way in range(2):
            plane = z - far if way == 0 else z + far

            @pl.when(plane >= 0 if way == 0 else plane < 4)
            def _():
                work(plane)

    def relay(group, far):
        def work(plane):
            xy_landed(0, group, plane)
            xy_copy(2, group, plane).start()
            xy_landed(1, group, plane)
            xy_copy(3, group, plane).start()

        either(far, work)

    def settle(group):
        def work(plane):
            xy_landed(2, group, plane)
            xy_landed(3, group, plane)

        for far in (1, 2, 3):
            either(far, work)

    rows = tok.shape[0]

    def normalize(half):
        inputs = all_tok[half].astype(F32)
        center = inputs - jnp.mean(inputs, axis=-1, keepdims=True)
        inverse = lax.rsqrt(jnp.mean(center * center, axis=-1, keepdims=True) + 1e-05)
        normed = center * inverse
        here = pl.ds(pl.multiple_of(half * rows, rows), rows)
        norm_one[here, :] = (normed * vec_row(vec, 0, D) + vec_row(vec, D, 2 * D)).astype(BF16)
        norm_two[here, :] = (
            normed * vec_row(vec, 2 * D, 3 * D) + vec_row(vec, 3 * D, 4 * D)
        ).astype(BF16)

    for copy in locals_:
        copy.wait()
    normalize(c)
    spread(0, 1)
    for number, target in enumerate((all_tok, all_cot)):
        piece = target.at[1 - c]
        remote(piece, piece, pair_send.at[number], pair_recv.at[number], to_pair).wait_recv()
    normalize(1 - c)
    spread(0, 2)
    relay(0, 1)
    spread(0, 3)
    relay(0, 2)
    spread(1, 1)
    relay(0, 3)
    settle(0)

    half_rot = ROT // 2
    cosine, sine = cos_ref[...], sin_ref[...]

    def turn(block, cosine, sine):
        front, back = block[:half_rot], block[half_rot:ROT]
        return jnp.concatenate(
            [front * cosine - back * sine, back * cosine + front * sine, block[ROT:]], axis=0
        )

    projected = (
        jnp.dot(norm_one[...], full_in[:, :attn_cols], preferred_element_type=F32)
        + core_bias(vec, c, 0, attn_cols)
    ).T
    key_t = turn(projected[HALF_D : HALF_D + HEAD_DIM], cosine, sine)
    kv_all[z] = jnp.concatenate([key_t, projected[HALF_D + HEAD_DIM :]], axis=0).astype(BF16)

    def kv_copy(k):
        return remote(
            kv_all.at[z], kv_all.at[z], kv_send.at[0, k], kv_recv.at[0, k], (q, lax.rem(z + k, 4), c)
        )

    for k in (1, 2, 3):

        @pl.when(z + k < 4)
        def _():
            kv_copy(k).start()

    for head in range(HALF_HEADS):
        block = turn(projected[head * HEAD_DIM : (head + 1) * HEAD_DIM], cosine, sine) * 0.125
        q_all[:, head * CHUNK : (head + 1) * CHUNK] = block.astype(BF16)
    spread(1, 2)
    dkeys[...] = jnp.zeros_like(dkeys)
    dvalues[...] = jnp.zeros_like(dvalues)

    def spread_block(index):
        place_rows = pl.ds(pl.multiple_of(index * CHUNK, CHUNK), CHUNK)
        turned = kv_all[index].astype(F32).T.astype(BF16)
        keys[place_rows, :] = turned[:, :HEAD_DIM]
        values[place_rows, :] = turned[:, HEAD_DIM:]

    spread_block(z)
    relay(1, 1)
    for k in (1, 2, 3):

        @pl.when(z - k >= 0)
        def _():
            source = lax.rem(z + 4 - k, 4)
            remote(
                kv_all.at[source], kv_all.at[source], kv_send.at[0, k], kv_recv.at[0, k], to_pair
            ).wait_recv()
            spread_block(source)

    width = 2 * CHUNK
    cos_two = jnp.concatenate([cosine, cosine], axis=1)
    sin_two = jnp.concatenate([sine, sine], axis=1)
    polls = {
        (0, 0, 0): ((spread, 1, 3),),
        (0, 0, 1): ((relay, 1, 2),),
        (0, 0, 3): ((spread, 2, 1),),
        (1, 0, 0): ((relay, 1, 3),),
        (1, 0, 1): ((spread, 2, 2),),
        (1, 0, 3): ((relay, 2, 1), (spread, 2, 3)),
        (0, 1, 1): ((relay, 2, 2),),
        (1, 1, 0): ((relay, 2, 3),),
    }

    def poll(pair, late, index):
        for (number, phase, chunk), work in polls.items():
            if phase == late:

                @pl.when(jnp.logical_and(pair == number, index == chunk))
                def _():
                    for action, group, far in work:
                        action(group, far)

    def upstream_heads():
        settle(1)
        for head in range(HALF_HEADS):
            part = full_out[pl.ds(head * HEAD_DIM, HEAD_DIM), :]
            for half in range(2):
                g_all[:, pl.ds(head * CHUNK + half * rows, rows)] = lax.dot_general(
                    part, all_cot[half], contract_cols, preferred_element_type=F32
                ).astype(BF16)

    def rows_at(index):
        return pl.ds(pl.multiple_of(index * CHUNK, CHUNK), CHUNK)

    def forward_pair(pair, slot):
        cols = pl.ds(pl.multiple_of(pair * width, width), width)
        queries = q_all[:, cols]

        def forward(index, state, diagonal):
            top, total, out = state
            part = jnp.dot(keys[rows_at(index), :], queries, preferred_element_type=F32)
            if diagonal:
                key_place = lax.broadcasted_iota(jnp.int32, (CHUNK, width), 0)
                row_place = lax.rem(lax.broadcasted_iota(jnp.int32, (CHUNK, width), 1), CHUNK)
                part = jnp.where(key_place > row_place, neg_fill, part)
            above = jnp.maximum(top, jnp.max(part, axis=0, keepdims=True))
            part = jnp.exp(part - above)
            rounded = part.astype(BF16)
            weights[slot, rows_at(index), :] = rounded
            tops[slot, index] = above
            scale = jnp.exp(top - above)
            total = total * scale + jnp.sum(part, axis=0, keepdims=True)
            out = out * scale + jnp.dot(
                kv_all[index, HEAD_DIM:, :], rounded, preferred_element_type=F32
            )
            return above, total, out

        state = (
            jnp.full((1, width), neg_fill, F32),
            jnp.zeros((1, width), F32),
            jnp.zeros((HEAD_DIM, width), F32),
        )

        def forward_or_not(index, state):
            poll(pair, 0, index)
            return lax.cond(
                index < z, lambda old: forward(index, old, False), lambda old: old, state
            )

        state = lax.fori_loop(0, 4, forward_or_not, state)
        top, total, out = forward(z, state, True)
        inverse = 1.0 / total
        out = out * inverse
        base = pl.multiple_of(pair * 2 * HEAD_DIM, 2 * HEAD_DIM)
        second = pl.multiple_of(base + HEAD_DIM, HEAD_DIM)
        att_ref[pl.ds(base, HEAD_DIM), :] = out[:, :CHUNK].astype(BF16)
        att_ref[pl.ds(second, HEAD_DIM), :] = out[:, CHUNK:].astype(BF16)
        kept_out[slot] = out
        kept_top[slot] = top
        kept_inverse[slot] = inverse

    def backward_pair(pair, slot):
        cols = pl.ds(pl.multiple_of(pair * width, width), width)
        queries = q_all[:, cols]
        grads = g_all[:, cols].astype(F32)
        top, inverse = kept_top[slot], kept_inverse[slot]
        inner = jnp.sum(grads * kept_out[slot], axis=0, keepdims=True)

        def backward(index, dq):
            here = rows_at(index)
            factor = inverse * jnp.exp(tops[slot, index] - top)
            scaled = (grads * factor).astype(BF16)
            dprob = jnp.dot(values[here, :], scaled, preferred_element_type=F32)
            rounded = weights[slot, here, :]
            dscore = (rounded.astype(F32) * (dprob - inner * factor)).astype(BF16)
            dkeys[here, :] += lax.dot_general(
                dscore, queries, contract_cols, preferred_element_type=F32
            )
            dvalues[here, :] += lax.dot_general(
                rounded, scaled, contract_cols, preferred_element_type=F32
            )
            return dq + jnp.dot(kv_all[index, :HEAD_DIM, :], dscore, preferred_element_type=F32)

        def backward_or_not(index, dq):
            poll(pair, 1, index)
            return lax.cond(index <= z, lambda old: backward(index, old), lambda old: old, dq)

        dq = lax.fori_loop(0, 4, backward_or_not, jnp.zeros((HEAD_DIM, width), F32))
        dq = turn(dq * 0.125, cos_two, -sin_two)
        base = pl.multiple_of(pair * 2 * HEAD_DIM, 2 * HEAD_DIM)
        second = pl.multiple_of(base + HEAD_DIM, HEAD_DIM)
        dq_ref[pl.ds(base, HEAD_DIM), :] = dq[:, :CHUNK].astype(BF16)
        dq_ref[pl.ds(second, HEAD_DIM), :] = dq[:, CHUNK:].astype(BF16)

    def phase(step, carry):
        pair = jnp.where(step < 4, lax.rem(step, 2), 2)
        slot = lax.rem(pair, 2)
        ahead = jnp.logical_or(step < 2, step == 4)

        @pl.when(ahead)
        def _():
            forward_pair(pair, slot)

        pl.when(step == 1)(upstream_heads)

        @pl.when(jnp.logical_not(ahead))
        def _():
            backward_pair(pair, slot)

        return carry

    lax.fori_loop(0, 6, phase, 0)

    for index in range(4):
        here = pl.ds(index * CHUNK, CHUNK)
        dkv_ref[index] = jnp.concatenate([dkeys[here, :], dvalues[here, :]], axis=1)
    settle(2)
    for number in range(2):
        pair_copy(number).wait_send()
    for k in (1, 2, 3):

        @pl.when(z + k < 4)
        def _():
            kv_copy(k).wait_send()

    for group in range(3):
        for way in range(2):

            @pl.when(z_room(way))
            def _():
                z_copy(group, z, way).wait_send()

                for far in (1, 2, 3):
                    plane = z - far if way == 0 else z + far

                    @pl.when(plane >= 0 if way == 0 else plane < 4)
                    def _():
                        z_copy(group, plane, way).wait_send()

        for plane in range(4):

            @pl.when(z != plane)
            def _():
                for path in range(4):
                    xy_copy(path, group, plane).wait_send()


def front(in_master, out_master, tok, cot, vec, cosine, sine):
    rows, width = tok.shape
    core_cols = (in_master.shape[1] + 2 * HEAD_DIM) // 2
    chip_rows = 2 * rows
    dma = pltpu.SemaphoreType.DMA
    return pl.pallas_call(
        front_kernel,
        out_shape=(
            jax.ShapeDtypeStruct((4 * in_master.shape[0], core_cols), BF16),
            jax.ShapeDtypeStruct((2 * out_master.shape[0], width), BF16),
            jax.ShapeDtypeStruct((2, rows, width), BF16),
            jax.ShapeDtypeStruct((2, rows, width), BF16),
            jax.ShapeDtypeStruct((chip_rows, width), BF16),
            jax.ShapeDtypeStruct((chip_rows, width), BF16),
            jax.ShapeDtypeStruct((HALF_D, chip_rows), BF16),
            jax.ShapeDtypeStruct((HALF_D, chip_rows), BF16),
            jax.ShapeDtypeStruct((4, chip_rows, 2 * HEAD_DIM), F32),
        ),
        in_specs=vmem_specs(7),
        out_specs=vmem_specs(9),
        scratch_shapes=[
            pltpu.VMEM((HEAD_DIM, HALF_HEADS * CHUNK), BF16),
            pltpu.VMEM((HEAD_DIM, HALF_HEADS * CHUNK), BF16),
            pltpu.VMEM((4, 2 * HEAD_DIM, CHUNK), BF16),
            pltpu.VMEM((4 * CHUNK, HEAD_DIM), BF16),
            pltpu.VMEM((4 * CHUNK, HEAD_DIM), BF16),
            pltpu.VMEM((2, 4 * CHUNK, 2 * CHUNK), BF16),
            pltpu.VMEM((2, 4, 1, 2 * CHUNK), F32),
            pltpu.VMEM((2, HEAD_DIM, 2 * CHUNK), F32),
            pltpu.VMEM((2, 1, 2 * CHUNK), F32),
            pltpu.VMEM((2, 1, 2 * CHUNK), F32),
            pltpu.VMEM((4 * CHUNK, HEAD_DIM), F32),
            pltpu.VMEM((4 * CHUNK, HEAD_DIM), F32),
            dma((3, 4, 2)),
            dma((3, 4)),
            dma((4, 3, 4)),
            dma((4, 3, 4)),
            dma((2,)),
            dma((2,)),
            dma((1, 4)),
            dma((1, 4)),
            dma((2,)),
        ],
        compiler_params=pltpu.CompilerParams(
            collective_id=0, has_side_effects=True, vmem_limit_bytes=VMEM_LIMIT
        ),
        name="front",
    )(in_master, out_master, tok, cot, vec, cosine, sine)


PLANE_ORDER = (2, 1, 3, 0)
HIDDEN_BLOCK = 512
ROOT_HALF = 0.7071067811865476
GAUSS = 0.3989422804014327


def back_kernel(
    full_in,
    full_out,
    all_tok,
    all_cot,
    norm_one,
    norm_two,
    att_ref,
    dq_ref,
    dkv_part,
    vec_ref,
    cos_ref,
    sin_ref,
    output_ref,
    input_grad_ref,
    sum_in,
    sum_out,
    vec_sum,
    one_t,
    two_t,
    act,
    dhid,
    branch_t,
    qkv_grad,
    partial_out,
    upstream,
    out_other,
    up_other,
    g_in,
    g_out,
    x_in,
    x_out,
    y_in,
    y_out,
    ax_in,
    ax_out,
    ay_in,
    ay_out,
    bx_in,
    bx_out,
    by_in,
    by_out,
    t_in,
    t_out,
    z_in,
    z_out,
    own_in,
    own_out,
    vec_send,
    vec_recv,
    vec_zone,
    pair_in,
    summed,
    zone,
    dkv,
    send_sem,
    recv_sem,
    vec_send_sem,
    vec_recv_sem,
    last_send_sem,
    last_recv_sem,
    pair_send_sem,
    pair_recv_sem,
    part_send_sem,
    part_recv_sem,
    zone_send_sem,
    zone_recv_sem,
):
    z, q, c, qx, qy, xn, yn = places()
    dg = (1 - qy) * 2 + 1 - qx
    to_x, to_y, to_pair = (xn, z, c), (yn, z, c), (q, z, 1 - c)
    greet([(q, lax.rem(z + k, 4), c) for k in (1, 2, 3)] + [to_x, to_y, to_pair])
    sent = []

    def send(source, target, sems, index, device):
        copy = remote(source, target, sems[0].at[index], sems[1].at[index], device)
        copy.start()
        sent.append(copy)

    def landed(target, sems, index):
        remote(target, target, sems[0].at[index], sems[1].at[index], to_pair).wait_recv()

    main = (send_sem, recv_sem)
    vecs = (vec_send_sem, vec_recv_sem)
    lasts = (last_send_sem, last_recv_sem)
    pairs = (pair_send_sem, pair_recv_sem)
    parts = (part_send_sem, part_recv_sem)
    grads = (g_in, g_out)
    halves = tuple(ref.shape[-1] // 2 for ref in grads)
    first = tuple(pl.ds(0, half) for half in halves)
    second = tuple(pl.ds(half, half) for half in halves)
    from_x, from_y = (x_in, x_out), (y_in, y_out)
    ax, ay, bx, by = (ax_in, ax_out), (ay_in, ay_out), (bx_in, bx_out), (by_in, by_out)
    totals, zones, own = (t_in, t_out), (z_in, z_out), (own_in, own_out)
    outs = (sum_in, sum_out)
    rows = all_tok.shape[1]
    mine = pl.ds(pl.multiple_of(c * rows, rows), rows)
    other = pl.ds(pl.multiple_of((1 - c) * rows, rows), rows)
    attn_cols = HALF_D + 2 * HEAD_DIM
    hidden = full_in.shape[1] - attn_cols

    def plane_of(step):
        return lax.rem(z + PLANE_ORDER[step % 4], 4)

    def kind(step):
        return 1 if step < 4 else 0

    def exchange(step):
        h, a, j = plane_of(step), kind(step), step % 4
        if a == 1:
            size = 4 * OUT_ROWS
            left = branch_t[pl.ds(pl.multiple_of(h * size, 16), size), :]
            for half in range(2):
                cols = pl.ds(half * halves[1], halves[1])
                block = sum(
                    jnp.dot(
                        left[:, k * rows : (k + 1) * rows],
                        all_cot[k, :, cols],
                        preferred_element_type=F32,
                    )
                    for k in range(2)
                ).astype(BF16)
                for quarter in range(4):
                    g_out[h, quarter // 2, quarter % 2, :, cols] = block[
                        quarter * OUT_ROWS : (quarter + 1) * OUT_ROWS
                    ]
        else:
            size = 4 * IN_ROWS
            here = pl.ds(pl.multiple_of(h * size, 16), size)
            for number in range(4):
                cols = pl.ds(number * HIDDEN_BLOCK, HIDDEN_BLOCK)
                if number == 0:
                    block = jnp.dot(one_t[here, :], qkv_grad[...], preferred_element_type=F32)
                else:
                    block = jnp.dot(
                        two_t[here, :],
                        dhid[:, pl.ds((number - 1) * HIDDEN_BLOCK, HIDDEN_BLOCK)],
                        preferred_element_type=F32,
                    )
                block = block.astype(BF16)
                for quarter in range(4):
                    g_in[h, quarter // 2, quarter % 2, :, cols] = block[
                        quarter * IN_ROWS : (quarter + 1) * IN_ROWS
                    ]
        send(grads[a].at[h, :, 1 - qx, :, first[a]], from_x[a].at[j], main, (j, 0, a), to_x)
        send(grads[a].at[h, 1 - qy, :, :, second[a]], from_y[a].at[j], main, (j, 1, a), to_y)

    def halve(step):
        h, a, j = plane_of(step), kind(step), step % 4
        landed(from_x[a].at[j], main, (j, 0, a))
        ax[a][j] = (
            grads[a][h, 1 - qy, qx, :, first[a]].astype(F32) + from_x[a][j, 1 - qy].astype(F32)
        ).astype(BF16)
        send(ax[a].at[j], ay[a].at[j], main, (j, 2, a), to_y)
        landed(from_y[a].at[j], main, (j, 1, a))
        bx[a][j] = (
            grads[a][h, qy, 1 - qx, :, second[a]].astype(F32) + from_y[a][j, 1 - qx].astype(F32)
        ).astype(BF16)
        send(bx[a].at[j], by[a].at[j], main, (j, 3, a), to_x)

    def finish(step):
        h, a, j = plane_of(step), kind(step), step % 4
        shift = PLANE_ORDER[j]
        landed(ay[a].at[j], main, (j, 2, a))
        left = (
            grads[a][h, qy, qx, :, first[a]].astype(F32)
            + from_x[a][j, qy].astype(F32)
            + ay[a][j].astype(F32)
        )
        landed(by[a].at[j], main, (j, 3, a))
        right = (
            grads[a][h, qy, qx, :, second[a]].astype(F32)
            + from_y[a][j, qx].astype(F32)
            + by[a][j].astype(F32)
        )
        if shift == 0:
            own[a][:, first[a]] = left
            own[a][:, second[a]] = right
        else:
            totals[a][shift - 1, :, first[a]] = left.astype(BF16)
            totals[a][shift - 1, :, second[a]] = right.astype(BF16)
            send(totals[a].at[shift - 1], zones[a].at[shift - 1], main, (j, 4, a), (q, h, c))

    def share(a):
        for j in range(3):
            landed(zones[a].at[PLANE_ORDER[j] - 1], main, (j, 4, a))
        whole = own[a][...] + zones[a][0].astype(F32) + zones[a][1].astype(F32) + zones[a][2].astype(F32)
        outs[a][c, q] = whole.astype(BF16)
        piece = outs[a].at[c, q]
        send(piece, piece, lasts, (0, a), to_x)
        send(piece, piece, lasts, (1, a), to_y)
        send(piece, piece, pairs, (0, a), to_pair)

    def pass_on(a):
        piece = outs[a].at[c, xn]
        landed(piece, lasts, (0, a))
        part = outs[a].at[c, xn, :, first[a]]
        send(part, part, lasts, (2, a), to_y)
        send(piece, piece, pairs, (1, a), to_pair)
        piece = outs[a].at[c, yn]
        landed(piece, lasts, (1, a))
        part = outs[a].at[c, yn, :, second[a]]
        send(part, part, lasts, (3, a), to_x)
        send(piece, piece, pairs, (2, a), to_pair)

    def close(a):
        landed(outs[a].at[c, dg, :, first[a]], lasts, (2, a))
        landed(outs[a].at[c, dg, :, second[a]], lasts, (3, a))
        piece = outs[a].at[c, dg]
        send(piece, piece, pairs, (3, a), to_pair)

    def zone_copy(k):
        target = lax.rem(z + 4 - k, 4)
        return remote(
            summed.at[target],
            zone.at[k - 1],
            zone_send_sem.at[k],
            zone_recv_sem.at[k],
            (q, target, c),
        )

    send(dkv_part.at[:, other, :], pair_in, parts, 0, to_pair)

    branch_t[pl.ds(0, HALF_D), :] = att_ref[...]
    bias_up = core_bias(vec_ref, c, attn_cols, attn_cols + hidden)

    def before_gelu(number):
        return (
            jnp.dot(
                norm_two[...],
                full_in[:, pl.ds(attn_cols + number * HIDDEN_BLOCK, HIDDEN_BLOCK)],
                preferred_element_type=F32,
            )
            + bias_up[:, number * HIDDEN_BLOCK : (number + 1) * HIDDEN_BLOCK]
        )

    for number in range(hidden // HIDDEN_BLOCK):
        before = before_gelu(number)
        active = 0.5 * before * (1.0 + lax.erf(before * ROOT_HALF))
        act[:, pl.ds(number * HIDDEN_BLOCK, HIDDEN_BLOCK)] = active.astype(BF16)
        branch_t[pl.ds(HALF_D + number * HIDDEN_BLOCK, HIDDEN_BLOCK), :] = active.T.astype(BF16)
    exchange(0)
    exchange(1)
    landed(pair_in, parts, 0)
    for index in range(4):
        summed[index] = dkv_part[index, mine, :] + pair_in[index]
    for k in (1, 2, 3):

        @pl.when(z - k >= 0)
        def _():
            zone_copy(k).start()

    one_t[...] = norm_one[...].astype(F32).T.astype(BF16)
    two_t[...] = norm_two[...].astype(F32).T.astype(BF16)
    for number in range(hidden // HIDDEN_BLOCK):
        cols = pl.ds(number * HIDDEN_BLOCK, HIDDEN_BLOCK)
        before = before_gelu(number)
        slope = 0.5 * (1.0 + lax.erf(before * ROOT_HALF)) + before * (
            GAUSS * jnp.exp(-0.5 * before * before)
        )
        for k in range(2):
            here = pl.ds(k * rows, rows)
            back = lax.dot_general(
                all_cot[k],
                full_out[pl.ds(HALF_D + number * HIDDEN_BLOCK, HIDDEN_BLOCK), :],
                contract_cols,
                preferred_element_type=F32,
            )
            dhid[here, cols] = (back * slope[k * rows : (k + 1) * rows, :]).astype(BF16)
    halve(0)
    exchange(2)
    dkv[mine, :] = summed[z]
    for k in (1, 2, 3):

        @pl.when(z + k < 4)
        def _():
            remote(
                zone.at[k - 1], zone.at[k - 1], zone_send_sem.at[k], zone_recv_sem.at[k], to_pair
            ).wait_recv()
            dkv[mine, :] += zone[k - 1]

    send(dkv.at[mine, :], dkv.at[mine, :], parts, 1, to_pair)
    halve(1)
    exchange(3)
    finish(0)
    partial_out[...] = jnp.dot(
        att_ref[...].astype(F32).T.astype(BF16), full_out[:HALF_D, :], preferred_element_type=F32
    ) + jnp.dot(act[...], full_out[pl.ds(HALF_D, hidden), :], preferred_element_type=F32)
    send(partial_out.at[other, :], out_other, parts, 2, to_pair)
    landed(dkv.at[other, :], parts, 1)
    half_rot = ROT // 2
    turned = dkv[...].T
    front_part, back_part = turned[:half_rot], turned[half_rot:ROT]
    cosine, sine = cos_ref[...], sin_ref[...]
    turned = jnp.concatenate(
        [
            front_part * cosine + back_part * sine,
            back_part * cosine - front_part * sine,
            turned[ROT:],
        ],
        axis=0,
    )
    qkv_grad[:, :HALF_D] = dq_ref[...].astype(F32).T.astype(BF16)
    qkv_grad[:, HALF_D:] = turned.T.astype(BF16)
    halve(2)
    exchange(4)
    finish(1)
    keep = jnp.where(c == 0, 1.0, 0.0)
    vec_send[...] = jnp.zeros_like(vec_send)
    mine_vec = vec_send.at[0]
    column = lax.broadcasted_iota(jnp.int32, (1, attn_cols), 1)
    once = jnp.where(column < HALF_D, 1.0, keep)
    first_rows = jnp.zeros((1, D), F32)
    sums = [first_rows] * 4
    gain_one, gain_two = vec_row(vec_ref, 0, D), vec_row(vec_ref, 2 * D, 3 * D)
    for k in range(2):
        here = pl.ds(k * rows, rows)
        inputs = all_tok[k].astype(F32)
        center = inputs - jnp.mean(inputs, axis=-1, keepdims=True)
        inverse = lax.rsqrt(jnp.mean(center * center, axis=-1, keepdims=True) + 1e-05)
        normed = center * inverse
        masked = (qkv_grad[here, :].astype(F32) * once).astype(BF16)
        one = lax.dot_general(
            masked, full_in[:, :attn_cols], contract_cols, preferred_element_type=F32
        )
        two = lax.dot_general(
            dhid[here, :],
            full_in[:, pl.ds(attn_cols, hidden)],
            contract_cols,
            preferred_element_type=F32,
        )
        terms = (one * normed, one, two * normed, two)
        sums = [old + jnp.sum(term, axis=0, keepdims=True) for old, term in zip(sums, terms)]
        upstream[here, :] = one * gain_one + two * gain_two
    send(upstream.at[other, :], up_other, parts, 3, to_pair)
    halve(3)
    exchange(5)
    finish(2)
    for number in range(4):
        mine_vec[number : number + 1, :D] = sums[number]
    mine_vec[4:5, :D] = jnp.sum(all_cot[c].astype(F32), axis=0, keepdims=True)
    query_sums = jnp.sum(qkv_grad[...].astype(F32), axis=0, keepdims=True) * once
    hidden_sums = [
        jnp.sum(
            dhid[:, pl.ds(number * HIDDEN_BLOCK, HIDDEN_BLOCK)].astype(F32), axis=0, keepdims=True
        )
        for number in range(hidden // HIDDEN_BLOCK)
    ]
    for core in range(2):
        for number, piece in enumerate([query_sums] + hidden_sums):
            row = 4 * core + number
            mine_vec[row : row + 1, D:] = jnp.where(c == core, piece, 0.0)
    send(vec_send.at[0], vec_recv.at[0], vecs, 0, to_x)
    halve(4)
    exchange(6)
    finish(3)
    landed(vec_recv.at[0], vecs, 0)
    vec_send[1] = vec_send[0] + vec_recv[0]
    send(vec_send.at[1], vec_recv.at[1], vecs, 1, to_y)
    halve(5)
    exchange(7)
    finish(4)
    share(1)
    landed(vec_recv.at[1], vecs, 1)
    vec_send[2] = vec_send[1] + vec_recv[1]
    send(vec_send.at[2], vec_recv.at[2], vecs, 2, to_pair)
    halve(6)
    finish(5)
    pass_on(1)
    landed(vec_recv.at[2], vecs, 2)
    vec_send[3] = vec_send[2] + vec_recv[2]
    vec_zone[z] = vec_send[3]
    for k in (1, 2, 3):
        send(vec_send.at[3], vec_zone.at[z], vecs, 2 + k, (q, lax.rem(z + k, 4), c))
    halve(7)
    finish(6)
    close(1)
    landed(out_other, parts, 2)
    output_ref[...] = (
        all_tok[c].astype(F32) + (partial_out[mine, :] + out_other[...]) + vec_row(vec_ref, 4 * D, 5 * D)
    ).astype(BF16)
    landed(up_other, parts, 3)
    inputs = all_tok[c].astype(F32)
    center = inputs - jnp.mean(inputs, axis=-1, keepdims=True)
    inverse = lax.rsqrt(jnp.mean(center * center, axis=-1, keepdims=True) + 1e-05)
    normed = center * inverse
    total = upstream[mine, :] + up_other[...]
    inside = (
        total
        - jnp.mean(total, axis=-1, keepdims=True)
        - normed * jnp.mean(total * normed, axis=-1, keepdims=True)
    )
    finish(7)
    share(0)
    input_grad_ref[...] = (all_cot[c].astype(F32) + inverse * inside).astype(BF16)
    pass_on(0)
    for k in (1, 2, 3):
        landed(vec_zone.at[lax.rem(z + 4 - k, 4)], vecs, 2 + k)
    vec_sum[...] = (vec_zone[0] + vec_zone[1]) + (vec_zone[2] + vec_zone[3])
    close(0)
    for a in (1, 0):
        for index, quarter in enumerate((q, xn, yn, dg)):
            landed(outs[a].at[1 - c, quarter], pairs, (index, a))
    for copy in sent:
        copy.wait_send()
    for k in (1, 2, 3):

        @pl.when(z - k >= 0)
        def _():
            zone_copy(k).wait_send()


def back(full_in, full_out, all_tok, all_cot, norm_one, norm_two, att_t, dq_t, dkv, vec, cosine, sine):
    rows = all_tok.shape[1]
    chip_rows = 2 * rows
    cols_in, cols_out = full_in.shape[1], full_out.shape[1]
    hidden = cols_in - HALF_D - 2 * HEAD_DIM
    kv_width = 2 * HEAD_DIM
    vec_shape = (8, D + HALF_D + kv_width)
    dma = pltpu.SemaphoreType.DMA

    def both(lead, cut, kind):
        return [
            pltpu.VMEM(lead + (IN_ROWS, cols_in // cut), kind),
            pltpu.VMEM(lead + (OUT_ROWS, cols_out // cut), kind),
        ]

    def twice(*shape):
        return [dma(shape), dma(shape)]

    return pl.pallas_call(
        back_kernel,
        out_shape=(
            jax.ShapeDtypeStruct((rows, D), BF16),
            jax.ShapeDtypeStruct((rows, D), BF16),
            jax.ShapeDtypeStruct((2, 4, IN_ROWS, cols_in), BF16),
            jax.ShapeDtypeStruct((2, 4, OUT_ROWS, cols_out), BF16),
            jax.ShapeDtypeStruct(vec_shape, F32),
        ),
        in_specs=vmem_specs(12),
        out_specs=vmem_specs(5),
        scratch_shapes=[
            pltpu.VMEM((D, chip_rows), BF16),
            pltpu.VMEM((D, chip_rows), BF16),
            pltpu.VMEM((chip_rows, hidden), BF16),
            pltpu.VMEM((chip_rows, hidden), BF16),
            pltpu.VMEM((HALF_D + hidden, chip_rows), BF16),
            pltpu.VMEM((chip_rows, HALF_D + kv_width), BF16),
            pltpu.VMEM((chip_rows, D), F32),
            pltpu.VMEM((chip_rows, D), F32),
            pltpu.VMEM((rows, D), F32),
            pltpu.VMEM((rows, D), F32),
        ]
        + both((4, 2, 2), 1, BF16)
        + both((4, 2), 2, BF16)
        + both((4, 2), 2, BF16)
        + both((4,), 2, BF16) * 4
        + both((3,), 1, BF16) * 2
        + both((), 1, F32)
        + [
            pltpu.VMEM((4,) + vec_shape, F32),
            pltpu.VMEM((3,) + vec_shape, F32),
            pltpu.VMEM((4,) + vec_shape, F32),
            pltpu.VMEM((4, rows, kv_width), F32),
            pltpu.VMEM((4, rows, kv_width), F32),
            pltpu.VMEM((3, rows, kv_width), F32),
            pltpu.VMEM((chip_rows, kv_width), F32),
        ]
        + twice(4, 5, 2)
        + twice(6)
        + twice(4, 2)
        + twice(4, 2)
        + twice(4)
        + twice(4),
        compiler_params=pltpu.CompilerParams(
            collective_id=1, has_side_effects=True, vmem_limit_bytes=BACK_LIMIT
        ),
        name="back",
    )(full_in, full_out, all_tok, all_cot, norm_one, norm_two, att_t, dq_t, dkv, vec, cosine, sine)


ADAM_ROWS = 32
ADAM_OUT_ROWS = 96


def adam_fast(master, moment, second, gradient, step_rate, decay_rate):
    moment_new = 0.5 * moment + 0.5 * gradient
    second_new = 0.5 * second + 0.5 * gradient * gradient
    scale = 1.0 / (1.0 - 0.5**ADAM_STEP)
    normalized = moment_new * scale / (jnp.sqrt(second_new * scale) + adam_epsilon)
    return moment_new, second_new, master - step_rate * (normalized + decay_rate * master)


def adam_kernel(
    grad_in,
    grad_out,
    in_master,
    in_moment,
    in_second,
    out_master,
    out_moment,
    out_second,
    grad_vec,
    vec,
    vec_moment,
    vec_second,
    in_m,
    in_s,
    in_w,
    in_c,
    out_m,
    out_s,
    out_w,
    out_c,
    vec_m,
    vec_s,
    vec_w,
    held_gi,
    held_go,
    held_in,
    held_out,
    low_in,
    low_out,
    load_in,
    load_out,
    store_in,
    store_out,
):
    z = lax.axis_index("head")
    rows_in, cols_in = in_master.shape
    rows_out = out_master.shape[0]
    ff = cols_in - KV_END
    count_in, count_out = rows_in // ADAM_ROWS, rows_out // ADAM_OUT_ROWS
    half, attn = count_out // 2, HALF_D // ADAM_OUT_ROWS

    def in_rows(number):
        return pl.ds(pl.multiple_of(number * ADAM_ROWS, ADAM_ROWS), ADAM_ROWS)

    def out_rows(number):
        core, place = number // half, lax.rem(number, half)
        first = jnp.where(
            place < attn, core * attn + place, 2 * attn + core * (half - attn) + place - attn
        )
        block = jnp.where(z == 0, first, number)
        return pl.ds(pl.multiple_of(block * ADAM_OUT_ROWS, 8), ADAM_OUT_ROWS)

    def loads_in(number):
        here = in_rows(number)
        copies = [
            pltpu.make_async_copy(ref.at[here, :], held_in.at[k, here, :], load_in.at[number, k])
            for k, ref in enumerate((in_master, in_moment, in_second))
        ]
        return copies + [
            pltpu.make_async_copy(grad_in.at[:, here, :], held_gi.at[:, here, :], load_in.at[number, 3])
        ]

    def loads_out(number):
        here = out_rows(number)
        core, place = number // half, lax.rem(number, half)
        rows = pl.ds(pl.multiple_of(place * ADAM_OUT_ROWS, 16), ADAM_OUT_ROWS)
        copies = [
            pltpu.make_async_copy(ref.at[here, :], held_out.at[k, number], load_out.at[number, k])
            for k, ref in enumerate((out_master, out_moment, out_second))
        ]
        return copies + [
            pltpu.make_async_copy(grad_out.at[core, rows, :], held_go.at[number], load_out.at[number, 3])
        ]

    def stores_in(number):
        here = in_rows(number)
        copies = [
            pltpu.make_async_copy(held_in.at[k, here, :], ref.at[here, :], store_in.at[number, k])
            for k, ref in enumerate((in_w, in_m, in_s))
        ]
        return copies + [
            pltpu.make_async_copy(low_in.at[here, :], in_c.at[here, :], store_in.at[number, 3])
        ]

    def stores_out(number):
        here = out_rows(number)
        copies = [
            pltpu.make_async_copy(held_out.at[k, number], ref.at[here, :], store_out.at[number, k])
            for k, ref in enumerate((out_w, out_m, out_s))
        ]
        return copies + [
            pltpu.make_async_copy(low_out.at[number], out_c.at[here, :], store_out.at[number, 3])
        ]

    def every(count, copies_of, start):
        def one(number, carry):
            for copy in copies_of(number):
                copy.start() if start else copy.wait()
            return carry

        lax.fori_loop(0, count, one, 0)

    every(count_out, loads_out, True)
    every(count_in, loads_in, True)

    def step_out(number, carry):
        for copy in loads_out(number):
            copy.wait()
        first, new_second, weights = adam_fast(
            held_out[0, number],
            held_out[1, number],
            held_out[2, number],
            held_go[number].astype(F32),
            matrix_rate,
            weight_decay,
        )
        held_out[0, number] = weights
        held_out[1, number] = first
        held_out[2, number] = new_second
        low_out[number] = weights.astype(BF16)
        for copy in stores_out(number):
            copy.start()
        return carry

    lax.fori_loop(0, count_out, step_out, 0)

    def step_in(number, carry):
        for copy in loads_in(number):
            copy.wait()
        here = in_rows(number)
        joined = join_columns(
            (held_gi[0, here, :].astype(F32), held_gi[1, here, :].astype(F32)), ff, rows_out
        )
        first, new_second, weights = adam_fast(
            held_in[0, here, :], held_in[1, here, :], held_in[2, here, :], joined, matrix_rate, weight_decay
        )
        held_in[0, here, :] = weights
        held_in[1, here, :] = first
        held_in[2, here, :] = new_second
        low_in[here, :] = weights.astype(BF16)
        for copy in stores_in(number):
            copy.start()
        return carry

    lax.fori_loop(0, count_in, step_in, 0)
    cores = [
        jnp.concatenate([grad_vec[4 * core + row : 4 * core + row + 1, D:] for row in range(4)], axis=1)
        for core in range(2)
    ]
    whole = jnp.concatenate(
        [grad_vec[row : row + 1, :D] for row in range(5)] + [join_columns(cores, ff, rows_out)], axis=1
    )
    size = whole.shape[1]
    results = adam_fast(
        vec_row(vec, 0, size), vec_row(vec_moment, 0, size), vec_row(vec_second, 0, size), whole, vector_rate, 0.0
    )
    for target, result in zip((vec_m, vec_s, vec_w), results):
        for row in range(size // LANES):
            target[row : row + 1, :] = result[:, row * LANES : (row + 1) * LANES]
    every(count_out, stores_out, False)
    every(count_in, stores_in, False)


def adam(grad_in, grad_out, in_arrays, out_arrays, grad_vec, vec_arrays):
    rows_in, cols_in = in_arrays[0].shape
    rows_out, cols_out = out_arrays[0].shape
    count_in, count_out = rows_in // ADAM_ROWS, rows_out // ADAM_OUT_ROWS
    anywhere = pl.BlockSpec(memory_space=pl.ANY)
    still = pl.BlockSpec(memory_space=pltpu.VMEM)
    dma = pltpu.SemaphoreType.DMA

    def shapes(array, low):
        whole = jax.ShapeDtypeStruct(array.shape, F32)
        return [whole] * 3 + ([jax.ShapeDtypeStruct(array.shape, BF16)] if low else [])

    return pl.pallas_call(
        adam_kernel,
        out_shape=shapes(in_arrays[0], True) + shapes(out_arrays[0], True) + shapes(vec_arrays[0], False),
        in_specs=[anywhere] * 8 + [still] * 4,
        out_specs=[anywhere] * 8 + [still] * 3,
        scratch_shapes=[
            pltpu.VMEM(grad_in.shape, BF16),
            pltpu.VMEM((count_out, ADAM_OUT_ROWS, cols_out), BF16),
            pltpu.VMEM((3, rows_in, cols_in), F32),
            pltpu.VMEM((3, count_out, ADAM_OUT_ROWS, cols_out), F32),
            pltpu.VMEM((rows_in, cols_in), BF16),
            pltpu.VMEM((count_out, ADAM_OUT_ROWS, cols_out), BF16),
            dma((count_in, 4)),
            dma((count_out, 4)),
            dma((count_in, 4)),
            dma((count_out, 4)),
        ],
        compiler_params=pltpu.CompilerParams(vmem_limit_bytes=ADAM_LIMIT),
        name="adam",
    )(grad_in, grad_out, *in_arrays, *out_arrays, grad_vec, *vec_arrays)


def fast_shards(
    tokens,
    cotangent,
    in_master,
    in_moment,
    in_second,
    out_master,
    out_moment,
    out_second,
    vec_master,
    vec_moment,
    vec_second,
    rotary_scale,
):
    z = lax.axis_index("head")
    chip_rows = 2 * tokens.shape[0]
    size = vec_master.shape[0]
    vec, moments, seconds = (
        array.reshape(-1, LANES) for array in (vec_master, vec_moment, vec_second)
    )
    positions = (z * chip_rows + jnp.arange(chip_rows, dtype=jnp.int32)).astype(F32)
    cosine, sine_table = rotary_tables(positions, rotary_scale[0].astype(F32))
    cosine, sine_table = cosine.T, sine_table.T
    full_in, full_out, all_tok, all_cot, norm_one, norm_two, att_t, dq_t, dkv = front(
        in_master, out_master, tokens, cotangent, vec, cosine, sine_table
    )
    output, input_grad, sum_in, sum_out, sum_vec = back(
        full_in, full_out, all_tok, all_cot, norm_one, norm_two, att_t, dq_t, dkv, vec, cosine, sine_table
    )
    updated = adam(
        sum_in.reshape(2, -1, sum_in.shape[-1]),
        sum_out.reshape(2, -1, D),
        (in_master, in_moment, in_second),
        (out_master, out_moment, out_second),
        sum_vec,
        (vec, moments, seconds),
    )
    return (output, input_grad, *updated[:8], *(array.reshape(size) for array in updated[8:]))


def solution(mesh):
    placed = (
        P(("dp", "head", "ctx"), None),
        P(("dp", "head", "ctx"), None),
        P("head", None),
        P("head", None),
        P("head", None),
        P("head", None),
        P("head", None),
        P("head", None),
        P(),
        P(),
        P(),
        P(),
    )
    paired = dict(mesh.shape) == {"dp": 4, "head": 4, "ctx": 2}
    body = fast_shards if paired else shards
    return jax.shard_map(
        body,
        mesh=mesh,
        in_specs=placed,
        out_specs=(
            P(("dp", "head", "ctx"), None),
            P(("dp", "head", "ctx"), None),
            P("head", None),
            P("head", None),
            P("head", None),
            P("head", None),
            P("head", None),
            P("head", None),
            P("head", None),
            P("head", None),
            P(),
            P(),
            P(),
        ),
        check_vma=False,
    )
```
